256 devices in a mesh: member: 2 (over z), lat: 128 (over x, y, core).
Axes of the slice: x: 8, y: 8, z: 2, core: 2. Of those that a mesh axis runs over, the one named last changes fastest.
The devices are a block of a 8x8x16 slice.
Arguments:
- height: float32 [1024, 32, 1440], P(('member', 'lat')), parts along dimension 0, may hold values from -6 to 6
- zonal_courant: float32 [1024, 32, 1440], P(('member', 'lat')), parts along dimension 0, may hold values from -1.5 to 1.5
- merid_courant: float32 [1024, 32, 1440], P(('member', 'lat')), parts along dimension 0, may hold values from -1.5 to 1.5
- rates: float32 [64], P('member'), parts along dimension 0, may hold values from 0.05 to 0.5
- thresholds: float32 [64], P('member'), parts along dimension 0, may hold values from -3 to 3
- flags: int32 [512], replicated, may hold values from 0 to 1, as said below
- cutoffs: int32 [512], replicated, may hold values from 45 to 360
Outputs:
- filtered_height: float32 [1024, 32, 1440], P(('member', 'lat')), parts along dimension 0
The draws below stay inside these ranges and needn't reach their ends.
There are 2 independent parts, one for each index of `member`. The reference program is written for one: setup_inputs(seed, part) draws one part's arguments, and reference() takes and returns one part's arrays. A program takes and returns all parts, laid end to end along the dimension named above; an argument that names none is the same for every part. Nothing has to cross between parts.
Inputs may be any that keep to these rules, and one draw needn't show every extreme that they name: flags is 1 on a southern band of rows that starts at row 0 and on a northern band that ends at row 511, each band 512 // 8 to 128 rows long, and 0 on all other rows.
All inputs are finite; a program needn't handle non-finite values.
Results may differ from the reference program's by a relative error of at most 0.00007.
Values sent between devices are 32-bit elements; how exact they have to be, the bound alone decides.
A program may use at most 64 MiB of HBM per device.

```python
import math
import jax
import jax.numpy as jnp

NLON = 1440
LEV = 32
NLAT = 512


def draw_flags(key, part):
    south_key = jax.random.fold_in(key, 11)
    north_key = jax.random.fold_in(key, 23)
    south = jax.random.randint(south_key, (), NLAT // 8, NLAT // 4 + 1)
    north = jax.random.randint(north_key, (), NLAT // 8, NLAT // 4 + 1)
    rows = jnp.arange(NLAT, dtype=jnp.int32)
    return ((rows < south) | (rows >= NLAT - north)).astype(jnp.int32)


def with_ends(drawn, stream_key, low, high):
    spot = [jax.random.randint(jax.random.fold_in(stream_key, axis), (), 0, length) for axis, length in enumerate(drawn.shape)]
    widest = drawn.shape.index(max(drawn.shape))
    beside = spot[:widest] + [(spot[widest] + 1) % drawn.shape[widest]] + spot[widest + 1:]
    return drawn.at[tuple(spot)].set(low).at[tuple(beside)].set(high)


def block_levels(rng, shape, cuts, smallest, high):
    loudness = 1.0
    for axis_at, blocks in cuts:
        draws = jax.random.uniform(jax.random.fold_in(jax.random.fold_in(rng, 6), axis_at), (blocks,), jnp.float32, smallest / len(cuts), high / len(cuts))
        loudness = loudness * jnp.repeat(jnp.exp(draws), shape[axis_at] // blocks).reshape((-1,) + (1,) * (len(shape) - 1 - axis_at))
    return loudness


def normal_values(own_key, shape, scale, bound, pieces=(), kind=jnp.bfloat16):
    gain = block_levels(own_key, shape, pieces, -0.22, 0.18) if pieces else 1.0
    result = jax.random.normal(own_key, shape, jnp.float32) * scale * gain
    return jnp.minimum(jnp.maximum(result, -bound), bound).astype(kind)


def setup_inputs(seed: int = 0, part: int = 0) -> dict:
    splits = jax.random.split(jax.random.key(seed), 8)
    part_splits = jax.random.split(jax.random.fold_in(splits[7], part), 8)
    return {
        "height": normal_values(part_splits[0], (NLAT, LEV, NLON), 1.0, 6.0, ((0, 128),), jnp.float32),
        "zonal_courant": normal_values(part_splits[1], (NLAT, LEV, NLON), 0.3, 1.5, ((0, 128),), jnp.float32),
        "merid_courant": normal_values(part_splits[2], (NLAT, LEV, NLON), 0.3, 1.5, ((0, 128),), jnp.float32),
        "rates": jnp.clip(jnp.exp(jax.random.uniform(part_splits[3], (LEV,), jnp.float32, math.log(0.05), math.log(0.5))), 0.05, 0.5),
        "thresholds": normal_values(part_splits[4], (LEV,), 1.0, 3.0, (), jnp.float32),
        "flags": draw_flags(jax.random.fold_in(splits[7], 71), part),
        "cutoffs": with_ends(jax.random.randint(splits[6], (NLAT,), NLON // 32, NLON // 4 + 1), jax.random.fold_in(splits[6], 1), NLON // 32, (NLON // 4 + 1) - 1).astype(jnp.int32),
    }


def reference(height, zonal_courant, merid_courant, rates, thresholds, flags, cutoffs):
    rows = jnp.arange(NLAT, dtype=jnp.int32)
    cos_rows = jnp.sin(jnp.pi * (rows.astype(jnp.float32) + 0.5) / NLAT)
    faces = jnp.arange(NLAT + 1, dtype=jnp.int32)
    cos_faces = jnp.where((faces > 0) & (faces < NLAT), jnp.sin(jnp.pi * faces.astype(jnp.float32) / NLAT), jnp.float32(0.0))
    east = jnp.roll(height, -1, axis=2)
    west = jnp.roll(height, 1, axis=2)
    far_east = jnp.roll(height, -2, axis=2)
    face_height = (7.0 * (height + east) - (west + far_east)) / 12.0
    face_speed = 0.5 * (zonal_courant + jnp.roll(zonal_courant, -1, axis=2))
    zonal_flux = face_speed * face_height
    zonal_div = zonal_flux - jnp.roll(zonal_flux, 1, axis=2)
    padded_height = jnp.pad(height, ((2, 2), (0, 0), (0, 0)))
    padded_speed = jnp.pad(merid_courant, ((2, 2), (0, 0), (0, 0)))
    count = NLAT + 1
    merid_face = (7.0 * (padded_height[1:count + 1] + padded_height[2:count + 2]) - (padded_height[0:count] + padded_height[3:count + 3])) / 12.0
    merid_speed = 0.5 * (padded_speed[1:count + 1] + padded_speed[2:count + 2]) * cos_faces[:, None, None]
    merid_flux = merid_speed * merid_face
    merid_div = (merid_flux[1:] - merid_flux[:-1]) / cos_rows[:, None, None]
    source = -rates[None, :, None] * jax.nn.softplus(height - thresholds[None, :, None])
    level_mean = jnp.sum(jnp.sum(source, axis=2) * cos_rows[:, None], axis=0) / (NLON * jnp.sum(cos_rows))
    updated = height - zonal_div - merid_div + source - level_mean[None, :, None]
    waves = jnp.maximum(jnp.arange(NLON // 2 + 1), 1).astype(jnp.float32)
    ratio = cutoffs.astype(jnp.float32)[:, None] / waves[None, :]
    damp = jnp.where(flags[:, None] > 0, jnp.minimum(1.0, ratio * ratio), 1.0)
    spectrum = jnp.fft.rfft(updated, axis=2)
    filtered = jnp.fft.irfft(spectrum * damp[:, None, :], n=NLON, axis=2)
    return filtered.astype(jnp.float32)
```

```python
import functools
import math

import jax
import jax.numpy as jnp
import numpy as np
from jax import lax
from jax.experimental import pallas as pl
from jax.experimental.pallas import tpu as pltpu
from jax.sharding import Mesh
from jax.sharding import PartitionSpec as P

MESH = pl.DeviceIdType.MESH
NX, NY, NC = 8, 8, 2
RADIX = 12
HALF = 128
ROOT = math.sqrt(0.75)


def filter_tables(nlon):
    count = nlon // RADIX
    tiles = RADIX // 2
    fwd = np.zeros((tiles, 2 * HALF, 2 * HALF))
    inv = np.zeros((tiles, 2 * HALF, 2 * HALF))
    waves = np.zeros((8, 2 * HALF), np.int64)
    r = np.arange(count)

    def trig(k):
        angle = 2.0 * np.pi / nlon * ((r * k) % nlon)
        return np.cos(angle), np.sin(angle)

    def real_part(base, shift):
        lane = base
        for q in range(count // 2 + 1):
            k = RADIX * q + shift
            if k > nlon // 2:
                continue
            cos, sin = trig(k)
            weight = (1.0 if k in (0, nlon // 2) else 2.0) / nlon
            rows = slice(base, base + count)
            fwd[0, rows, lane] = cos
            inv[0, lane, rows] = cos * weight
            waves[0, lane] = k
            lane += 1
            if k not in (0, nlon // 2):
                fwd[0, rows, lane] = sin
                inv[0, lane, rows] = sin * weight
                waves[0, lane] = k
                lane += 1
        assert lane == base + count

    real_part(0, 0)
    real_part(HALF, RADIX // 2)
    for m in range(1, tiles):
        for q in range(count):
            k = RADIX * q + m
            cos, sin = trig(k)
            fwd[m, 0:count, q] = cos
            fwd[m, HALF : HALF + count, q] = -sin
            fwd[m, 0:count, HALF + q] = sin
            fwd[m, HALF : HALF + count, HALF + q] = cos
            waves[m, q] = waves[m, HALF + q] = min(k, nlon - k)
        inv[m] = fwd[m].T * (2.0 / nlon)
    inv_square = 1.0 / np.maximum(waves, 1).astype(np.float64) ** 2

    def halves(table):
        hi = table.astype(np.float32).astype(jnp.bfloat16)
        lo = (table - hi.astype(np.float64)).astype(np.float32).astype(jnp.bfloat16)
        return np.stack([hi, lo])

    return halves(fwd), halves(inv), inv_square.astype(np.float32)


def row_scalars(nlat):
    rows = np.arange(nlat)
    cos_row = np.sin(np.pi * (rows + 0.5) / nlat)
    faces = np.arange(nlat + 1)
    cos_face = np.where((faces > 0) & (faces < nlat), np.sin(np.pi * faces / nlat), 0.0)
    table = np.zeros((3 * nlat + HALF,))
    table[0:nlat] = cos_row
    table[nlat : 2 * nlat] = 1.0 / cos_row
    table[2 * nlat : 3 * nlat + 1] = cos_face / 24.0
    return table.astype(np.float32), float(np.sum(cos_row))


def twelve(e, o):
    plus, minus = e[0] + e[6], e[0] - e[6]
    e15p, e15m, e24p, e24m = e[1] + e[5], e[1] - e[5], e[2] + e[4], e[2] - e[4]
    a, b = plus + e24p, e15p + e[3]
    big, mid = ROOT * e15m, minus + 0.5 * e24m
    c, d = plus - 0.5 * e24p, 0.5 * e15p - e[3]
    even = [a + b, mid + big, c + d, minus - e24m, c - d, mid - big, a - b]
    o15p, o15m, o24p, o24m = o[0] + o[4], o[0] - o[4], o[1] + o[3], o[1] - o[3]
    f, g = 0.5 * o15p + o[2], ROOT * o24p
    s, t = ROOT * o15m, ROOT * o24m
    odd = [f + g, s + t, o15p - o[2], s - t, f - g]
    return even, odd


def split(x):
    hi = x.astype(jnp.bfloat16)
    return hi, (x - hi.astype(jnp.float32)).astype(jnp.bfloat16)


def kernel(
    dims, area, chunks,
    h_hbm, z_hbm, c_hbm, rates_hbm, thr_hbm, flags_hbm, cut_hbm, scal_hbm, ksq_hbm, fwd_hbm, inv_hbm,
    out,
    h, z, c, rates, thr, flags, cut, scal, ksq, fwd, inv,
    halo_h, halo_c, base, s_lo, s_hi, factor, ymat, wmat, part, xbuf, ysum, ybuf,
    in_sem, halo_send, halo_recv, x_send, x_recv, y_send, y_recv,
):
    rows, levels, nlon, nlat = dims
    count = nlon // RADIX
    x, y, core = lax.axis_index("lat_0"), lax.axis_index("lat_1"), lax.axis_index("lat_2")
    position = (x * NY + y) * NC + core
    total = NX * NY * NC

    local = [
        pltpu.make_async_copy(src, dst, in_sem.at[i])
        for i, (src, dst) in enumerate(
            [
                (h_hbm, h), (c_hbm, c), (rates_hbm, rates), (thr_hbm, thr), (scal_hbm, scal), (z_hbm, z),
                (flags_hbm, flags), (cut_hbm, cut), (ksq_hbm, ksq), (fwd_hbm, fwd), (inv_hbm, inv),
            ]
        )
    ]
    for copy in local:
        copy.start()

    def along(step):
        p = lax.rem(position + total + step, total)
        return {"lat_0": p // (NY * NC), "lat_1": lax.rem(p // NC, NY), "lat_2": lax.rem(p, NC)}

    def at_x(dx, k):
        return {"lat_0": lax.rem(x + dx, NX), "lat_1": y, "lat_2": k}

    def at_y(dy, k):
        return {"lat_0": x, "lat_1": lax.rem(y + dy + NY, NY), "lat_2": k}

    barrier = pltpu.get_barrier_semaphore()
    peers = [along(1), along(-1), at_x(0, 1 - core)]
    for k in range(NC):
        peers += [at_x(d, k) for d in range(1, NX)] + [at_y(d, k) for d in range(1, NY)]
    for peer in peers:
        pl.semaphore_signal(barrier, inc=1, device_id=peer, device_id_type=MESH)
    ymat[...] = jnp.zeros_like(ymat)
    pl.semaphore_wait(barrier, len(peers))

    local[0].wait()
    local[1].wait()
    halos = []
    for i, (start, size) in enumerate(chunks):
        lev = pl.ds(start, size)
        group = []
        for side, step, h_rows, c_row in ((0, 1, rows - 2, rows - 1), (1, -1, 0, 0)):
            group.append(
                pltpu.make_async_remote_copy(
                    h.at[pl.ds(h_rows, 2), lev], halo_h.at[side, :, lev],
                    halo_send.at[i, side, 0], halo_recv.at[i, side, 0], device_id=along(step), device_id_type=MESH,
                )
            )
            group.append(
                pltpu.make_async_remote_copy(
                    c.at[c_row, lev], halo_c.at[side, lev],
                    halo_send.at[i, side, 1], halo_recv.at[i, side, 1], device_id=along(step), device_id_type=MESH,
                )
            )
        for copy in group:
            copy.start()
        halos.append(group)

    for i in (2, 3, 4):
        local[i].wait()
    first = position * rows

    lane = lax.broadcasted_iota(jnp.int32, (8, HALF), 1)
    tile = jnp.zeros((8, HALF), jnp.float32)
    sub = lax.broadcasted_iota(jnp.int32, (8, 1), 0)

    def column(ref, start):
        value = jnp.zeros((8, 1), jnp.float32)
        for k in range(8):
            value = jnp.where(sub == k, ref[start + k], value)
        return value

    for g in range(levels // 8):
        lev = pl.ds(8 * g, 8)
        rate, threshold = column(rates, 8 * g), column(thr, 8 * g)
        sums = jnp.zeros((8, 1), jnp.float32)
        for r in range(rows):
            height = h[r, lev, :]
            s = height - threshold
            source = -rate * (jnp.maximum(s, 0.0) + jnp.log(1.0 + jnp.exp(-jnp.abs(s))))
            base[r, lev, :] = height + source
            sums = sums + scal[first + r] * jnp.sum(source, axis=1, keepdims=True)
        tile = jnp.where(lane == g, sums, tile)
    part[...] = tile

    x_out = [
        pltpu.make_async_remote_copy(
            part, xbuf.at[core], x_send.at[0], x_recv.at[core], device_id=at_x(0, 1 - core), device_id_type=MESH
        )
    ]
    for d in range(1, NX):
        for k in range(NC):
            x_out.append(
                pltpu.make_async_remote_copy(
                    part, xbuf.at[(NX - d) * NC + core], x_send.at[d * NC + k], x_recv.at[(NX - d) * NC + core],
                    device_id=at_x(d, k), device_id_type=MESH,
                )
            )
    for copy in x_out:
        copy.start()

    local[5].wait()

    def inv_cos(r):
        return scal[nlat + first + r]

    def face(f):
        return scal[2 * nlat + first + f]

    def west(a):
        return pltpu.roll(a, 1, axis=1)

    def east(a):
        return pltpu.roll(a, nlon - 1, axis=1)

    def local_terms(g, carry):
        lev = pl.ds(pl.multiple_of(8 * g, 8), 8)
        hr = [h[r, lev, :] for r in range(rows)]
        cr = [c[r, lev, :] for r in range(rows)]
        low = face(1) * (cr[0] + cr[1])
        high = face(3) * (cr[2] + cr[3])
        s_lo[lev, :] = low
        s_hi[lev, :] = high
        f1 = low * (7.0 * (hr[0] + hr[1]) - hr[2])
        f2 = face(2) * (cr[1] + cr[2]) * (7.0 * (hr[1] + hr[2]) - (hr[0] + hr[3]))
        f3 = high * (7.0 * (hr[2] + hr[3]) - hr[1])
        terms = [f1, f2 - f1, f3 - f2, -f3]
        for r in range(rows):
            pair = hr[r] + east(hr[r])
            zr = z[r, lev, :]
            speed = zr + east(zr)
            flux = speed * (8.0 * pair - (west(pair) + east(pair))) * (1.0 / 24.0)
            base[r, lev, :] = base[r, lev, :] - (flux - west(flux)) - terms[r] * inv_cos(r)
        return carry

    lax.fori_loop(0, levels // 8, local_terms, 0)

    for i in (6, 7, 8):
        local[i].wait()
    for r in range(rows):
        cutoff = cut[first + r].astype(jnp.float32)
        flag = flags[first + r].astype(jnp.float32)
        factor[r] = flag * (1.0 - jnp.minimum(1.0, cutoff * cutoff * ksq[...]))

    def landed(ref, sem):
        pltpu.make_async_copy(ref, ref, sem).wait()

    landed(xbuf.at[1 - core], x_recv.at[1 - core])
    total_x = part[...] + xbuf[1 - core]
    for slot in range(NC, NX * NC):
        landed(xbuf.at[slot], x_recv.at[slot])
        total_x = total_x + xbuf[slot]
    ysum[...] = total_x
    sign = 1 - 2 * core
    y_out = []
    for d in range(1, 4):
        for k in range(NC):
            y_out.append(
                pltpu.make_async_remote_copy(
                    ysum, ybuf.at[3 * core + d - 1], y_send.at[2 * d - 2 + k], y_recv.at[3 * core + d - 1],
                    device_id=at_y(sign * d, k), device_id_type=MESH,
                )
            )
    y_out.append(
        pltpu.make_async_remote_copy(
            ysum, ybuf.at[6], y_send.at[6], y_recv.at[6], device_id=at_y(4, core), device_id_type=MESH
        )
    )
    for copy in y_out:
        copy.start()

    local[9].wait()
    local[10].wait()
    keep_lo = jnp.where(position > 0, 1.0, 0.0)
    keep_hi = jnp.where(position < total - 1, 1.0, 0.0)
    for i, (start, size) in enumerate(chunks):
        for copy in halos[i]:
            copy.wait_recv()

        def edges(g, carry):
            lev = pl.ds(pl.multiple_of(start + 8 * g, 8), 8)
            h0, h1, h2, h3 = (h[r, lev, :] for r in range(rows))
            below, below2 = halo_h[0, 1, lev, :], halo_h[0, 0, lev, :]
            above, above2 = halo_h[1, 0, lev, :], halo_h[1, 1, lev, :]
            t1 = keep_lo * (s_lo[lev, :] * below)
            t3 = keep_hi * (s_hi[lev, :] * above)
            f0 = face(0) * (halo_c[0, lev, :] + c[0, lev, :]) * (7.0 * (below + h0) - (below2 + h1))
            f4 = face(4) * (halo_c[1, lev, :] + c[3, lev, :]) * (7.0 * (above + h3) - (above2 + h2))
            base[0, lev, :] = base[0, lev, :] + (t1 + f0) * inv_cos(0)
            base[1, lev, :] = base[1, lev, :] - t1 * inv_cos(1)
            base[2, lev, :] = base[2, lev, :] + t3 * inv_cos(2)
            base[3, lev, :] = base[3, lev, :] - (t3 + f4) * inv_cos(3)
            return carry

        lax.fori_loop(0, size // 8, edges, 0)

        blocks = size // 16
        units = rows * size

        def block_of(b):
            r = b // blocks
            lev = pl.ds(pl.multiple_of(start + 16 * lax.rem(b, blocks), 16), 16)
            return r, lev, pl.ds(pl.multiple_of(16 * b, 16), 16), pl.ds(pl.multiple_of(units + 16 * b, 16), 16)

        def forward(b, carry):
            r, lev, at_hi, at_lo = block_of(b)
            u = [base[r, lev, count * j : count * (j + 1)] for j in range(RADIX)]
            e = [u[0]] + [u[j] + u[RADIX - j] for j in range(1, 6)] + [u[6]]
            o = [u[j] - u[RADIX - j] for j in range(1, 6)]
            even, odd = twelve(e, o)
            halves = [(even[0], even[6])] + [(even[m], odd[m - 1]) for m in range(1, 6)]
            for m, pair in enumerate(halves):
                for k, value in enumerate(pair):
                    hi, lo = split(value)
                    ymat[m, at_hi, HALF * k : HALF * k + count] = hi
                    ymat[m, at_lo, HALF * k : HALF * k + count] = lo
            return carry

        lax.fori_loop(0, rows * blocks, forward, 0)

        def product(hilo, table):
            first_part = jnp.dot(hilo, table[0], preferred_element_type=jnp.float32)
            second = jnp.dot(hilo[0:units], table[1], preferred_element_type=jnp.float32)
            return first_part[0:units] + first_part[units : 2 * units] + second

        for m in range(RADIX // 2):
            waves = product(ymat[m, 0 : 2 * units, :], (fwd[0, m], fwd[1, m]))
            scaled = jnp.concatenate(
                [waves[r * size : (r + 1) * size] * factor[r, m : m + 1, :] for r in range(rows)], axis=0
            )
            wmat[m, 0:units, :] = product(jnp.concatenate(split(scaled), axis=0), (inv[0, m], inv[1, m]))

        def backward(b, carry):
            r, lev, at, _ = block_of(b)
            w = [[wmat[m, at, HALF * k : HALF * k + count] for k in range(2)] for m in range(RADIX // 2)]
            even, odd = twelve([w[0][0]] + [w[m][0] for m in range(1, 6)] + [w[0][1]], [w[m][1] for m in range(1, 6)])
            removed = [even[0]] + [even[j] + odd[j - 1] for j in range(1, 6)] + [even[6]]
            removed += [even[RADIX - j] - odd[RADIX - j - 1] for j in range(7, RADIX)]
            for j in range(RADIX):
                cols = slice(count * j, count * (j + 1))
                out[r, lev, cols] = base[r, lev, cols] - removed[j]
            return carry

        lax.fori_loop(0, rows * blocks, backward, 0)

    mean = ysum[...]
    for slot in range(7):
        landed(ybuf.at[slot], y_recv.at[slot])
        mean = mean + ybuf[slot]
    mean = mean * (1.0 / area)
    for g in range(levels // 8):
        lev = pl.ds(8 * g, 8)
        shift = jnp.sum(jnp.where(lane == g, mean, 0.0), axis=1, keepdims=True)
        for r in range(rows):
            out[r, lev, :] = out[r, lev, :] - shift

    for group in halos:
        for copy in group:
            copy.wait_send()
    for copy in x_out + y_out:
        copy.wait_send()


def local(height, zonal, merid, rates, thresholds, flags, cutoffs):
    rows, levels, nlon = height.shape
    nlat = rows * NX * NY * NC
    fwd, inv, ksq = filter_tables(nlon)
    scalars, cos_sum = row_scalars(nlat)
    chunks = ((0, levels // 2), (levels // 2, levels // 2))
    most = rows * max(size for _, size in chunks)
    tiles = RADIX // 2
    dims = (rows, levels, nlon, nlat)
    f32, bf16 = jnp.float32, jnp.bfloat16
    vmem, smem, dma = pltpu.VMEM, pltpu.SMEM, pltpu.SemaphoreType.DMA
    operands = (height, zonal, merid, rates, thresholds, flags, cutoffs, scalars, ksq, fwd, inv)
    return pl.pallas_call(
        functools.partial(kernel, dims, nlon * cos_sum, chunks),
        out_shape=jax.ShapeDtypeStruct(height.shape, f32),
        in_specs=[pl.BlockSpec(memory_space=pl.ANY)] * len(operands),
        out_specs=pl.BlockSpec(memory_space=vmem),
        scratch_shapes=[
            vmem(height.shape, f32), vmem(height.shape, f32), vmem(height.shape, f32),
            smem(rates.shape, f32), smem(thresholds.shape, f32), smem(flags.shape, jnp.int32),
            smem(cutoffs.shape, jnp.int32), smem(scalars.shape, f32),
            vmem(ksq.shape, f32), vmem(fwd.shape, bf16), vmem(inv.shape, bf16),
            vmem((2, 2, levels, nlon), f32), vmem((2, levels, nlon), f32), vmem(height.shape, f32),
            vmem((levels, nlon), f32), vmem((levels, nlon), f32), vmem((rows, 8, 2 * HALF), f32),
            vmem((tiles, 2 * most, 2 * HALF), bf16), vmem((tiles, most, 2 * HALF), f32),
            vmem((8, HALF), f32), vmem((NX * NC, 8, HALF), f32), vmem((8, HALF), f32), vmem((7, 8, HALF), f32),
            dma((11,)), dma((len(chunks), 2, 2)), dma((len(chunks), 2, 2)),
            dma((NX * NC,)), dma((NX * NC,)), dma((7,)), dma((7,)),
        ],
        compiler_params=pltpu.CompilerParams(collective_id=0, has_side_effects=True),
        name="advect_filter",
    )(*operands)


def solution(mesh):
    finer = Mesh(
        mesh.devices.reshape(mesh.shape["member"], NX, NY, NC), ("member", "lat_0", "lat_1", "lat_2")
    )
    whole = P(("member", "lat_0", "lat_1", "lat_2"), None, None)
    placed = (whole, whole, whole, P("member"), P("member"), P(), P())
    return jax.shard_map(local, mesh=finer, in_specs=placed, out_specs=whole, check_vma=False)
```

```python
import functools
import math

import jax
import jax.numpy as jnp
import numpy as np
from jax import lax
from jax.experimental import pallas as pl
from jax.experimental.pallas import tpu as pltpu
from jax.sharding import Mesh
from jax.sharding import PartitionSpec as P

MESH = pl.DeviceIdType.MESH
NX, NY, NC = 8, 8, 2
RADIX = 12
HALF = 128
ROOT = math.sqrt(0.75)


def filter_tables(nlon):
    count = nlon // RADIX
    tiles = RADIX // 2
    fwd = np.zeros((tiles, 2 * HALF, 2 * HALF))
    inv = np.zeros((tiles, 2 * HALF, 2 * HALF))
    waves = np.zeros((8, 2 * HALF), np.int64)
    r = np.arange(count)

    def trig(k):
        angle = 2.0 * np.pi / nlon * ((r * k) % nlon)
        return np.cos(angle), np.sin(angle)

    def real_part(base, shift):
        lane = base
        for q in range(count // 2 + 1):
            k = RADIX * q + shift
            if k > nlon // 2:
                continue
            cos, sin = trig(k)
            weight = (1.0 if k in (0, nlon // 2) else 2.0) / nlon
            rows = slice(base, base + count)
            fwd[0, rows, lane] = cos
            inv[0, lane, rows] = cos * weight
            waves[0, lane] = k
            lane += 1
            if k not in (0, nlon // 2):
                fwd[0, rows, lane] = sin
                inv[0, lane, rows] = sin * weight
                waves[0, lane] = k
                lane += 1
        assert lane == base + count

    real_part(0, 0)
    real_part(HALF, RADIX // 2)
    for m in range(1, tiles):
        for q in range(count):
            k = RADIX * q + m
            cos, sin = trig(k)
            fwd[m, 0:count, q] = cos
            fwd[m, HALF : HALF + count, q] = -sin
            fwd[m, 0:count, HALF + q] = sin
            fwd[m, HALF : HALF + count, HALF + q] = cos
            waves[m, q] = waves[m, HALF + q] = min(k, nlon - k)
        inv[m] = fwd[m].T * (2.0 / nlon)
    inv_square = 1.0 / np.maximum(waves, 1).astype(np.float64) ** 2

    def halves(table):
        hi = table.astype(np.float32).astype(jnp.bfloat16)
        lo = (table - hi.astype(np.float64)).astype(np.float32).astype(jnp.bfloat16)
        return np.stack([hi, lo])

    return halves(fwd), halves(inv), inv_square.astype(np.float32)


def row_scalars(nlat):
    rows = np.arange(nlat)
    cos_row = np.sin(np.pi * (rows + 0.5) / nlat)
    faces = np.arange(nlat + 1)
    cos_face = np.where((faces > 0) & (faces < nlat), np.sin(np.pi * faces / nlat), 0.0)
    table = np.zeros((3 * nlat + HALF,))
    table[0:nlat] = cos_row
    table[nlat : 2 * nlat] = 1.0 / cos_row
    table[2 * nlat : 3 * nlat + 1] = cos_face / 24.0
    return table.astype(np.float32), float(np.sum(cos_row))


def twelve(e, o):
    plus, minus = e[0] + e[6], e[0] - e[6]
    e15p, e15m, e24p, e24m = e[1] + e[5], e[1] - e[5], e[2] + e[4], e[2] - e[4]
    a, b = plus + e24p, e15p + e[3]
    big, mid = ROOT * e15m, minus + 0.5 * e24m
    c, d = plus - 0.5 * e24p, 0.5 * e15p - e[3]
    even = [a + b, mid + big, c + d, minus - e24m, c - d, mid - big, a - b]
    o15p, o15m, o24p, o24m = o[0] + o[4], o[0] - o[4], o[1] + o[3], o[1] - o[3]
    f, g = 0.5 * o15p + o[2], ROOT * o24p
    s, t = ROOT * o15m, ROOT * o24m
    odd = [f + g, s + t, o15p - o[2], s - t, f - g]
    return even, odd


def split(x):
    hi = x.astype(jnp.bfloat16)
    return hi, (x - hi.astype(jnp.float32)).astype(jnp.bfloat16)


def kernel(
    dims, area, chunks,
    h_hbm, z_hbm, c_hbm, rates_hbm, thr_hbm, flags_hbm, cut_hbm, scal_hbm, ksq_hbm, fwd_hbm, inv_hbm,
    out,
    h, z, c, rates, thr, flags, cut, scal, ksq, fwd, inv,
    halo_h, halo_c, base, s_lo, s_hi, factor, ymat, wmat, part, xbuf, ysum, ybuf,
    mean, mean_in,
    in_sem, halo_send, halo_recv, x_send, x_recv, y_send, y_recv, mean_send, mean_recv, low_in, root_in,
):
    rows, levels, nlon, nlat = dims
    count = nlon // RADIX
    x, y, core = lax.axis_index("lat_0"), lax.axis_index("lat_1"), lax.axis_index("lat_2")
    position = (x * NY + y) * NC + core
    total = NX * NY * NC

    local = [
        pltpu.make_async_copy(src, dst, in_sem.at[i])
        for i, (src, dst) in enumerate(
            [
                (h_hbm, h), (c_hbm, c), (rates_hbm, rates), (thr_hbm, thr), (scal_hbm, scal), (z_hbm, z),
                (flags_hbm, flags), (cut_hbm, cut), (ksq_hbm, ksq), (fwd_hbm, fwd), (inv_hbm, inv),
            ]
        )
    ]
    for copy in local:
        copy.start()

    last = NX * NY * NC - 1
    is_root = jnp.logical_and(x == 0, core == 1)

    def along(step):
        p = lax.rem(position + total + step, total)
        return {"lat_0": p // (NY * NC), "lat_1": lax.rem(p // NC, NY), "lat_2": lax.rem(p, NC)}

    def row(k):
        return {"lat_0": jnp.int32(k // NC), "lat_1": y, "lat_2": jnp.int32(k % NC)}

    def column(d):
        return {"lat_0": jnp.int32(0), "lat_1": y + d, "lat_2": jnp.int32(1)}

    def signal(sem, device):
        pl.semaphore_signal(sem, inc=1, device_id=device, device_id_type=MESH)

    barrier = pltpu.get_barrier_semaphore()

    @pl.when(position > 0)
    def _():
        signal(barrier, along(-1))

    @pl.when(is_root)
    def _():
        for k in range(NX * NC):
            if k != 1:
                signal(barrier, row(k))
        for d in range(1, NY):

            @pl.when(y >= d)
            def _():
                signal(barrier, column(-d))

    pl.semaphore_wait(barrier, jnp.where(position < last, 1, 0) + jnp.where(is_root, NY - 1 - y, 1))

    @pl.when(position < last)
    def _():
        signal(low_in, along(1))

    @pl.when(is_root)
    def _():
        for d in range(1, NY):

            @pl.when(y + d < NY)
            def _():
                signal(root_in.at[d - 1], column(d))

    local[0].wait()
    local[1].wait()

    def halo_copies(i, side):
        start, size = chunks[i]
        lev = pl.ds(start, size)
        step, h_row, c_row = ((1, rows - 2, rows - 1), (-1, 0, 0))[side]
        sems = [(halo_send.at[i, side, k], halo_recv.at[i, side, k]) for k in range(2)]
        pairs = ((h.at[pl.ds(h_row, 2), lev], halo_h.at[side, :, lev]), (c.at[c_row, lev], halo_c.at[side, lev]))
        return [
            pltpu.make_async_remote_copy(
                src, dst, send, recv, device_id=along(step), device_id_type=MESH
            )
            for (src, dst), (send, recv) in zip(pairs, sems)
        ]

    @pl.when(position < last)
    def _():
        for i in range(len(chunks)):
            for copy in halo_copies(i, 0):
                copy.start()

    ymat[...] = jnp.zeros_like(ymat)

    @pl.when(position == 0)
    def _():
        halo_h[0] = jnp.zeros_like(halo_h[0])
        halo_c[0] = jnp.zeros_like(halo_c[0])

    @pl.when(position == last)
    def _():
        halo_h[1] = jnp.zeros_like(halo_h[1])
        halo_c[1] = jnp.zeros_like(halo_c[1])

    for i in (2, 3, 4):
        local[i].wait()
    first = position * rows

    lane = lax.broadcasted_iota(jnp.int32, (8, HALF), 1)
    tile = jnp.zeros((8, HALF), jnp.float32)
    sub = lax.broadcasted_iota(jnp.int32, (8, 1), 0)

    def levels_of(ref, start):
        value = jnp.zeros((8, 1), jnp.float32)
        for k in range(8):
            value = jnp.where(sub == k, ref[start + k], value)
        return value

    for g in range(levels // 8):
        lev = pl.ds(8 * g, 8)
        rate, threshold = levels_of(rates, 8 * g), levels_of(thr, 8 * g)
        sums = jnp.zeros((8, 1), jnp.float32)
        for r in range(rows):
            height = h[r, lev, :]
            s = height - threshold
            source = -rate * (jnp.maximum(s, 0.0) + jnp.log(1.0 + jnp.exp(-jnp.abs(s))))
            base[r, lev, :] = height + source
            sums = sums + scal[first + r] * jnp.sum(source, axis=1, keepdims=True)
        tile = jnp.where(lane == g, sums, tile)
    part[...] = tile

    def part_copy(slot):
        return pltpu.make_async_remote_copy(
            part, xbuf.at[slot], x_send, x_recv.at[slot], device_id=row(1), device_id_type=MESH
        )

    @pl.when(jnp.logical_not(is_root))
    def _():
        part_copy(x * NC + core).start()

    @pl.when(position > 0)
    def _():
        pl.semaphore_wait(low_in, 1)
        for i in range(len(chunks)):
            for copy in halo_copies(i, 1):
                copy.start()

    local[5].wait()

    def inv_cos(r):
        return scal[nlat + first + r]

    def face(f):
        return scal[2 * nlat + first + f]

    def west(a):
        return pltpu.roll(a, 1, axis=1)

    def east(a):
        return pltpu.roll(a, nlon - 1, axis=1)

    def local_terms(g, carry):
        lev = pl.ds(pl.multiple_of(8 * g, 8), 8)
        hr = [h[r, lev, :] for r in range(rows)]
        cr = [c[r, lev, :] for r in range(rows)]
        low = face(1) * (cr[0] + cr[1])
        high = face(3) * (cr[2] + cr[3])
        s_lo[lev, :] = low
        s_hi[lev, :] = high
        f1 = low * (7.0 * (hr[0] + hr[1]) - hr[2])
        f2 = face(2) * (cr[1] + cr[2]) * (7.0 * (hr[1] + hr[2]) - (hr[0] + hr[3]))
        f3 = high * (7.0 * (hr[2] + hr[3]) - hr[1])
        terms = [f1, f2 - f1, f3 - f2, -f3]
        for r in range(rows):
            pair = hr[r] + east(hr[r])
            zr = z[r, lev, :]
            speed = zr + east(zr)
            flux = speed * (8.0 * pair - (west(pair) + east(pair))) * (1.0 / 24.0)
            base[r, lev, :] = base[r, lev, :] - (flux - west(flux)) - terms[r] * inv_cos(r)
        return carry

    lax.fori_loop(0, levels // 8, local_terms, 0)

    for i in (6, 7, 8):
        local[i].wait()
    for r in range(rows):
        cutoff = cut[first + r].astype(jnp.float32)
        flag = flags[first + r].astype(jnp.float32)
        factor[r] = flag * (1.0 - jnp.minimum(1.0, cutoff * cutoff * ksq[...]))

    def landed(ref, sem):
        pltpu.make_async_copy(ref, ref, sem).wait()

    def sum_copy(d):
        return pltpu.make_async_remote_copy(
            ysum, ybuf.at[y], y_send.at[y + d], y_recv.at[y], device_id=column(d), device_id_type=MESH
        )

    def mean_copy(k):
        return pltpu.make_async_remote_copy(
            mean, mean_in, mean_send.at[k], mean_recv, device_id=row(k), device_id_type=MESH
        )

    @pl.when(is_root)
    def _():
        acc = part[...]
        for k in range(NX * NC):
            if k != 1:
                landed(xbuf.at[k], x_recv.at[k])
                acc = acc + xbuf[k]
        ysum[...] = acc
        for d in range(1, NY):

            @pl.when(y + d < NY)
            def _():
                sum_copy(d).start()

        for d in range(1, NY):

            @pl.when(y >= d)
            def _():
                pl.semaphore_wait(root_in.at[d - 1], 1)
                sum_copy(-d).start()

        mean[...] = acc
        for k in range(NY):

            @pl.when(y != k)
            def _():
                landed(ybuf.at[k], y_recv.at[k])
                mean[...] = mean[...] + ybuf[k]

        mean[...] = mean[...] * (1.0 / area)
        for k in range(NX * NC):
            if k != 1:
                mean_copy(k).start()
        mean_in[...] = mean[...]

    local[9].wait()
    local[10].wait()
    for i, (start, size) in enumerate(chunks):
        @pl.when(position > 0)
        def _():
            for copy in halo_copies(i, 0):
                copy.wait_recv()

        @pl.when(position < last)
        def _():
            for copy in halo_copies(i, 1):
                copy.wait_recv()

        def edges(g, carry):
            lev = pl.ds(pl.multiple_of(start + 8 * g, 8), 8)
            h0, h1, h2, h3 = (h[r, lev, :] for r in range(rows))
            below, below2 = halo_h[0, 1, lev, :], halo_h[0, 0, lev, :]
            above, above2 = halo_h[1, 0, lev, :], halo_h[1, 1, lev, :]
            t1 = s_lo[lev, :] * below
            t3 = s_hi[lev, :] * above
            f0 = face(0) * (halo_c[0, lev, :] + c[0, lev, :]) * (7.0 * (below + h0) - (below2 + h1))
            f4 = face(4) * (halo_c[1, lev, :] + c[3, lev, :]) * (7.0 * (above + h3) - (above2 + h2))
            base[0, lev, :] = base[0, lev, :] + (t1 + f0) * inv_cos(0)
            base[1, lev, :] = base[1, lev, :] - t1 * inv_cos(1)
            base[2, lev, :] = base[2, lev, :] + t3 * inv_cos(2)
            base[3, lev, :] = base[3, lev, :] - (t3 + f4) * inv_cos(3)
            return carry

        lax.fori_loop(0, size // 8, edges, 0)

        blocks = size // 16
        units = rows * size

        def block_of(b):
            r = b // blocks
            lev = pl.ds(pl.multiple_of(start + 16 * lax.rem(b, blocks), 16), 16)
            return r, lev, pl.ds(pl.multiple_of(16 * b, 16), 16), pl.ds(pl.multiple_of(units + 16 * b, 16), 16)

        def forward(b, carry):
            r, lev, at_hi, at_lo = block_of(b)
            u = [base[r, lev, count * j : count * (j + 1)] for j in range(RADIX)]
            e = [u[0]] + [u[j] + u[RADIX - j] for j in range(1, 6)] + [u[6]]
            o = [u[j] - u[RADIX - j] for j in range(1, 6)]
            even, odd = twelve(e, o)
            halves = [(even[0], even[6])] + [(even[m], odd[m - 1]) for m in range(1, 6)]
            for m, pair in enumerate(halves):
                for k, value in enumerate(pair):
                    hi, lo = split(value)
                    ymat[m, at_hi, HALF * k : HALF * k + count] = hi
                    ymat[m, at_lo, HALF * k : HALF * k + count] = lo
            return carry

        lax.fori_loop(0, rows * blocks, forward, 0)

        def product(hilo, table):
            first_part = jnp.dot(hilo, table[0], preferred_element_type=jnp.float32)
            second = jnp.dot(hilo[0:units], table[1], preferred_element_type=jnp.float32)
            return first_part[0:units] + first_part[units : 2 * units] + second

        for m in range(RADIX // 2):
            waves = product(ymat[m, 0 : 2 * units, :], (fwd[0, m], fwd[1, m]))
            scaled = jnp.concatenate(
                [waves[r * size : (r + 1) * size] * factor[r, m : m + 1, :] for r in range(rows)], axis=0
            )
            wmat[m, 0:units, :] = product(jnp.concatenate(split(scaled), axis=0), (inv[0, m], inv[1, m]))

        def backward(b, carry):
            r, lev, at, _ = block_of(b)
            w = [[wmat[m, at, HALF * k : HALF * k + count] for k in range(2)] for m in range(RADIX // 2)]
            even, odd = twelve([w[0][0]] + [w[m][0] for m in range(1, 6)] + [w[0][1]], [w[m][1] for m in range(1, 6)])
            removed = [even[0]] + [even[j] + odd[j - 1] for j in range(1, 6)] + [even[6]]
            removed += [even[RADIX - j] - odd[RADIX - j - 1] for j in range(7, RADIX)]
            for j in range(RADIX):
                cols = slice(count * j, count * (j + 1))
                out[r, lev, cols] = base[r, lev, cols] - removed[j]
            return carry

        lax.fori_loop(0, rows * blocks, backward, 0)

    @pl.when(jnp.logical_not(is_root))
    def _():
        mean_copy(0).wait_recv()

    for g in range(levels // 8):
        lev = pl.ds(8 * g, 8)
        shift = jnp.sum(jnp.where(lane == g, mean_in[...], 0.0), axis=1, keepdims=True)
        for r in range(rows):
            out[r, lev, :] = out[r, lev, :] - shift

    for side, sender in ((0, position < last), (1, position > 0)):

        @pl.when(sender)
        def _():
            for i in range(len(chunks)):
                for copy in halo_copies(i, side):
                    copy.wait_send()

    @pl.when(is_root)
    def _():
        for d in range(1, NY):
            for step, used in ((d, y + d < NY), (-d, y >= d)):

                @pl.when(used)
                def _():
                    sum_copy(step).wait_send()

        for k in range(NX * NC):
            if k != 1:
                mean_copy(k).wait_send()

    @pl.when(jnp.logical_not(is_root))
    def _():
        part_copy(x * NC + core).wait_send()


def local(height, zonal, merid, rates, thresholds, flags, cutoffs):
    rows, levels, nlon = height.shape
    nlat = rows * NX * NY * NC
    fwd, inv, ksq = filter_tables(nlon)
    scalars, cos_sum = row_scalars(nlat)
    chunks = ((0, levels // 2), (levels // 2, levels // 2))
    most = rows * max(size for _, size in chunks)
    tiles = RADIX // 2
    dims = (rows, levels, nlon, nlat)
    f32, bf16 = jnp.float32, jnp.bfloat16
    vmem, smem, dma = pltpu.VMEM, pltpu.SMEM, pltpu.SemaphoreType.DMA
    operands = (height, zonal, merid, rates, thresholds, flags, cutoffs, scalars, ksq, fwd, inv)
    operands = [pltpu.with_memory_space_constraint(jnp.asarray(a), pltpu.HBM) for a in operands]
    return pl.pallas_call(
        functools.partial(kernel, dims, nlon * cos_sum, chunks),
        out_shape=vmem(height.shape, f32),
        in_specs=[pl.BlockSpec(memory_space=pltpu.HBM)] * len(operands),
        out_specs=pl.BlockSpec(memory_space=vmem),
        scratch_shapes=[
            vmem(height.shape, f32), vmem(height.shape, f32), vmem(height.shape, f32),
            smem(rates.shape, f32), smem(thresholds.shape, f32), smem(flags.shape, jnp.int32),
            smem(cutoffs.shape, jnp.int32), smem(scalars.shape, f32),
            vmem(ksq.shape, f32), vmem(fwd.shape, bf16), vmem(inv.shape, bf16),
            vmem((2, 2, levels, nlon), f32), vmem((2, levels, nlon), f32), vmem(height.shape, f32),
            vmem((levels, nlon), f32), vmem((levels, nlon), f32), vmem((rows, 8, 2 * HALF), f32),
            vmem((tiles, 2 * most, 2 * HALF), bf16), vmem((tiles, most, 2 * HALF), f32),
            vmem((8, HALF), f32), vmem((NX * NC, 8, HALF), f32), vmem((8, HALF), f32), vmem((NY, 8, HALF), f32),
            vmem((8, HALF), f32), vmem((8, HALF), f32),
            dma((11,)), dma((len(chunks), 2, 2)), dma((len(chunks), 2, 2)),
            dma, dma((NX * NC,)), dma((NY,)), dma((NY,)), dma((NX * NC,)), dma,
            pltpu.SemaphoreType.REGULAR, pltpu.SemaphoreType.REGULAR((NY - 1,)),
        ],
        compiler_params=pltpu.CompilerParams(collective_id=0, has_side_effects=True, vmem_limit_bytes=16 * 2**20),
        name="advect_filter",
    )(*operands)


def solution(mesh):
    finer = Mesh(
        mesh.devices.reshape(mesh.shape["member"], NX, NY, NC), ("member", "lat_0", "lat_1", "lat_2")
    )
    whole = P(("member", "lat_0", "lat_1", "lat_2"), None, None)
    placed = (whole, whole, whole, P("member"), P("member"), P(), P())
    return jax.shard_map(local, mesh=finer, in_specs=placed, out_specs=whole, check_vma=False)
```

```python
import functools
import math

import jax
import jax.numpy as jnp
import numpy as np
from jax import lax
from jax.experimental import pallas as pl
from jax.experimental.pallas import tpu as pltpu
from jax.sharding import Mesh
from jax.sharding import PartitionSpec as P

MESH = pl.DeviceIdType.MESH
NX, NY, NC = 8, 8, 2
RADIX = 12
HALF = 128
ROOT = math.sqrt(0.75)


def filter_tables(nlon):
    count = nlon // RADIX
    tiles = RADIX // 2
    fwd = np.zeros((tiles, 2 * HALF, 2 * HALF))
    inv = np.zeros((tiles, 2 * HALF, 2 * HALF))
    waves = np.zeros((8, 2 * HALF), np.int64)
    r = np.arange(count)

    def trig(k):
        angle = 2.0 * np.pi / nlon * ((r * k) % nlon)
        return np.cos(angle), np.sin(angle)

    def real_part(base, shift):
        lane = base
        for q in range(count // 2 + 1):
            k = RADIX * q + shift
            if k > nlon // 2:
                continue
            cos, sin = trig(k)
            weight = (1.0 if k in (0, nlon // 2) else 2.0) / nlon
            rows = slice(base, base + count)
            fwd[0, rows, lane] = cos
            inv[0, lane, rows] = cos * weight
            waves[0, lane] = k
            lane += 1
            if k not in (0, nlon // 2):
                fwd[0, rows, lane] = sin
                inv[0, lane, rows] = sin * weight
                waves[0, lane] = k
                lane += 1
        assert lane == base + count

    real_part(0, 0)
    real_part(HALF, RADIX // 2)
    for m in range(1, tiles):
        for q in range(count):
            k = RADIX * q + m
            cos, sin = trig(k)
            fwd[m, 0:count, q] = cos
            fwd[m, HALF : HALF + count, q] = -sin
            fwd[m, 0:count, HALF + q] = sin
            fwd[m, HALF : HALF + count, HALF + q] = cos
            waves[m, q] = waves[m, HALF + q] = min(k, nlon - k)
        inv[m] = fwd[m].T * (2.0 / nlon)
    inv_square = 1.0 / np.maximum(waves, 1).astype(np.float64) ** 2

    def halves(table):
        hi = table.astype(np.float32).astype(jnp.bfloat16)
        lo = (table - hi.astype(np.float64)).astype(np.float32).astype(jnp.bfloat16)
        return np.stack([hi, lo])

    return halves(fwd), halves(inv), inv_square.astype(np.float32)


def row_scalars(nlat):
    rows = np.arange(nlat)
    cos_row = np.sin(np.pi * (rows + 0.5) / nlat)
    faces = np.arange(nlat + 1)
    cos_face = np.where((faces > 0) & (faces < nlat), np.sin(np.pi * faces / nlat), 0.0)
    table = np.zeros((3 * nlat + HALF,))
    table[0:nlat] = cos_row
    table[nlat : 2 * nlat] = 1.0 / cos_row
    table[2 * nlat : 3 * nlat + 1] = cos_face / 24.0
    return table.astype(np.float32), float(np.sum(cos_row))


def twelve(e, o):
    plus, minus = e[0] + e[6], e[0] - e[6]
    e15p, e15m, e24p, e24m = e[1] + e[5], e[1] - e[5], e[2] + e[4], e[2] - e[4]
    a, b = plus + e24p, e15p + e[3]
    big, mid = ROOT * e15m, minus + 0.5 * e24m
    c, d = plus - 0.5 * e24p, 0.5 * e15p - e[3]
    even = [a + b, mid + big, c + d, minus - e24m, c - d, mid - big, a - b]
    o15p, o15m, o24p, o24m = o[0] + o[4], o[0] - o[4], o[1] + o[3], o[1] - o[3]
    f, g = 0.5 * o15p + o[2], ROOT * o24p
    s, t = ROOT * o15m, ROOT * o24m
    odd = [f + g, s + t, o15p - o[2], s - t, f - g]
    return even, odd


def split(x):
    hi = x.astype(jnp.bfloat16)
    return hi, (x - hi.astype(jnp.float32)).astype(jnp.bfloat16)


def kernel(
    dims, area,
    h_hbm, z_hbm, c_hbm, rates_hbm, thr_hbm, flags_hbm, cut_hbm, scal_hbm, ksq_hbm, fwd_hbm, inv_hbm,
    out,
    h, z, c, rates, thr, flags, cut, scal, ksq, fwd, inv,
    halo_h, halo_c, base, s_lo, s_hi, factor, ymat, wmat, part, xbuf, ysum, ybuf,
    mean, mean_in,
    in_sem, halo_send, halo_recv, x_send, x_recv, y_send, y_recv, mean_send, mean_recv, low_in, below_in, above_in,
):
    rows, levels, nlon, nlat = dims
    count = nlon // RADIX
    x, y, core = lax.axis_index("lat_0"), lax.axis_index("lat_1"), lax.axis_index("lat_2")
    position = (x * NY + y) * NC + core
    total = NX * NY * NC

    pairs = [(h_hbm.at[r], h.at[r]) for r in range(rows)]
    pairs += [(rates_hbm, rates), (thr_hbm, thr), (scal_hbm, scal), (c_hbm, c), (z_hbm, z)]
    pairs += [(flags_hbm, flags), (cut_hbm, cut), (ksq_hbm, ksq), (fwd_hbm, fwd), (inv_hbm, inv)]
    local = [pltpu.make_async_copy(src, dst, in_sem.at[i]) for i, (src, dst) in enumerate(pairs)]
    h_in, small_in, c_in, z_in, rest_in = local[0:4], local[4:7], local[7], local[8], local[9:]
    for copy in h_in + small_in + [c_in]:
        copy.start()

    last = total - 1
    first = position * rows
    is_root = jnp.logical_and(x == 0, core == 1)

    def along(step):
        p = lax.rem(position + total + step, total)
        return {"lat_0": p // (NY * NC), "lat_1": lax.rem(p // NC, NY), "lat_2": lax.rem(p, NC)}

    def row(k):
        return {"lat_0": jnp.int32(k // NC), "lat_1": y, "lat_2": jnp.int32(k % NC)}

    def column(d):
        return {"lat_0": jnp.int32(0), "lat_1": y + d, "lat_2": jnp.int32(1)}

    def signal(sem, device):
        pl.semaphore_signal(sem, inc=1, device_id=device, device_id_type=MESH)

    barrier = pltpu.get_barrier_semaphore()

    @pl.when(position > 0)
    def _():
        signal(barrier, along(-1))

    @pl.when(is_root)
    def _():
        for k in range(NX * NC):
            if k != 1:
                signal(barrier, row(k))

        @pl.when(y > 0)
        def _():
            signal(barrier, column(-1))

    greeted = jnp.where(is_root, jnp.where(y < NY - 1, 1, 0), 1) + jnp.where(position < last, 1, 0)
    pl.semaphore_wait(barrier, greeted)

    @pl.when(position < last)
    def _():
        signal(low_in, along(1))

    @pl.when(is_root)
    def _():
        @pl.when(y > 0)
        def _():
            pl.semaphore_wait(below_in, 1)

        @pl.when(y < NY - 1)
        def _():
            signal(below_in, column(1))

        @pl.when(y == NY - 1)
        def _():
            signal(above_in, column(-1))


    def halo_copy(side, field):
        step, h_row, c_row = ((1, rows - 2, rows - 1), (-1, 0, 0))[side]
        src = (h.at[pl.ds(h_row, 2)], c.at[c_row])[field]
        dst = (halo_h.at[side], halo_c.at[side])[field]
        return pltpu.make_async_remote_copy(
            src, dst, halo_send.at[side, field], halo_recv.at[side, field], device_id=along(step), device_id_type=MESH
        )

    base[:, :, nlon:] = jnp.zeros((rows, levels, base.shape[2] - nlon), jnp.float32)

    @pl.when(position == 0)
    def _():
        halo_h[0] = jnp.zeros_like(halo_h[0])
        halo_c[0] = jnp.zeros_like(halo_c[0])

    @pl.when(position == last)
    def _():
        halo_h[1] = jnp.zeros_like(halo_h[1])
        halo_c[1] = jnp.zeros_like(halo_c[1])

    for copy in small_in + h_in:
        copy.wait()

    @pl.when(core == 0)
    def _():
        halo_copy(0, 0).start()

    lane = lax.broadcasted_iota(jnp.int32, (8, HALF), 1)
    tile = jnp.zeros((8, HALF), jnp.float32)
    sub = lax.broadcasted_iota(jnp.int32, (8, 1), 0)

    def levels_of(ref, start):
        value = jnp.zeros((8, 1), jnp.float32)
        for k in range(8):
            value = jnp.where(sub == k, ref[start + k], value)
        return value

    for g in range(levels // 8):
        lev = pl.ds(8 * g, 8)
        rate, threshold = levels_of(rates, 8 * g), levels_of(thr, 8 * g)
        sums = jnp.zeros((8, 1), jnp.float32)
        for r in range(rows):
            height = h[r, lev, :]
            s = height - threshold
            source = -rate * (jnp.maximum(s, 0.0) + jnp.log(1.0 + jnp.exp(-jnp.abs(s))))
            base[r, lev, 0:nlon] = height + source
            sums = sums + scal[first + r] * jnp.sum(source, axis=1, keepdims=True)
        tile = jnp.where(lane == g, sums, tile)
    part[...] = tile

    def part_copy(slot):
        return pltpu.make_async_remote_copy(
            part, xbuf.at[slot], x_send, x_recv.at[slot], device_id=row(1), device_id_type=MESH
        )

    @pl.when(jnp.logical_not(is_root))
    def _():
        part_copy(x * NC + core).start()

    for copy in [z_in] + rest_in:
        copy.start()
    c_in.wait()

    @pl.when(jnp.logical_and(core != 0, position < last))
    def _():
        halo_copy(0, 0).start()

    @pl.when(position < last)
    def _():
        halo_copy(0, 1).start()

    z_in.wait()

    def inv_cos(r):
        return scal[nlat + first + r]

    def face(f):
        return scal[2 * nlat + first + f]

    def west(a):
        return pltpu.roll(a, 1, axis=1)

    def east(a):
        return pltpu.roll(a, nlon - 1, axis=1)

    def local_terms(g, carry):
        lev = pl.ds(pl.multiple_of(8 * g, 8), 8)
        hr = [h[r, lev, :] for r in range(rows)]
        cr = [c[r, lev, :] for r in range(rows)]
        low = face(1) * (cr[0] + cr[1])
        high = face(3) * (cr[2] + cr[3])
        s_lo[lev, :] = low
        s_hi[lev, :] = high
        f1 = low * (7.0 * (hr[0] + hr[1]) - hr[2])
        f2 = face(2) * (cr[1] + cr[2]) * (7.0 * (hr[1] + hr[2]) - (hr[0] + hr[3]))
        f3 = high * (7.0 * (hr[2] + hr[3]) - hr[1])
        terms = [f1, f2 - f1, f3 - f2, -f3]
        for r in range(rows):
            pair = hr[r] + east(hr[r])
            zr = z[r, lev, :]
            speed = zr + east(zr)
            flux = speed * (8.0 * pair - (west(pair) + east(pair))) * (1.0 / 24.0)
            base[r, lev, 0:nlon] = base[r, lev, 0:nlon] - (flux - west(flux)) - terms[r] * inv_cos(r)
        return carry

    lax.fori_loop(0, levels // 8, local_terms, 0)

    @pl.when(position > 0)
    def _():
        pl.semaphore_wait(low_in, 1)
        halo_copy(1, 0).start()
        halo_copy(1, 1).start()

    for copy in rest_in[0:3]:
        copy.wait()
    for r in range(rows):
        cutoff = cut[first + r].astype(jnp.float32)
        flag = flags[first + r].astype(jnp.float32)
        factor[r] = flag * (1.0 - jnp.minimum(1.0, cutoff * cutoff * ksq[...]))

    def landed(ref, sem):
        pltpu.make_async_copy(ref, ref, sem).wait()

    def sum_copy(d):
        return pltpu.make_async_remote_copy(
            ysum, ybuf.at[y], y_send.at[y + d], y_recv.at[y], device_id=column(d), device_id_type=MESH
        )

    def mean_copy(k):
        return pltpu.make_async_remote_copy(
            mean, mean_in, mean_send.at[k], mean_recv, device_id=row(k), device_id_type=MESH
        )

    def gather_row():
        for k in range(NX * NC):
            if k != 1:
                landed(xbuf.at[k], x_recv.at[k])
        acc = part[...]
        for k in range(NX * NC):
            if k != 1:
                acc = acc + xbuf[k]
        ysum[...] = acc
        for d in range(1, NY):
            for step, used in ((d, y + d < NY), (-d, y >= d)):

                @pl.when(used)
                def _():
                    sum_copy(step).start()

    def spread_mean():
        for k in range(NY):

            @pl.when(y != k)
            def _():
                landed(ybuf.at[k], y_recv.at[k])

        acc = ysum[...]
        for k in range(NY):
            acc = acc + jnp.where(y != k, ybuf[k], 0.0)
        mean[...] = acc * (1.0 / area)
        for k in range(NX * NC):
            if k != 1:
                mean_copy(k).start()
        mean_in[...] = acc * (1.0 / area)

    @pl.when(is_root)
    def _():
        @pl.when(y < NY - 1)
        def _():
            pl.semaphore_wait(above_in, 1)

            @pl.when(y > 0)
            def _():
                signal(above_in, column(-1))

        @pl.when(y > 0)
        def _():
            gather_row()

    for copy in rest_in[3:]:
        copy.wait()
    lanes = lax.broadcasted_iota(jnp.int32, (16, HALF), 1)
    units = 2 * levels
    blocks = levels // 16

    def edges_above(g, carry):
        lev = pl.ds(pl.multiple_of(8 * g, 8), 8)
        above, above2 = halo_h[1, 0, lev, :], halo_h[1, 1, lev, :]
        t3 = s_hi[lev, :] * above
        f4 = face(4) * (halo_c[1, lev, :] + c[3, lev, :]) * (7.0 * (above + h[3, lev, :]) - (above2 + h[2, lev, :]))
        base[2, lev, 0:nlon] = base[2, lev, 0:nlon] + t3 * inv_cos(2)
        base[3, lev, 0:nlon] = base[3, lev, 0:nlon] - (t3 + f4) * inv_cos(3)
        return carry

    def edges_below(g, carry):
        lev = pl.ds(pl.multiple_of(8 * g, 8), 8)
        below, below2 = halo_h[0, 1, lev, :], halo_h[0, 0, lev, :]
        t1 = s_lo[lev, :] * below
        f0 = face(0) * (halo_c[0, lev, :] + c[0, lev, :]) * (7.0 * (below + h[0, lev, :]) - (below2 + h[1, lev, :]))
        base[0, lev, 0:nlon] = base[0, lev, 0:nlon] + (t1 + f0) * inv_cos(0)
        base[1, lev, 0:nlon] = base[1, lev, 0:nlon] - t1 * inv_cos(1)
        return carry

    def product(hilo, table):
        first_part = jnp.dot(hilo, table[0], preferred_element_type=jnp.float32)
        second = jnp.dot(hilo[0:units], table[1], preferred_element_type=jnp.float32)
        return first_part[0:units] + first_part[units : 2 * units] + second

    def filter_rows(row0):
        def block_of(b):
            lev = pl.ds(pl.multiple_of(16 * lax.rem(b, blocks), 16), 16)
            at_hi, at_lo = pl.multiple_of(16 * b, 16), pl.multiple_of(units + 16 * b, 16)
            return row0 + b // blocks, lev, pl.ds(at_hi, 16), pl.ds(at_lo, 16)

        def forward(b, carry):
            r, lev, at_hi, at_lo = block_of(b)
            v = [base[r, lev, HALF * j : HALF * (j + 1)] for j in range(RADIX)]
            u = [v[0]] + [
                pltpu.roll(jnp.where(lanes >= HALF - 8 * j, v[j - 1], v[j]), 8 * j, axis=1) for j in range(1, RADIX)
            ]
            e = [u[0]] + [u[j] + u[RADIX - j] for j in range(1, 6)] + [u[6]]
            o = [u[j] - u[RADIX - j] for j in range(1, 6)]
            even, odd = twelve(e, o)
            halves = [(even[0], even[6])] + [(even[m], odd[m - 1]) for m in range(1, 6)]
            for m, pair in enumerate(halves):
                for k, value in enumerate(pair):
                    hi, lo = split(value)
                    ymat[m, at_hi, HALF * k : HALF * (k + 1)] = hi
                    ymat[m, at_lo, HALF * k : HALF * (k + 1)] = lo
            return carry

        def backward(b, carry):
            r, lev, at, _ = block_of(b)
            w = [[wmat[m, at, HALF * k : HALF * (k + 1)] for k in range(2)] for m in range(RADIX // 2)]
            even, odd = twelve([w[0][0]] + [w[m][0] for m in range(1, 6)] + [w[0][1]], [w[m][1] for m in range(1, 6)])
            removed = [even[0]] + [even[j] + odd[j - 1] for j in range(1, 6)] + [even[6]]
            removed += [even[RADIX - j] - odd[RADIX - j - 1] for j in range(7, RADIX)]
            back = [removed[0]] + [pltpu.roll(removed[j], HALF - 8 * j, axis=1) for j in range(1, RADIX)]
            for j in range(RADIX):
                if j < RADIX - 1:
                    piece = jnp.where(lanes < count - 8 * j, back[j], back[j + 1])
                    out[r, lev, HALF * j : HALF * (j + 1)] = base[r, lev, HALF * j : HALF * (j + 1)] - piece
                else:
                    left = base[r, lev, HALF * j : HALF * (j + 1)] - back[j]
                    out[r, lev, HALF * j : nlon] = left[:, 0 : nlon - HALF * j]
            return carry

        lax.fori_loop(0, 2 * blocks, forward, 0)
        for m in range(RADIX // 2):
            waves = product(ymat[m], (fwd[0, m], fwd[1, m]))
            scaled = jnp.concatenate(
                [waves[r * levels : (r + 1) * levels] * factor[row0 + r, m : m + 1, :] for r in range(2)], axis=0
            )
            wmat[m] = product(jnp.concatenate(split(scaled), axis=0), (inv[0, m], inv[1, m]))
        lax.fori_loop(0, 2 * blocks, backward, 0)

    @pl.when(position < last)
    def _():
        halo_copy(1, 0).wait_recv()
        halo_copy(1, 1).wait_recv()

    lax.fori_loop(0, levels // 8, edges_above, 0)
    filter_rows(2)

    @pl.when(jnp.logical_and(is_root, y == 0))
    def _():
        gather_row()
        spread_mean()

    @pl.when(position > 0)
    def _():
        halo_copy(0, 0).wait_recv()
        halo_copy(0, 1).wait_recv()

    lax.fori_loop(0, levels // 8, edges_below, 0)
    filter_rows(0)

    @pl.when(jnp.logical_and(is_root, y > 0))
    def _():
        spread_mean()

    @pl.when(jnp.logical_not(is_root))
    def _():
        mean_copy(0).wait_recv()

    for g in range(levels // 8):
        lev = pl.ds(8 * g, 8)
        shift = jnp.sum(jnp.where(lane == g, mean_in[...], 0.0), axis=1, keepdims=True)
        for r in range(rows):
            out[r, lev, :] = out[r, lev, :] - shift

    for side, sender in ((0, position < last), (1, position > 0)):

        @pl.when(sender)
        def _():
            halo_copy(side, 0).wait_send()
            halo_copy(side, 1).wait_send()

    @pl.when(is_root)
    def _():
        for d in range(1, NY):
            for step, used in ((d, y + d < NY), (-d, y >= d)):

                @pl.when(used)
                def _():
                    sum_copy(step).wait_send()

        for k in range(NX * NC):
            if k != 1:
                mean_copy(k).wait_send()

    @pl.when(jnp.logical_not(is_root))
    def _():
        part_copy(x * NC + core).wait_send()


def local(height, zonal, merid, rates, thresholds, flags, cutoffs):
    rows, levels, nlon = height.shape
    nlat = rows * NX * NY * NC
    fwd, inv, ksq = filter_tables(nlon)
    scalars, cos_sum = row_scalars(nlat)
    tiles = RADIX // 2
    dims = (rows, levels, nlon, nlat)
    f32, bf16 = jnp.float32, jnp.bfloat16
    vmem, smem, dma = pltpu.VMEM, pltpu.SMEM, pltpu.SemaphoreType.DMA
    operands = (height, zonal, merid, rates, thresholds, flags, cutoffs, scalars, ksq, fwd, inv)
    operands = [pltpu.with_memory_space_constraint(jnp.asarray(a), pltpu.HBM) for a in operands]
    return pl.pallas_call(
        functools.partial(kernel, dims, nlon * cos_sum),
        out_shape=vmem(height.shape, f32),
        in_specs=[pl.BlockSpec(memory_space=pltpu.HBM)] * len(operands),
        out_specs=pl.BlockSpec(memory_space=vmem),
        scratch_shapes=[
            vmem(height.shape, f32), vmem(height.shape, f32), vmem(height.shape, f32),
            smem(rates.shape, f32), smem(thresholds.shape, f32), smem(flags.shape, jnp.int32),
            smem(cutoffs.shape, jnp.int32), smem(scalars.shape, f32),
            vmem(ksq.shape, f32), vmem(fwd.shape, bf16), vmem(inv.shape, bf16),
            vmem((2, 2, levels, nlon), f32), vmem((2, levels, nlon), f32), vmem((rows, levels, RADIX * HALF), f32),
            vmem((levels, nlon), f32), vmem((levels, nlon), f32), vmem((rows, 8, 2 * HALF), f32),
            vmem((tiles, 4 * levels, 2 * HALF), bf16), vmem((tiles, 2 * levels, 2 * HALF), f32),
            vmem((8, HALF), f32), vmem((NX * NC, 8, HALF), f32), vmem((8, HALF), f32), vmem((NY, 8, HALF), f32),
            vmem((8, HALF), f32), vmem((8, HALF), f32),
            dma((14,)), dma((2, 2)), dma((2, 2)),
            dma, dma((NX * NC,)), dma((NY,)), dma((NY,)), dma((NX * NC,)), dma,
            *[pltpu.SemaphoreType.REGULAR] * 3,
        ],
        compiler_params=pltpu.CompilerParams(collective_id=0, has_side_effects=True, vmem_limit_bytes=16 * 2**20),
        name="advect_filter",
    )(*operands)


def solution(mesh):
    finer = Mesh(
        mesh.devices.reshape(mesh.shape["member"], NX, NY, NC), ("member", "lat_0", "lat_1", "lat_2")
    )
    whole = P(("member", "lat_0", "lat_1", "lat_2"), None, None)
    placed = (whole, whole, whole, P("member"), P("member"), P(), P())
    return jax.shard_map(local, mesh=finer, in_specs=placed, out_specs=whole, check_vma=False)
```

```python
import functools
import math

import jax
import jax.numpy as jnp
import numpy as np
from jax import lax
from jax.experimental import pallas as pl
from jax.experimental.pallas import tpu as pltpu
from jax.sharding import Mesh
from jax.sharding import PartitionSpec as P

MESH = pl.DeviceIdType.MESH
NX, NY, NC = 8, 8, 2
RADIX = 12
HALF = 128
ROOT = math.sqrt(0.75)


def filter_tables(nlon):
    count = nlon // RADIX
    tiles = RADIX // 2
    fwd = np.zeros((tiles, 2 * HALF, 2 * HALF))
    inv = np.zeros((tiles, 2 * HALF, 2 * HALF))
    waves = np.zeros((8, 2 * HALF), np.int64)
    r = np.arange(count)

    def trig(k):
        angle = 2.0 * np.pi / nlon * ((r * k) % nlon)
        return np.cos(angle), np.sin(angle)

    def real_part(base, shift):
        lane = base
        for q in range(count // 2 + 1):
            k = RADIX * q + shift
            if k > nlon // 2:
                continue
            cos, sin = trig(k)
            weight = (1.0 if k in (0, nlon // 2) else 2.0) / nlon
            rows = slice(base, base + count)
            fwd[0, rows, lane] = cos
            inv[0, lane, rows] = cos * weight
            waves[0, lane] = k
            lane += 1
            if k not in (0, nlon // 2):
                fwd[0, rows, lane] = sin
                inv[0, lane, rows] = sin * weight
                waves[0, lane] = k
                lane += 1
        assert lane == base + count

    real_part(0, 0)
    real_part(HALF, RADIX // 2)
    for m in range(1, tiles):
        for q in range(count):
            k = RADIX * q + m
            cos, sin = trig(k)
            fwd[m, 0:count, q] = cos
            fwd[m, HALF : HALF + count, q] = -sin
            fwd[m, 0:count, HALF + q] = sin
            fwd[m, HALF : HALF + count, HALF + q] = cos
            waves[m, q] = waves[m, HALF + q] = min(k, nlon - k)
        inv[m] = fwd[m].T * (2.0 / nlon)
    inv_square = 1.0 / np.maximum(waves, 1).astype(np.float64) ** 2

    def halves(table):
        hi = table.astype(np.float32).astype(jnp.bfloat16)
        lo = (table - hi.astype(np.float64)).astype(np.float32).astype(jnp.bfloat16)
        return np.stack([hi, lo])

    return halves(fwd), halves(inv), inv_square.astype(np.float32)


def row_scalars(nlat):
    rows = np.arange(nlat)
    cos_row = np.sin(np.pi * (rows + 0.5) / nlat)
    faces = np.arange(nlat + 1)
    cos_face = np.where((faces > 0) & (faces < nlat), np.sin(np.pi * faces / nlat), 0.0)
    table = np.zeros((3 * nlat + HALF,))
    table[0:nlat] = cos_row
    table[nlat : 2 * nlat] = 1.0 / cos_row
    table[2 * nlat : 3 * nlat + 1] = cos_face / 24.0
    return table.astype(np.float32), float(np.sum(cos_row))


def twelve(e, o):
    plus, minus = e[0] + e[6], e[0] - e[6]
    e15p, e15m, e24p, e24m = e[1] + e[5], e[1] - e[5], e[2] + e[4], e[2] - e[4]
    a, b = plus + e24p, e15p + e[3]
    big, mid = ROOT * e15m, minus + 0.5 * e24m
    c, d = plus - 0.5 * e24p, 0.5 * e15p - e[3]
    even = [a + b, mid + big, c + d, minus - e24m, c - d, mid - big, a - b]
    o15p, o15m, o24p, o24m = o[0] + o[4], o[0] - o[4], o[1] + o[3], o[1] - o[3]
    f, g = 0.5 * o15p + o[2], ROOT * o24p
    s, t = ROOT * o15m, ROOT * o24m
    odd = [f + g, s + t, o15p - o[2], s - t, f - g]
    return even, odd


def split(x):
    hi = x.astype(jnp.bfloat16)
    return hi, (x - hi.astype(jnp.float32)).astype(jnp.bfloat16)


def kernel(
    dims, area,
    h_hbm, z_hbm, c_hbm, rates_hbm, thr_hbm, flags_hbm, cut_hbm, scal_hbm, ksq_hbm, fwd_hbm, inv_hbm,
    out,
    h, z, c, rates, thr, flags, cut, scal, ksq, fwd, inv,
    halo_h, halo_c, base, s_lo, s_hi, factor, ymat, wmat, part, xbuf, ysum, ybuf,
    mean_in, level_rates, level_thresholds,
    in_sem, halo_send, halo_recv, x_send, x_recv, y_send, y_recv, mean_send, mean_recv, low_in,
):
    rows, levels, nlon, nlat = dims
    count = nlon // RADIX
    x, y, core = lax.axis_index("lat_0"), lax.axis_index("lat_1"), lax.axis_index("lat_2")
    position = (x * NY + y) * NC + core
    total = NX * NY * NC

    pairs = [(h_hbm.at[r], h.at[r]) for r in range(rows)]
    pairs += [(rates_hbm, rates), (thr_hbm, thr), (scal_hbm, scal), (c_hbm, c), (z_hbm, z)]
    pairs += [(flags_hbm, flags), (cut_hbm, cut), (ksq_hbm, ksq), (fwd_hbm, fwd), (inv_hbm, inv)]
    local = [pltpu.make_async_copy(src, dst, in_sem.at[i]) for i, (src, dst) in enumerate(pairs)]
    h_in, small_in, c_in, z_in, rest_in = local[0:4], local[4:7], local[7], local[8], local[9:]
    for copy in h_in + small_in + [c_in]:
        copy.start()

    last = total - 1
    first = position * rows
    is_root = jnp.logical_and(x == 0, core == 1)
    is_first = position == 1
    is_later_root = jnp.logical_and(is_root, y > 0)

    def along(step):
        p = lax.rem(position + total + step, total)
        return {"lat_0": p // (NY * NC), "lat_1": lax.rem(p // NC, NY), "lat_2": lax.rem(p, NC)}

    def row(k):
        return {"lat_0": jnp.int32(k // NC), "lat_1": y, "lat_2": jnp.int32(k % NC)}

    def root(k):
        return {"lat_0": jnp.int32(0), "lat_1": jnp.int32(k), "lat_2": jnp.int32(1)}

    def signal(sem, device):
        pl.semaphore_signal(sem, inc=1, device_id=device, device_id_type=MESH)

    barrier = pltpu.get_barrier_semaphore()

    @pl.when(position > 0)
    def _():
        signal(barrier, along(-1))

    @pl.when(is_root)
    def _():
        for k in range(NX * NC):
            if k != 1:
                signal(barrier, row(k))

    @pl.when(is_first)
    def _():
        for k in range(1, NY):
            signal(barrier, root(k))

    greeted = jnp.where(is_first, 0, 1) + jnp.where(position < last, 1, 0)
    pl.semaphore_wait(barrier, greeted)

    @pl.when(position < last)
    def _():
        signal(low_in, along(1))

    def halo_copy(side, field):
        step, h_row, c_row = ((1, rows - 2, rows - 1), (-1, 0, 0))[side]
        src = (h.at[pl.ds(h_row, 2)], c.at[c_row])[field]
        dst = (halo_h.at[side], halo_c.at[side])[field]
        return pltpu.make_async_remote_copy(
            src, dst, halo_send.at[side, field], halo_recv.at[side, field], device_id=along(step), device_id_type=MESH
        )

    base[:, :, nlon:] = jnp.zeros((rows, levels, base.shape[2] - nlon), jnp.float32)

    @pl.when(position == 0)
    def _():
        halo_h[0] = jnp.zeros_like(halo_h[0])
        halo_c[0] = jnp.zeros_like(halo_c[0])

    @pl.when(position == last)
    def _():
        halo_h[1] = jnp.zeros_like(halo_h[1])
        halo_c[1] = jnp.zeros_like(halo_c[1])

    for copy in small_in + h_in:
        copy.wait()

    @pl.when(core == 0)
    def _():
        halo_copy(0, 0).start()

    lane = lax.broadcasted_iota(jnp.int32, (8, HALF), 1)
    tile = jnp.zeros((8, HALF), jnp.float32)
    sub = lax.broadcasted_iota(jnp.int32, (8, 1), 0)

    def levels_of(ref, start):
        value = jnp.zeros((8, 1), jnp.float32)
        for k in range(8):
            value = jnp.where(sub == k, ref[start + k], value)
        return value

    full = nlon // HALF
    for g in range(levels // 8):
        lev = pl.ds(8 * g, 8)
        rate, threshold = levels_of(rates, 8 * g), levels_of(thr, 8 * g)
        wide, rest = 0.0, 0.0
        for r in range(rows):
            positive, factors = 0.0, 1.0
            for j in range(full):
                s = h[r, lev, HALF * j : HALF * (j + 1)] - threshold
                positive = positive + jnp.maximum(s, 0.0)
                factors = factors * (1.0 + jnp.exp(-jnp.abs(s)))
            s = h[r, lev, HALF * full : nlon] - threshold
            wide = wide + scal[first + r] * (positive + jnp.log(factors))
            rest = rest + scal[first + r] * (jnp.maximum(s, 0.0) + jnp.log(1.0 + jnp.exp(-jnp.abs(s))))
        sums = jnp.sum(wide, axis=1, keepdims=True) + jnp.sum(rest, axis=1, keepdims=True)
        tile = jnp.where(lane == g, -rate * sums, tile)
        level_rates[g], level_thresholds[g] = jnp.broadcast_to(rate, (8, HALF)), jnp.broadcast_to(threshold, (8, HALF))
    part[...] = tile

    def part_copy(slot):
        return pltpu.make_async_remote_copy(
            part, xbuf.at[slot], x_send, x_recv.at[slot], device_id=row(1), device_id_type=MESH
        )

    @pl.when(jnp.logical_not(is_root))
    def _():
        part_copy(x * NC + core).start()

    for copy in [z_in] + rest_in:
        copy.start()
    c_in.wait()

    @pl.when(jnp.logical_and(core != 0, position < last))
    def _():
        halo_copy(0, 0).start()

    @pl.when(position < last)
    def _():
        halo_copy(0, 1).start()

    z_in.wait()

    def inv_cos(r):
        return scal[nlat + first + r]

    def face(f):
        return scal[2 * nlat + first + f]

    def west(a):
        return pltpu.roll(a, 1, axis=1)

    def east(a):
        return pltpu.roll(a, nlon - 1, axis=1)

    def local_terms(g, carry):
        lev = pl.ds(pl.multiple_of(8 * g, 8), 8)
        hr = [h[r, lev, :] for r in range(rows)]
        rate, threshold = level_rates[g][:, 0:1], level_thresholds[g][:, 0:1]
        cr = [c[r, lev, :] for r in range(rows)]
        low = face(1) * (cr[0] + cr[1])
        high = face(3) * (cr[2] + cr[3])
        s_lo[lev, :] = low
        s_hi[lev, :] = high
        f1 = low * (7.0 * (hr[0] + hr[1]) - hr[2])
        f2 = face(2) * (cr[1] + cr[2]) * (7.0 * (hr[1] + hr[2]) - (hr[0] + hr[3]))
        f3 = high * (7.0 * (hr[2] + hr[3]) - hr[1])
        terms = [f1, f2 - f1, f3 - f2, -f3]
        for r in range(rows):
            pair = hr[r] + east(hr[r])
            zr = z[r, lev, :]
            speed = zr + east(zr)
            flux = speed * (8.0 * pair - (west(pair) + east(pair))) * (1.0 / 24.0)
            s = hr[r] - threshold
            source = rate * (jnp.maximum(s, 0.0) + jnp.log(1.0 + jnp.exp(-jnp.abs(s))))
            base[r, lev, 0:nlon] = (hr[r] - source) - (flux - west(flux)) - terms[r] * inv_cos(r)
        return carry

    lax.fori_loop(0, levels // 8, local_terms, 0)

    @pl.when(position > 0)
    def _():
        pl.semaphore_wait(low_in, 1)
        halo_copy(1, 0).start()
        halo_copy(1, 1).start()

    for copy in rest_in[0:3]:
        copy.wait()
    for r in range(rows):
        cutoff = cut[first + r].astype(jnp.float32)
        flag = flags[first + r].astype(jnp.float32)
        factor[r] = flag * (1.0 - jnp.minimum(1.0, cutoff * cutoff * ksq[...]))

    def landed(ref, sem):
        pltpu.make_async_copy(ref, ref, sem).wait()

    def sum_copy():
        return pltpu.make_async_remote_copy(
            ysum, ybuf.at[y], y_send, y_recv.at[y], device_id=root(0), device_id_type=MESH
        )

    def mean_copy(slot, device):
        return pltpu.make_async_remote_copy(
            mean_in, mean_in, mean_send.at[slot], mean_recv, device_id=device, device_id_type=MESH
        )

    members = [0] + [k for d in (4, 3, 5, 2, 6, 1, 7) for k in (NC * d, NC * d + 1)]

    def gather_row():
        for k in members:
            landed(xbuf.at[k], x_recv.at[k])
        acc = part[...]
        for k in members:
            acc = acc + xbuf[k]
        return acc

    def spread_row():
        for k in members[1:] + members[:1]:
            mean_copy(k, row(k)).start()

    @pl.when(is_later_root)
    def _():
        ysum[...] = gather_row()
        sum_copy().start()

    for copy in rest_in[3:]:
        copy.wait()
    lanes = lax.broadcasted_iota(jnp.int32, (16, HALF), 1)
    units = 2 * levels
    blocks = levels // 16

    def edges_above(g, carry):
        lev = pl.ds(pl.multiple_of(8 * g, 8), 8)
        above, above2 = halo_h[1, 0, lev, :], halo_h[1, 1, lev, :]
        t3 = s_hi[lev, :] * above
        f4 = face(4) * (halo_c[1, lev, :] + c[3, lev, :]) * (7.0 * (above + h[3, lev, :]) - (above2 + h[2, lev, :]))
        base[2, lev, 0:nlon] = base[2, lev, 0:nlon] + t3 * inv_cos(2)
        base[3, lev, 0:nlon] = base[3, lev, 0:nlon] - (t3 + f4) * inv_cos(3)
        return carry

    def edges_below(g, carry):
        lev = pl.ds(pl.multiple_of(8 * g, 8), 8)
        below, below2 = halo_h[0, 1, lev, :], halo_h[0, 0, lev, :]
        t1 = s_lo[lev, :] * below
        f0 = face(0) * (halo_c[0, lev, :] + c[0, lev, :]) * (7.0 * (below + h[0, lev, :]) - (below2 + h[1, lev, :]))
        base[0, lev, 0:nlon] = base[0, lev, 0:nlon] + (t1 + f0) * inv_cos(0)
        base[1, lev, 0:nlon] = base[1, lev, 0:nlon] - t1 * inv_cos(1)
        return carry

    def product(hilo, table):
        first_part = jnp.dot(hilo, table[0], preferred_element_type=jnp.float32)
        second = jnp.dot(hilo[0:units], table[1], preferred_element_type=jnp.float32)
        return first_part[0:units] + first_part[units : 2 * units] + second

    def filter_rows(row0):
        def block_of(b):
            return row0 + b // blocks, pl.ds(16 * (b % blocks), 16), pl.ds(16 * b, 16), pl.ds(units + 16 * b, 16)

        def forward(b):
            r, lev, at_hi, at_lo = block_of(b)
            v = [base[r, lev, HALF * j : HALF * (j + 1)] for j in range(RADIX)]
            u = [v[0]] + [
                pltpu.roll(jnp.where(lanes >= HALF - 8 * j, v[j - 1], v[j]), 8 * j, axis=1) for j in range(1, RADIX)
            ]
            e = [u[0]] + [u[j] + u[RADIX - j] for j in range(1, 6)] + [u[6]]
            o = [u[j] - u[RADIX - j] for j in range(1, 6)]
            even, odd = twelve(e, o)
            halves = [(even[0], even[6])] + [(even[m], odd[m - 1]) for m in range(1, 6)]
            for m, pair in enumerate(halves):
                for k, value in enumerate(pair):
                    hi, lo = split(value)
                    ymat[m, at_hi, HALF * k : HALF * (k + 1)] = hi
                    ymat[m, at_lo, HALF * k : HALF * (k + 1)] = lo

        def backward(b):
            r, lev, at, _ = block_of(b)
            w = [[wmat[m, at, HALF * k : HALF * (k + 1)] for k in range(2)] for m in range(RADIX // 2)]
            even, odd = twelve([w[0][0]] + [w[m][0] for m in range(1, 6)] + [w[0][1]], [w[m][1] for m in range(1, 6)])
            removed = [even[0]] + [even[j] + odd[j - 1] for j in range(1, 6)] + [even[6]]
            removed += [even[RADIX - j] - odd[RADIX - j - 1] for j in range(7, RADIX)]
            back = [removed[0]] + [pltpu.roll(removed[j], HALF - 8 * j, axis=1) for j in range(1, RADIX)]
            for j in range(RADIX):
                if j < RADIX - 1:
                    piece = jnp.where(lanes < count - 8 * j, back[j], back[j + 1])
                    out[r, lev, HALF * j : HALF * (j + 1)] = base[r, lev, HALF * j : HALF * (j + 1)] - piece
                else:
                    left = base[r, lev, HALF * j : HALF * (j + 1)] - back[j]
                    out[r, lev, HALF * j : nlon] = left[:, 0 : nlon - HALF * j]

        for b in range(2 * blocks):
            forward(b)
        for m in range(RADIX // 2):
            waves = product(ymat[m], (fwd[0, m], fwd[1, m]))
            scaled = jnp.concatenate(
                [waves[r * levels : (r + 1) * levels] * factor[row0 + r, m : m + 1, :] for r in range(2)], axis=0
            )
            wmat[m] = product(jnp.concatenate(split(scaled), axis=0), (inv[0, m], inv[1, m]))
        for b in range(2 * blocks):
            backward(b)

    @pl.when(position < last)
    def _():
        halo_copy(1, 0).wait_recv()
        halo_copy(1, 1).wait_recv()

    lax.fori_loop(0, levels // 8, edges_above, 0)
    filter_rows(2)

    @pl.when(is_first)
    def _():
        for k in range(1, NY):
            landed(ybuf.at[k], y_recv.at[k])
        acc = ybuf[1]
        for k in range(2, NY):
            acc = acc + ybuf[k]
        mean_in[...] = (gather_row() + acc) * (1.0 / area)
        spread_row()
        for k in range(1, NY):
            mean_copy(NX * NC + k, root(k)).start()

    @pl.when(position > 0)
    def _():
        halo_copy(0, 0).wait_recv()
        halo_copy(0, 1).wait_recv()

    lax.fori_loop(0, levels // 8, edges_below, 0)
    filter_rows(0)

    @pl.when(jnp.logical_not(is_first))
    def _():
        mean_copy(0, row(0)).wait_recv()

    @pl.when(is_later_root)
    def _():
        spread_row()

    for g in range(levels // 8):
        lev = pl.ds(8 * g, 8)
        shift = jnp.sum(jnp.where(lane == g, mean_in[...], 0.0), axis=1, keepdims=True)
        for r in range(rows):
            out[r, lev, :] = out[r, lev, :] - shift

    for side, sender in ((0, position < last), (1, position > 0)):

        @pl.when(sender)
        def _():
            halo_copy(side, 0).wait_send()
            halo_copy(side, 1).wait_send()

    @pl.when(is_later_root)
    def _():
        sum_copy().wait_send()

    @pl.when(is_root)
    def _():
        for k in members:
            mean_copy(k, row(k)).wait_send()

    @pl.when(is_first)
    def _():
        for k in range(1, NY):
            mean_copy(NX * NC + k, root(k)).wait_send()

    @pl.when(jnp.logical_not(is_root))
    def _():
        part_copy(x * NC + core).wait_send()


def local(height, zonal, merid, rates, thresholds, flags, cutoffs):
    rows, levels, nlon = height.shape
    nlat = rows * NX * NY * NC
    fwd, inv, ksq = filter_tables(nlon)
    scalars, cos_sum = row_scalars(nlat)
    tiles = RADIX // 2
    dims = (rows, levels, nlon, nlat)
    f32, bf16 = jnp.float32, jnp.bfloat16
    vmem, smem, dma = pltpu.VMEM, pltpu.SMEM, pltpu.SemaphoreType.DMA
    operands = (height, zonal, merid, rates, thresholds, flags, cutoffs, scalars, ksq, fwd, inv)
    operands = [pltpu.with_memory_space_constraint(jnp.asarray(a), pltpu.HBM) for a in operands]
    return pl.pallas_call(
        functools.partial(kernel, dims, nlon * cos_sum),
        out_shape=vmem(height.shape, f32),
        in_specs=[pl.BlockSpec(memory_space=pltpu.HBM)] * len(operands),
        out_specs=pl.BlockSpec(memory_space=vmem),
        scratch_shapes=[
            vmem(height.shape, f32), vmem(height.shape, f32), vmem(height.shape, f32),
            smem(rates.shape, f32), smem(thresholds.shape, f32), smem(flags.shape, jnp.int32),
            smem(cutoffs.shape, jnp.int32), smem(scalars.shape, f32),
            vmem(ksq.shape, f32), vmem(fwd.shape, bf16), vmem(inv.shape, bf16),
            vmem((2, 2, levels, nlon), f32), vmem((2, levels, nlon), f32), vmem((rows, levels, RADIX * HALF), f32),
            vmem((levels, nlon), f32), vmem((levels, nlon), f32), vmem((rows, 8, 2 * HALF), f32),
            vmem((tiles, 4 * levels, 2 * HALF), bf16), vmem((tiles, 2 * levels, 2 * HALF), f32),
            vmem((8, HALF), f32), vmem((NX * NC, 8, HALF), f32), vmem((8, HALF), f32), vmem((NY, 8, HALF), f32),
            vmem((8, HALF), f32), vmem((levels // 8, 8, HALF), f32), vmem((levels // 8, 8, HALF), f32),
            dma((14,)), dma((2, 2)), dma((2, 2)),
            dma, dma((NX * NC,)), dma, dma((NY,)), dma((NX * NC + NY,)), dma, pltpu.SemaphoreType.REGULAR,
        ],
        compiler_params=pltpu.CompilerParams(collective_id=0, has_side_effects=True, vmem_limit_bytes=16 * 2**20),
        name="advect_filter",
    )(*operands)


def solution(mesh):
    finer = Mesh(
        mesh.devices.reshape(mesh.shape["member"], NX, NY, NC), ("member", "lat_0", "lat_1", "lat_2")
    )
    whole = P(("member", "lat_0", "lat_1", "lat_2"), None, None)
    placed = (whole, whole, whole, P("member"), P("member"), P(), P())
    return jax.shard_map(local, mesh=finer, in_specs=placed, out_specs=whole, check_vma=False)
```

```python
import functools
import math

import jax
import jax.numpy as jnp
import numpy as np
from jax import lax
from jax.experimental import pallas as pl
from jax.experimental.pallas import tpu as pltpu
from jax.sharding import Mesh
from jax.sharding import PartitionSpec as P

MESH = pl.DeviceIdType.MESH
NX, NY, NC = 8, 8, 2
RADIX = 12
HALF = 128
ROOT = math.sqrt(0.75)


def filter_tables(nlon):
    count = nlon // RADIX
    tiles = RADIX // 2
    fwd = np.zeros((tiles, 2 * HALF, 2 * HALF))
    inv = np.zeros((tiles, 2 * HALF, 2 * HALF))
    waves = np.zeros((8, 2 * HALF), np.int64)
    r = np.arange(count)

    def trig(k):
        angle = 2.0 * np.pi / nlon * ((r * k) % nlon)
        return np.cos(angle), np.sin(angle)

    def real_part(base, shift):
        lane = base
        for q in range(count // 2 + 1):
            k = RADIX * q + shift
            if k > nlon // 2:
                continue
            cos, sin = trig(k)
            weight = (1.0 if k in (0, nlon // 2) else 2.0) / nlon
            rows = slice(base, base + count)
            fwd[0, rows, lane] = cos
            inv[0, lane, rows] = cos * weight
            waves[0, lane] = k
            lane += 1
            if k not in (0, nlon // 2):
                fwd[0, rows, lane] = sin
                inv[0, lane, rows] = sin * weight
                waves[0, lane] = k
                lane += 1
        assert lane == base + count

    real_part(0, 0)
    real_part(HALF, RADIX // 2)
    for m in range(1, tiles):
        for q in range(count):
            k = RADIX * q + m
            cos, sin = trig(k)
            fwd[m, 0:count, q] = cos
            fwd[m, HALF : HALF + count, q] = -sin
            fwd[m, 0:count, HALF + q] = sin
            fwd[m, HALF : HALF + count, HALF + q] = cos
            waves[m, q] = waves[m, HALF + q] = min(k, nlon - k)
        inv[m] = fwd[m].T * (2.0 / nlon)
    inv_square = 1.0 / np.maximum(waves, 1).astype(np.float64) ** 2

    def halves(table):
        hi = table.astype(np.float32).astype(jnp.bfloat16)
        lo = (table - hi.astype(np.float64)).astype(np.float32).astype(jnp.bfloat16)
        return np.stack([hi, lo])

    return halves(fwd), halves(inv), inv_square.astype(np.float32)


def row_scalars(nlat):
    rows = np.arange(nlat)
    cos_row = np.sin(np.pi * (rows + 0.5) / nlat)
    faces = np.arange(nlat + 1)
    cos_face = np.where((faces > 0) & (faces < nlat), np.sin(np.pi * faces / nlat), 0.0)
    table = np.zeros((3 * nlat + HALF,))
    table[0:nlat] = cos_row
    table[nlat : 2 * nlat] = 1.0 / cos_row
    table[2 * nlat : 3 * nlat + 1] = cos_face / 24.0
    return table.astype(np.float32), float(np.sum(cos_row))


def twelve(e, o):
    plus, minus = e[0] + e[6], e[0] - e[6]
    e15p, e15m, e24p, e24m = e[1] + e[5], e[1] - e[5], e[2] + e[4], e[2] - e[4]
    a, b = plus + e24p, e15p + e[3]
    big, mid = ROOT * e15m, minus + 0.5 * e24m
    c, d = plus - 0.5 * e24p, 0.5 * e15p - e[3]
    even = [a + b, mid + big, c + d, minus - e24m, c - d, mid - big, a - b]
    o15p, o15m, o24p, o24m = o[0] + o[4], o[0] - o[4], o[1] + o[3], o[1] - o[3]
    f, g = 0.5 * o15p + o[2], ROOT * o24p
    s, t = ROOT * o15m, ROOT * o24m
    odd = [f + g, s + t, o15p - o[2], s - t, f - g]
    return even, odd


def split(x):
    hi = x.astype(jnp.bfloat16)
    return hi, (x - hi.astype(jnp.float32)).astype(jnp.bfloat16)


def kernel(
    dims, area,
    h_hbm, z_hbm, c_hbm, rates_hbm, thr_hbm, flags_hbm, cut_hbm, scal_hbm, ksq_hbm, fwd_hbm, inv_hbm,
    out,
    h, z, c, rates, thr, flags, cut, scal, ksq, fwd, inv,
    halo, base, s_lo, s_hi, factor, ymat, wmat, part, box, mean_in, level_rates, level_thresholds,
    in_sem, halo_send, halo_recv, up_send, x_recv, y_recv, mean_send, mean_recv, low_in,
):
    rows, levels, nlon, nlat = dims
    count = nlon // RADIX
    x, y, core = lax.axis_index("lat_0"), lax.axis_index("lat_1"), lax.axis_index("lat_2")
    position = (x * NY + y) * NC + core
    total = NX * NY * NC

    order = (2, 3, 0, 1)

    def fetch(src, dst, i):
        return pltpu.make_async_copy(src, dst, in_sem.at[i])

    h_in = {r: fetch(h_hbm.at[r], h.at[r], i) for i, r in enumerate(order)}
    c_in = fetch(c_hbm, c, 4)
    small_in = [fetch(rates_hbm, rates, 5), fetch(thr_hbm, thr, 6), fetch(scal_hbm, scal, 7)]
    z_in = fetch(z_hbm, z, 0)
    tables_in = [fetch(fwd_hbm, fwd, 1), fetch(inv_hbm, inv, 2)]
    factor_in = [fetch(flags_hbm, flags, 5), fetch(cut_hbm, cut, 6), fetch(ksq_hbm, ksq, 7)]
    for copy in small_in + [h_in[r] for r in order] + [c_in]:
        copy.start()

    last = total - 1
    first = position * rows
    is_root = jnp.logical_and(x == 0, core == 1)
    is_first = position == 1
    is_later_root = jnp.logical_and(is_root, y > 0)

    def along(step):
        p = lax.rem(position + total + step, total)
        return {"lat_0": p // (NY * NC), "lat_1": lax.rem(p // NC, NY), "lat_2": lax.rem(p, NC)}

    def row(k):
        return {"lat_0": jnp.int32(k // NC), "lat_1": y, "lat_2": jnp.int32(k % NC)}

    def root(k):
        return {"lat_0": jnp.int32(0), "lat_1": jnp.int32(k), "lat_2": jnp.int32(1)}

    def signal(sem, device):
        pl.semaphore_signal(sem, inc=1, device_id=device, device_id_type=MESH)

    barrier = pltpu.get_barrier_semaphore()

    @pl.when(position > 0)
    def _():
        signal(barrier, along(-1))

    @pl.when(is_root)
    def _():
        for k in range(NX * NC):
            if k != 1:
                signal(barrier, row(k))

    @pl.when(is_first)
    def _():
        for k in range(1, NY):
            signal(barrier, root(k))

    greeted = jnp.where(is_first, 0, 1) + jnp.where(position < last, 1, 0)
    pl.semaphore_wait(barrier, greeted)

    @pl.when(position < last)
    def _():
        signal(low_in, along(1))

    def landed(ref, sem):
        pltpu.make_async_copy(ref, ref, sem).wait()

    def halo_copy(side, field):
        step, h_row, c_row = ((1, rows - 2, rows - 1), (-1, 0, 0))[side]
        src = (h.at[pl.ds(h_row, 2)], c.at[pl.ds(c_row, 1)])[field]
        dst = halo.at[side, pl.ds((0, 2)[field], (2, 1)[field])]
        return pltpu.make_async_remote_copy(
            src, dst, halo_send.at[side], halo_recv.at[side], device_id=along(step), device_id_type=MESH
        )

    base[:, :, nlon:] = jnp.zeros((rows, levels, base.shape[2] - nlon), jnp.float32)

    @pl.when(position == 0)
    def _():
        halo[0] = jnp.zeros_like(halo[0])

    @pl.when(position == last)
    def _():
        halo[1] = jnp.zeros_like(halo[1])

    for copy in small_in:
        copy.wait()

    h_in[2].wait()
    h_in[3].wait()

    @pl.when(core == 0)
    def _():
        halo_copy(0, 0).start()

    lane = lax.broadcasted_iota(jnp.int32, (8, HALF), 1)
    tile = jnp.zeros((8, HALF), jnp.float32)
    sub = lax.broadcasted_iota(jnp.int32, (8, 1), 0)

    def levels_of(ref, start):
        value = jnp.zeros((8, 1), jnp.float32)
        for k in range(8):
            value = jnp.where(sub == k, ref[start + k], value)
        return value

    full = nlon // HALF
    groups = range(levels // 8)
    rate_of = [levels_of(rates, 8 * g) for g in groups]
    threshold_of = [levels_of(thr, 8 * g) for g in groups]
    wide, rest = [0.0 for g in groups], [0.0 for g in groups]
    for r in order:
        if r < 2:
            h_in[r].wait()
        for g in groups:
            lev = pl.ds(8 * g, 8)
            positive, factors = 0.0, 1.0
            for j in range(full):
                s = h[r, lev, HALF * j : HALF * (j + 1)] - threshold_of[g]
                positive = positive + jnp.maximum(s, 0.0)
                factors = factors * (1.0 + jnp.exp(-jnp.abs(s)))
            s = h[r, lev, HALF * full : nlon] - threshold_of[g]
            wide[g] = wide[g] + scal[first + r] * (positive + jnp.log(factors))
            rest[g] = rest[g] + scal[first + r] * (jnp.maximum(s, 0.0) + jnp.log(1.0 + jnp.exp(-jnp.abs(s))))
    short = jnp.zeros((8, HALF * (full + 1) - nlon), jnp.float32)
    for g in groups:
        sums = jnp.sum(wide[g] + jnp.concatenate([rest[g], short], axis=1), axis=1, keepdims=True)
        tile = jnp.where(lane == g, -rate_of[g] * sums, tile)
        level_rates[g] = jnp.broadcast_to(rate_of[g], (8, HALF))
        level_thresholds[g] = jnp.broadcast_to(threshold_of[g], (8, HALF))
    part[...] = tile

    def part_copy(slot):
        return pltpu.make_async_remote_copy(
            part, box.at[slot], up_send, x_recv, device_id=row(1), device_id_type=MESH
        )

    @pl.when(jnp.logical_not(is_root))
    def _():
        part_copy(x * NC + core).start()

    c_in.wait()
    for copy in [z_in] + factor_in + tables_in:
        copy.start()

    @pl.when(jnp.logical_and(core != 0, position < last))
    def _():
        halo_copy(0, 0).start()

    @pl.when(position < last)
    def _():
        halo_copy(0, 1).start()

    z_in.wait()

    def inv_cos(r):
        return scal[nlat + first + r]

    def face(f):
        return scal[2 * nlat + first + f]

    def west(a):
        return pltpu.roll(a, 1, axis=1)

    def east(a):
        return pltpu.roll(a, nlon - 1, axis=1)

    def local_terms(g, carry):
        lev = pl.ds(pl.multiple_of(8 * g, 8), 8)
        hr = [h[r, lev, :] for r in range(rows)]
        rate, threshold = level_rates[g][:, 0:1], level_thresholds[g][:, 0:1]
        cr = [c[r, lev, :] for r in range(rows)]
        low = face(1) * (cr[0] + cr[1])
        high = face(3) * (cr[2] + cr[3])
        s_lo[lev, :] = low
        s_hi[lev, :] = high
        f1 = low * (7.0 * (hr[0] + hr[1]) - hr[2])
        f2 = face(2) * (cr[1] + cr[2]) * (7.0 * (hr[1] + hr[2]) - (hr[0] + hr[3]))
        f3 = high * (7.0 * (hr[2] + hr[3]) - hr[1])
        terms = [f1, f2 - f1, f3 - f2, -f3]
        for r in range(rows):
            pair = hr[r] + east(hr[r])
            zr = z[r, lev, :]
            speed = zr + east(zr)
            flux = speed * (8.0 * pair - (west(pair) + east(pair))) * (1.0 / 24.0)
            s = hr[r] - threshold
            source = rate * (jnp.maximum(s, 0.0) + jnp.log(1.0 + jnp.exp(-jnp.abs(s))))
            base[r, lev, 0:nlon] = (hr[r] - source) - (flux - west(flux)) - terms[r] * inv_cos(r)
        return carry

    lax.fori_loop(0, levels // 8, local_terms, 0)

    @pl.when(position > 0)
    def _():
        pl.semaphore_wait(low_in, 1)
        halo_copy(1, 0).start()
        halo_copy(1, 1).start()

    for copy in factor_in:
        copy.wait()
    for r in range(rows):
        cutoff = cut[first + r].astype(jnp.float32)
        flag = flags[first + r].astype(jnp.float32)
        factor[r] = flag * (1.0 - jnp.minimum(1.0, cutoff * cutoff * ksq[...]))

    def sum_copy():
        return pltpu.make_async_remote_copy(
            part, box.at[NX * NC + y], up_send, y_recv, device_id=root(0), device_id_type=MESH
        )

    def mean_copy(device):
        return pltpu.make_async_remote_copy(
            mean_in, mean_in, mean_send, mean_recv, device_id=device, device_id_type=MESH
        )

    members = [k for d in (4, 3, 5, 2, 6, 1, 7) for k in (NC * d, NC * d + 1)] + [0]

    def gather_row():
        landed(box.at[pl.ds(0, len(members))], x_recv)
        acc = part[...]
        for k in members:
            acc = acc + box[k]
        return acc

    def spread_row():
        for k in members:
            mean_copy(row(k)).start()

    @pl.when(is_later_root)
    def _():
        part[...] = gather_row()
        sum_copy().start()

    for copy in tables_in:
        copy.wait()
    lanes = lax.broadcasted_iota(jnp.int32, (16, HALF), 1)
    units = 2 * levels
    blocks = levels // 16

    def edges_above(g, carry):
        lev = pl.ds(pl.multiple_of(8 * g, 8), 8)
        above, above2 = halo[1, 0, lev, :], halo[1, 1, lev, :]
        t3 = s_hi[lev, :] * above
        f4 = face(4) * (halo[1, 2, lev, :] + c[3, lev, :]) * (7.0 * (above + h[3, lev, :]) - (above2 + h[2, lev, :]))
        base[2, lev, 0:nlon] = base[2, lev, 0:nlon] + t3 * inv_cos(2)
        base[3, lev, 0:nlon] = base[3, lev, 0:nlon] - (t3 + f4) * inv_cos(3)
        return carry

    def edges_below(g, carry):
        lev = pl.ds(pl.multiple_of(8 * g, 8), 8)
        below, below2 = halo[0, 1, lev, :], halo[0, 0, lev, :]
        t1 = s_lo[lev, :] * below
        f0 = face(0) * (halo[0, 2, lev, :] + c[0, lev, :]) * (7.0 * (below + h[0, lev, :]) - (below2 + h[1, lev, :]))
        base[0, lev, 0:nlon] = base[0, lev, 0:nlon] + (t1 + f0) * inv_cos(0)
        base[1, lev, 0:nlon] = base[1, lev, 0:nlon] - t1 * inv_cos(1)
        return carry

    def product(hilo, table):
        first_part = jnp.dot(hilo, table[0], preferred_element_type=jnp.float32)
        second = jnp.dot(hilo[0:units], table[1], preferred_element_type=jnp.float32)
        return first_part[0:units] + first_part[units : 2 * units] + second

    def filter_rows(row0):
        def block_of(b):
            return row0 + b // blocks, pl.ds(16 * (b % blocks), 16), pl.ds(16 * b, 16), pl.ds(units + 16 * b, 16)

        def forward(b):
            r, lev, at_hi, at_lo = block_of(b)
            v = [base[r, lev, HALF * j : HALF * (j + 1)] for j in range(RADIX)]
            u = [v[0]] + [
                pltpu.roll(jnp.where(lanes >= HALF - 8 * j, v[j - 1], v[j]), 8 * j, axis=1) for j in range(1, RADIX)
            ]
            e = [u[0]] + [u[j] + u[RADIX - j] for j in range(1, 6)] + [u[6]]
            o = [u[j] - u[RADIX - j] for j in range(1, 6)]
            even, odd = twelve(e, o)
            halves = [(even[0], even[6])] + [(even[m], odd[m - 1]) for m in range(1, 6)]
            for m, pair in enumerate(halves):
                for k, value in enumerate(pair):
                    hi, lo = split(value)
                    ymat[m, at_hi, HALF * k : HALF * (k + 1)] = hi
                    ymat[m, at_lo, HALF * k : HALF * (k + 1)] = lo

        def backward(b):
            r, lev, at, _ = block_of(b)
            w = [[wmat[m, at, HALF * k : HALF * (k + 1)] for k in range(2)] for m in range(RADIX // 2)]
            even, odd = twelve([w[0][0]] + [w[m][0] for m in range(1, 6)] + [w[0][1]], [w[m][1] for m in range(1, 6)])
            removed = [even[0]] + [even[j] + odd[j - 1] for j in range(1, 6)] + [even[6]]
            removed += [even[RADIX - j] - odd[RADIX - j - 1] for j in range(7, RADIX)]
            back = [removed[0]] + [pltpu.roll(removed[j], HALF - 8 * j, axis=1) for j in range(1, RADIX)]
            for j in range(RADIX):
                if j < RADIX - 1:
                    piece = jnp.where(lanes < count - 8 * j, back[j], back[j + 1])
                    out[r, lev, HALF * j : HALF * (j + 1)] = base[r, lev, HALF * j : HALF * (j + 1)] - piece
                else:
                    left = base[r, lev, HALF * j : HALF * (j + 1)] - back[j]
                    out[r, lev, HALF * j : nlon] = left[:, 0 : nlon - HALF * j]

        for b in range(2 * blocks):
            forward(b)
        for m in range(RADIX // 2):
            waves = product(ymat[m], (fwd[0, m], fwd[1, m]))
            scaled = jnp.concatenate(
                [waves[r * levels : (r + 1) * levels] * factor[row0 + r, m : m + 1, :] for r in range(2)], axis=0
            )
            wmat[m] = product(jnp.concatenate(split(scaled), axis=0), (inv[0, m], inv[1, m]))
        for b in range(2 * blocks):
            backward(b)

    @pl.when(position < last)
    def _():
        landed(halo.at[1], halo_recv.at[1])

    lax.fori_loop(0, levels // 8, edges_above, 0)
    filter_rows(2)

    @pl.when(is_first)
    def _():
        landed(box.at[pl.ds(NX * NC + 1, NY - 1)], y_recv)
        acc = box[NX * NC + 1]
        for k in range(2, NY):
            acc = acc + box[NX * NC + k]
        mean_in[...] = (gather_row() + acc) * (1.0 / area)
        for k in (1, 4, 3, 5, 2, 6, 7):
            mean_copy(root(k)).start()
        spread_row()

    @pl.when(position > 0)
    def _():
        landed(halo.at[0], halo_recv.at[0])

    lax.fori_loop(0, levels // 8, edges_below, 0)
    filter_rows(0)

    @pl.when(jnp.logical_not(is_first))
    def _():
        landed(mean_in, mean_recv)

    @pl.when(is_later_root)
    def _():
        spread_row()

    for g in range(levels // 8):
        lev = pl.ds(8 * g, 8)
        shift = jnp.sum(jnp.where(lane == g, mean_in[...], 0.0), axis=1, keepdims=True)
        for r in range(rows):
            out[r, lev, :] = out[r, lev, :] - shift

    for side, sender in ((0, position < last), (1, position > 0)):

        @pl.when(sender)
        def _():
            landed(halo.at[side], halo_send.at[side])

    @pl.when(is_first)
    def _():
        landed(box.at[pl.ds(0, len(members) + NY - 1)], mean_send)

    @pl.when(is_later_root)
    def _():
        landed(box.at[pl.ds(0, len(members))], mean_send)

    @pl.when(jnp.logical_not(is_first))
    def _():
        landed(part, up_send)


def local(height, zonal, merid, rates, thresholds, flags, cutoffs):
    rows, levels, nlon = height.shape
    nlat = rows * NX * NY * NC
    fwd, inv, ksq = filter_tables(nlon)
    scalars, cos_sum = row_scalars(nlat)
    tiles = RADIX // 2
    dims = (rows, levels, nlon, nlat)
    f32, bf16 = jnp.float32, jnp.bfloat16
    vmem, smem, dma = pltpu.VMEM, pltpu.SMEM, pltpu.SemaphoreType.DMA
    operands = (height, zonal, merid, rates, thresholds, flags, cutoffs, scalars, ksq, fwd, inv)
    operands = [pltpu.with_memory_space_constraint(jnp.asarray(a), pltpu.HBM) for a in operands]
    return pl.pallas_call(
        functools.partial(kernel, dims, nlon * cos_sum),
        out_shape=vmem(height.shape, f32),
        in_specs=[pl.BlockSpec(memory_space=pltpu.HBM)] * len(operands),
        out_specs=pl.BlockSpec(memory_space=vmem),
        scratch_shapes=[
            vmem(height.shape, f32), vmem(height.shape, f32), vmem(height.shape, f32),
            smem(rates.shape, f32), smem(thresholds.shape, f32), smem(flags.shape, jnp.int32),
            smem(cutoffs.shape, jnp.int32), smem(scalars.shape, f32),
            vmem(ksq.shape, f32), vmem(fwd.shape, bf16), vmem(inv.shape, bf16),
            vmem((2, 3, levels, nlon), f32), vmem((rows, levels, RADIX * HALF), f32),
            vmem((levels, nlon), f32), vmem((levels, nlon), f32), vmem((rows, 8, 2 * HALF), f32),
            vmem((tiles, 4 * levels, 2 * HALF), bf16), vmem((tiles, 2 * levels, 2 * HALF), f32),
            vmem((8, HALF), f32), vmem((NX * NC + NY, 8, HALF), f32), vmem((8, HALF), f32),
            vmem((levels // 8, 8, HALF), f32), vmem((levels // 8, 8, HALF), f32),
            dma((8,)), dma((2,)), dma((2,)), dma, dma, dma, dma, dma, pltpu.SemaphoreType.REGULAR,
        ],
        compiler_params=pltpu.CompilerParams(collective_id=0, has_side_effects=True, vmem_limit_bytes=16 * 2**20),
        name="advect_filter",
    )(*operands)


def solution(mesh):
    finer = Mesh(
        mesh.devices.reshape(mesh.shape["member"], NX, NY, NC), ("member", "lat_0", "lat_1", "lat_2")
    )
    whole = P(("member", "lat_0", "lat_1", "lat_2"), None, None)
    placed = (whole, whole, whole, P("member"), P("member"), P(), P())
    return jax.shard_map(local, mesh=finer, in_specs=placed, out_specs=whole, check_vma=False)
```

```python
import functools
import math

import jax
import jax.numpy as jnp
import numpy as np
from jax import lax
from jax.experimental import pallas as pl
from jax.experimental.pallas import tpu as pltpu
from jax.sharding import Mesh
from jax.sharding import PartitionSpec as P

MESH = pl.DeviceIdType.MESH
NX, NY, NC = 8, 8, 2
RADIX = 12
HALF = 128
ROOT = math.sqrt(0.75)


def filter_tables(nlon):
    count = nlon // RADIX
    tiles = RADIX // 2
    fwd = np.zeros((tiles, 2 * HALF, 2 * HALF))
    inv = np.zeros((tiles, 2 * HALF, 2 * HALF))
    waves = np.zeros((8, 2 * HALF), np.int64)
    r = np.arange(count)

    def trig(k):
        angle = 2.0 * np.pi / nlon * ((r * k) % nlon)
        return np.cos(angle), np.sin(angle)

    def real_part(base, shift):
        lane = base
        for q in range(count // 2 + 1):
            k = RADIX * q + shift
            if k > nlon // 2:
                continue
            cos, sin = trig(k)
            weight = (1.0 if k in (0, nlon // 2) else 2.0) / nlon
            rows = slice(base, base + count)
            fwd[0, rows, lane] = cos
            inv[0, lane, rows] = cos * weight
            waves[0, lane] = k
            lane += 1
            if k not in (0, nlon // 2):
                fwd[0, rows, lane] = sin
                inv[0, lane, rows] = sin * weight
                waves[0, lane] = k
                lane += 1
        assert lane == base + count

    real_part(0, 0)
    real_part(HALF, RADIX // 2)
    for m in range(1, tiles):
        for q in range(count):
            k = RADIX * q + m
            cos, sin = trig(k)
            fwd[m, 0:count, q] = cos
            fwd[m, HALF : HALF + count, q] = -sin
            fwd[m, 0:count, HALF + q] = sin
            fwd[m, HALF : HALF + count, HALF + q] = cos
            waves[m, q] = waves[m, HALF + q] = min(k, nlon - k)
        inv[m] = fwd[m].T * (2.0 / nlon)
    inv_square = 1.0 / np.maximum(waves, 1).astype(np.float64) ** 2

    def halves(table):
        hi = table.astype(np.float32).astype(jnp.bfloat16)
        lo = (table - hi.astype(np.float64)).astype(np.float32).astype(jnp.bfloat16)
        return np.stack([hi, lo])

    return halves(fwd), halves(inv), inv_square.astype(np.float32)


def row_scalars(nlat):
    rows = np.arange(nlat)
    cos_row = np.sin(np.pi * (rows + 0.5) / nlat)
    faces = np.arange(nlat + 1)
    cos_face = np.where((faces > 0) & (faces < nlat), np.sin(np.pi * faces / nlat), 0.0)
    table = np.zeros((3 * nlat + HALF,))
    table[0:nlat] = cos_row
    table[nlat : 2 * nlat] = 1.0 / cos_row
    table[2 * nlat : 3 * nlat + 1] = cos_face / 24.0
    return table.astype(np.float32), float(np.sum(cos_row))


def twelve(e, o):
    plus, minus = e[0] + e[6], e[0] - e[6]
    e15p, e15m, e24p, e24m = e[1] + e[5], e[1] - e[5], e[2] + e[4], e[2] - e[4]
    a, b = plus + e24p, e15p + e[3]
    big, mid = ROOT * e15m, minus + 0.5 * e24m
    c, d = plus - 0.5 * e24p, 0.5 * e15p - e[3]
    even = [a + b, mid + big, c + d, minus - e24m, c - d, mid - big, a - b]
    o15p, o15m, o24p, o24m = o[0] + o[4], o[0] - o[4], o[1] + o[3], o[1] - o[3]
    f, g = 0.5 * o15p + o[2], ROOT * o24p
    s, t = ROOT * o15m, ROOT * o24m
    odd = [f + g, s + t, o15p - o[2], s - t, f - g]
    return even, odd


def split(x):
    hi = x.astype(jnp.bfloat16)
    return hi, (x - hi.astype(jnp.float32)).astype(jnp.bfloat16)


def kernel(
    dims, area,
    h_hbm, z_hbm, c_hbm, rates_hbm, thr_hbm, flags_hbm, cut_hbm, scal_hbm, ksq_hbm, fwd_hbm, inv_hbm,
    out,
    h, z, c, rates, thr, flags, cut, scal, ksq, fwd, inv,
    halo, base, s_lo, s_hi, factor, ymat, wmat, part, box, mean_in, own_mean, level_rates, level_thresholds,
    in_sem, halo_send, halo_recv, up_send, x_recv, y_recv, mean_send, mean_recv, low_in,
):
    rows, levels, nlon, nlat = dims
    count = nlon // RADIX
    x, y, core = lax.axis_index("lat_0"), lax.axis_index("lat_1"), lax.axis_index("lat_2")
    position = (x * NY + y) * NC + core
    total = NX * NY * NC

    order = (2, 3, 0, 1)

    def fetch(src, dst, i):
        return pltpu.make_async_copy(src, dst, in_sem.at[i])

    h_in = {r: fetch(h_hbm.at[r], h.at[r], i) for i, r in enumerate(order)}
    c_up = fetch(c_hbm.at[rows - 1], c.at[rows - 1], 4)
    c_in = fetch(c_hbm.at[pl.ds(0, rows - 1)], c.at[pl.ds(0, rows - 1)], 3)
    small_in = [fetch(rates_hbm, rates, 5), fetch(thr_hbm, thr, 6), fetch(scal_hbm, scal, 7)]
    z_in = fetch(z_hbm, z, 0)
    tables_in = [fetch(fwd_hbm, fwd, 1), fetch(inv_hbm, inv, 2)]
    factor_in = [fetch(flags_hbm, flags, 5), fetch(cut_hbm, cut, 6), fetch(ksq_hbm, ksq, 7)]
    for copy in small_in + [h_in[r] for r in order] + [c_up]:
        copy.start()

    last = total - 1
    first = position * rows
    is_root = jnp.logical_and(x == 0, core == 1)
    is_first = position == 1
    is_later_root = jnp.logical_and(is_root, y > 0)

    def along(step):
        p = lax.rem(position + total + step, total)
        return {"lat_0": p // (NY * NC), "lat_1": lax.rem(p // NC, NY), "lat_2": lax.rem(p, NC)}

    def row(k):
        return {"lat_0": jnp.int32(k // NC), "lat_1": y, "lat_2": jnp.int32(k % NC)}

    def root(k):
        return {"lat_0": jnp.int32(0), "lat_1": jnp.int32(k), "lat_2": jnp.int32(1)}

    def signal(sem, device):
        pl.semaphore_signal(sem, inc=1, device_id=device, device_id_type=MESH)

    barrier = pltpu.get_barrier_semaphore()

    @pl.when(position > 0)
    def _():
        signal(barrier, along(-1))

    @pl.when(is_root)
    def _():
        for k in range(NX * NC):
            if k != 1:
                signal(barrier, row(k))

    @pl.when(is_first)
    def _():
        for k in range(1, NY):
            signal(barrier, root(k))

    greeted = jnp.where(is_first, 0, 1) + jnp.where(position < last, 1, 0)
    pl.semaphore_wait(barrier, greeted)

    @pl.when(position < last)
    def _():
        signal(low_in, along(1))

    def landed(ref, sem):
        pltpu.make_async_copy(ref, ref, sem).wait()

    def halo_copy(side, field):
        step, h_row, c_row = ((1, rows - 2, rows - 1), (-1, 0, 0))[side]
        src = (h.at[pl.ds(h_row, 2)], c.at[pl.ds(c_row, 1)])[field]
        dst = halo.at[side, pl.ds((0, 2)[field], (2, 1)[field])]
        return pltpu.make_async_remote_copy(
            src, dst, halo_send.at[side], halo_recv.at[side], device_id=along(step), device_id_type=MESH
        )

    own_mean[...] = jnp.zeros_like(own_mean)
    base[:, :, nlon:] = jnp.zeros((rows, levels, base.shape[2] - nlon), jnp.float32)

    @pl.when(position == 0)
    def _():
        halo[0] = jnp.zeros_like(halo[0])

    @pl.when(position == last)
    def _():
        halo[1] = jnp.zeros_like(halo[1])

    for copy in small_in:
        copy.wait()

    h_in[2].wait()
    h_in[3].wait()

    @pl.when(core == 0)
    def _():
        halo_copy(0, 0).start()

    lane = lax.broadcasted_iota(jnp.int32, (8, HALF), 1)
    tile = jnp.zeros((8, HALF), jnp.float32)
    sub = lax.broadcasted_iota(jnp.int32, (8, 1), 0)

    def levels_of(ref, start):
        value = jnp.zeros((8, 1), jnp.float32)
        for k in range(8):
            value = jnp.where(sub == k, ref[start + k], value)
        return value

    full = nlon // HALF
    groups = range(levels // 8)
    rate_of = [levels_of(rates, 8 * g) for g in groups]
    threshold_of = [levels_of(thr, 8 * g) for g in groups]
    wide, rest = [0.0 for g in groups], [0.0 for g in groups]
    for r in order:
        if r < 2:
            h_in[r].wait()
        for g in groups:
            lev = pl.ds(8 * g, 8)
            positive, factors = 0.0, 1.0
            for j in range(full):
                s = h[r, lev, HALF * j : HALF * (j + 1)] - threshold_of[g]
                positive = positive + jnp.maximum(s, 0.0)
                factors = factors * (1.0 + jnp.exp(-jnp.abs(s)))
            s = h[r, lev, HALF * full : nlon] - threshold_of[g]
            wide[g] = wide[g] + scal[first + r] * (positive + jnp.log(factors))
            rest[g] = rest[g] + scal[first + r] * (jnp.maximum(s, 0.0) + jnp.log(1.0 + jnp.exp(-jnp.abs(s))))
    short = jnp.zeros((8, HALF * (full + 1) - nlon), jnp.float32)
    for g in groups:
        sums = jnp.sum(wide[g] + jnp.concatenate([rest[g], short], axis=1), axis=1, keepdims=True)
        tile = jnp.where(lane == g, -rate_of[g] * sums, tile)
        level_rates[g] = jnp.broadcast_to(rate_of[g], (8, HALF))
        level_thresholds[g] = jnp.broadcast_to(threshold_of[g], (8, HALF))
    part[...] = tile

    def part_copy(slot):
        return pltpu.make_async_remote_copy(
            part, box.at[slot], up_send, x_recv, device_id=row(1), device_id_type=MESH
        )

    @pl.when(jnp.logical_not(is_root))
    def _():
        part_copy(x * NC + core).start()

    c_up.wait()

    @pl.when(jnp.logical_and(core != 0, position < last))
    def _():
        halo_copy(0, 0).start()

    @pl.when(position < last)
    def _():
        halo_copy(0, 1).start()

    for copy in [c_in, z_in] + factor_in + tables_in:
        copy.start()

    c_in.wait()
    z_in.wait()

    def inv_cos(r):
        return scal[nlat + first + r]

    def face(f):
        return scal[2 * nlat + first + f]

    def west(a):
        return pltpu.roll(a, 1, axis=1)

    def east(a):
        return pltpu.roll(a, nlon - 1, axis=1)

    def local_terms(g, carry):
        lev = pl.ds(pl.multiple_of(8 * g, 8), 8)
        hr = [h[r, lev, :] for r in range(rows)]
        rate, threshold = level_rates[g][:, 0:1], level_thresholds[g][:, 0:1]
        cr = [c[r, lev, :] for r in range(rows)]
        low = face(1) * (cr[0] + cr[1])
        high = face(3) * (cr[2] + cr[3])
        s_lo[lev, :] = low
        s_hi[lev, :] = high
        f1 = low * (7.0 * (hr[0] + hr[1]) - hr[2])
        f2 = face(2) * (cr[1] + cr[2]) * (7.0 * (hr[1] + hr[2]) - (hr[0] + hr[3]))
        f3 = high * (7.0 * (hr[2] + hr[3]) - hr[1])
        terms = [f1, f2 - f1, f3 - f2, -f3]
        for r in range(rows):
            pair = hr[r] + east(hr[r])
            zr = z[r, lev, :]
            speed = zr + east(zr)
            flux = speed * (8.0 * pair - (west(pair) + east(pair))) * (1.0 / 24.0)
            s = hr[r] - threshold
            source = rate * (jnp.maximum(s, 0.0) + jnp.log(1.0 + jnp.exp(-jnp.abs(s))))
            base[r, lev, 0:nlon] = (hr[r] - source) - (flux - west(flux)) - terms[r] * inv_cos(r)
        return carry

    lax.fori_loop(0, levels // 8, local_terms, 0)

    @pl.when(position > 0)
    def _():
        pl.semaphore_wait(low_in, 1)
        halo_copy(1, 0).start()
        halo_copy(1, 1).start()

    for copy in factor_in:
        copy.wait()
    for r in range(rows):
        cutoff = cut[first + r].astype(jnp.float32)
        flag = flags[first + r].astype(jnp.float32)
        factor[r] = flag * (1.0 - jnp.minimum(1.0, cutoff * cutoff * ksq[...]))

    def sum_copy():
        return pltpu.make_async_remote_copy(
            part, box.at[NX * NC + y], up_send, y_recv, device_id=root(0), device_id_type=MESH
        )

    def mean_copy(device):
        return pltpu.make_async_remote_copy(
            own_mean, mean_in, mean_send, mean_recv, device_id=device, device_id_type=MESH
        )

    members = [k for d in (4, 3, 5, 2, 6, 1, 7) for k in (NC * d, NC * d + 1)] + [0]

    def gather_row():
        landed(box.at[pl.ds(0, len(members))], x_recv)
        acc = part[...]
        for k in members:
            acc = acc + box[k]
        return acc

    def spread_row():
        for k in members:
            mean_copy(row(k)).start()

    @pl.when(is_later_root)
    def _():
        part[...] = gather_row()
        sum_copy().start()

    for copy in tables_in:
        copy.wait()
    lanes = lax.broadcasted_iota(jnp.int32, (16, HALF), 1)
    units = 2 * levels
    blocks = levels // 16

    tail = nlon - HALF * (RADIX - 1)

    def piece(ref, j):
        if j < RADIX - 1:
            return ref[:, HALF * j : HALF * (j + 1)]
        return jnp.concatenate([ref[:, HALF * j : nlon], jnp.zeros((16, HALF - tail), jnp.float32)], axis=1)

    def with_halo(r, lev, j):
        side, near, far, edge, inner, f, through, outer = (
            (0, 1, 0, 0, 1, 0, s_lo, 0) if r < 2 else (1, 0, 1, rows - 1, rows - 2, rows, s_hi, rows - 1)
        )
        beside = piece(halo.at[side, near, lev], j)
        term = piece(through.at[lev], j) * beside
        if r == outer:
            speed = face(f) * (piece(halo.at[side, 2, lev], j) + piece(c.at[edge, lev], j))
            flux = speed * (
                7.0 * (beside + piece(h.at[edge, lev], j)) - (piece(halo.at[side, far, lev], j) + piece(h.at[inner, lev], j))
            )
            term = term + flux
        sign = 1.0 if r in (0, 2) else -1.0
        return base[r, lev, HALF * j : HALF * (j + 1)] + term * (sign * inv_cos(r))

    def product(hilo, table):
        first_part = jnp.dot(hilo, table[0], preferred_element_type=jnp.float32)
        second = jnp.dot(hilo[0:units], table[1], preferred_element_type=jnp.float32)
        return first_part[0:units] + first_part[units : 2 * units] + second

    def filter_rows(row0, shifts=None):
        def block_of(b):
            return row0 + b // blocks, pl.ds(16 * (b % blocks), 16), pl.ds(16 * b, 16), pl.ds(units + 16 * b, 16)

        def forward(b):
            r, lev, at_hi, at_lo = block_of(b)
            v = [with_halo(r, lev, j) for j in range(RADIX)]
            for j in range(RADIX):
                base[r, lev, HALF * j : HALF * (j + 1)] = v[j]
            u = [v[0]] + [
                pltpu.roll(jnp.where(lanes >= HALF - 8 * j, v[j - 1], v[j]), 8 * j, axis=1) for j in range(1, RADIX)
            ]
            e = [u[0]] + [u[j] + u[RADIX - j] for j in range(1, 6)] + [u[6]]
            o = [u[j] - u[RADIX - j] for j in range(1, 6)]
            even, odd = twelve(e, o)
            halves = [(even[0], even[6])] + [(even[m], odd[m - 1]) for m in range(1, 6)]
            for m, pair in enumerate(halves):
                for k, value in enumerate(pair):
                    hi, lo = split(value)
                    ymat[m, at_hi, HALF * k : HALF * (k + 1)] = hi
                    ymat[m, at_lo, HALF * k : HALF * (k + 1)] = lo

        def backward(b):
            r, lev, at, _ = block_of(b)
            w = [[wmat[m, at, HALF * k : HALF * (k + 1)] for k in range(2)] for m in range(RADIX // 2)]
            even, odd = twelve([w[0][0]] + [w[m][0] for m in range(1, 6)] + [w[0][1]], [w[m][1] for m in range(1, 6)])
            removed = [even[0]] + [even[j] + odd[j - 1] for j in range(1, 6)] + [even[6]]
            removed += [even[RADIX - j] - odd[RADIX - j - 1] for j in range(7, RADIX)]
            back = [removed[0]] + [pltpu.roll(removed[j], HALF - 8 * j, axis=1) for j in range(1, RADIX)]
            for j in range(RADIX):
                kept = base[r, lev, HALF * j : HALF * (j + 1)]
                if row0 == 0:
                    kept = kept - shifts[b % blocks]
                if j < RADIX - 1:
                    out[r, lev, HALF * j : HALF * (j + 1)] = kept - jnp.where(lanes < count - 8 * j, back[j], back[j + 1])
                else:
                    out[r, lev, HALF * j : nlon] = (kept - back[j])[:, 0:tail]

        for b in range(2 * blocks):
            forward(b)
        for m in range(RADIX // 2):
            waves = product(ymat[m], (fwd[0, m], fwd[1, m]))
            scaled = jnp.concatenate(
                [waves[r * levels : (r + 1) * levels] * factor[row0 + r, m : m + 1, :] for r in range(2)], axis=0
            )
            wmat[m] = product(jnp.concatenate(split(scaled), axis=0), (inv[0, m], inv[1, m]))
        if row0 == 0:
            for r in (2, 3):
                for b in range(blocks):
                    lev = pl.ds(16 * b, 16)
                    out[r, lev, :] = out[r, lev, :] - shifts[b]
        for b in range(2 * blocks):
            backward(b)

    @pl.when(position < last)
    def _():
        landed(halo.at[1], halo_recv.at[1])

    filter_rows(2)

    @pl.when(is_first)
    def _():
        landed(box.at[pl.ds(NX * NC + 1, NY - 1)], y_recv)
        acc = box[NX * NC + 1]
        for k in range(2, NY):
            acc = acc + box[NX * NC + k]
        own_mean[...] = (gather_row() + acc) * (1.0 / area)
        for k in (1, 4, 3, 5, 2, 6, 7):
            mean_copy(root(k)).start()
        spread_row()

    @pl.when(position > 0)
    def _():
        landed(halo.at[0], halo_recv.at[0])

    def mean_columns(ref):
        return [jnp.sum(jnp.where(lane == g, ref[...], 0.0), axis=1, keepdims=True) for g in groups]

    columns = mean_columns(own_mean)
    shifts = [jnp.concatenate(columns[2 * b : 2 * b + 2], axis=0) for b in range(blocks)]
    filter_rows(0, shifts)

    @pl.when(jnp.logical_not(is_first))
    def _():
        landed(mean_in, mean_recv)

    @pl.when(is_later_root)
    def _():
        own_mean[...] = mean_in[...]
        spread_row()

    @pl.when(jnp.logical_not(is_first))
    def _():
        for g, shift in zip(groups, mean_columns(mean_in)):
            lev = pl.ds(8 * g, 8)
            for r in range(rows):
                out[r, lev, :] = out[r, lev, :] - shift

    for side, sender in ((0, position < last), (1, position > 0)):

        @pl.when(sender)
        def _():
            landed(halo.at[side], halo_send.at[side])

    @pl.when(is_first)
    def _():
        landed(box.at[pl.ds(0, len(members) + NY - 1)], mean_send)

    @pl.when(is_later_root)
    def _():
        landed(box.at[pl.ds(0, len(members))], mean_send)

    @pl.when(jnp.logical_not(is_first))
    def _():
        landed(part, up_send)


def local(height, zonal, merid, rates, thresholds, flags, cutoffs):
    rows, levels, nlon = height.shape
    nlat = rows * NX * NY * NC
    fwd, inv, ksq = filter_tables(nlon)
    scalars, cos_sum = row_scalars(nlat)
    tiles = RADIX // 2
    dims = (rows, levels, nlon, nlat)
    f32, bf16 = jnp.float32, jnp.bfloat16
    vmem, smem, dma = pltpu.VMEM, pltpu.SMEM, pltpu.SemaphoreType.DMA
    operands = (height, zonal, merid, rates, thresholds, flags, cutoffs, scalars, ksq, fwd, inv)
    operands = [pltpu.with_memory_space_constraint(jnp.asarray(a), pltpu.HBM) for a in operands]
    return pl.pallas_call(
        functools.partial(kernel, dims, nlon * cos_sum),
        out_shape=vmem(height.shape, f32),
        in_specs=[pl.BlockSpec(memory_space=pltpu.HBM)] * len(operands),
        out_specs=pl.BlockSpec(memory_space=vmem),
        scratch_shapes=[
            vmem(height.shape, f32), vmem(height.shape, f32), vmem(height.shape, f32),
            smem(rates.shape, f32), smem(thresholds.shape, f32), smem(flags.shape, jnp.int32),
            smem(cutoffs.shape, jnp.int32), smem(scalars.shape, f32),
            vmem(ksq.shape, f32), vmem(fwd.shape, bf16), vmem(inv.shape, bf16),
            vmem((2, 3, levels, nlon), f32), vmem((rows, levels, RADIX * HALF), f32),
            vmem((levels, nlon), f32), vmem((levels, nlon), f32), vmem((rows, 8, 2 * HALF), f32),
            vmem((tiles, 4 * levels, 2 * HALF), bf16), vmem((tiles, 2 * levels, 2 * HALF), f32),
            vmem((8, HALF), f32), vmem((NX * NC + NY, 8, HALF), f32), vmem((8, HALF), f32),
            vmem((8, HALF), f32),
            vmem((levels // 8, 8, HALF), f32), vmem((levels // 8, 8, HALF), f32),
            dma((8,)), dma((2,)), dma((2,)), dma, dma, dma, dma, dma, pltpu.SemaphoreType.REGULAR,
        ],
        compiler_params=pltpu.CompilerParams(collective_id=0, has_side_effects=True, vmem_limit_bytes=16 * 2**20),
        name="advect_filter",
    )(*operands)


def solution(mesh):
    finer = Mesh(
        mesh.devices.reshape(mesh.shape["member"], NX, NY, NC), ("member", "lat_0", "lat_1", "lat_2")
    )
    whole = P(("member", "lat_0", "lat_1", "lat_2"), None, None)
    placed = (whole, whole, whole, P("member"), P("member"), P(), P())
    return jax.shard_map(local, mesh=finer, in_specs=placed, out_specs=whole, check_vma=False)
```

```python
import functools
import math

import jax
import jax.numpy as jnp
import numpy as np
from jax import lax
from jax.experimental import pallas as pl
from jax.experimental.pallas import tpu as pltpu
from jax.sharding import Mesh
from jax.sharding import PartitionSpec as P

MESH = pl.DeviceIdType.MESH
NX, NY, NC = 8, 8, 2
RADIX = 12
HALF = 128
ROOT = math.sqrt(0.75)
LOG2E = math.log2(math.e)


def filter_tables(nlon):
    count = nlon // RADIX
    tiles = RADIX // 2
    fwd = np.zeros((tiles, 2 * HALF, 2 * HALF))
    inv = np.zeros((tiles, 2 * HALF, 2 * HALF))
    waves = np.zeros((8, 2 * HALF), np.int64)
    r = np.arange(count)

    def trig(k):
        angle = 2.0 * np.pi / nlon * ((r * k) % nlon)
        return np.cos(angle), np.sin(angle)

    def real_part(base, shift):
        lane = base
        for q in range(count // 2 + 1):
            k = RADIX * q + shift
            if k > nlon // 2:
                continue
            cos, sin = trig(k)
            weight = (1.0 if k in (0, nlon // 2) else 2.0) / nlon
            rows = slice(base, base + count)
            fwd[0, rows, lane] = cos
            inv[0, lane, rows] = cos * weight
            waves[0, lane] = k
            lane += 1
            if k not in (0, nlon // 2):
                fwd[0, rows, lane] = sin
                inv[0, lane, rows] = sin * weight
                waves[0, lane] = k
                lane += 1
        assert lane == base + count

    real_part(0, 0)
    real_part(HALF, RADIX // 2)
    for m in range(1, tiles):
        for q in range(count):
            k = RADIX * q + m
            cos, sin = trig(k)
            fwd[m, 0:count, q] = cos
            fwd[m, HALF : HALF + count, q] = -sin
            fwd[m, 0:count, HALF + q] = sin
            fwd[m, HALF : HALF + count, HALF + q] = cos
            waves[m, q] = waves[m, HALF + q] = min(k, nlon - k)
        inv[m] = fwd[m].T * (2.0 / nlon)
    inv_square = 1.0 / np.maximum(waves, 1).astype(np.float64) ** 2

    def halves(table):
        hi = table.astype(np.float32).astype(jnp.bfloat16)
        lo = (table - hi.astype(np.float64)).astype(np.float32).astype(jnp.bfloat16)
        return np.stack([hi, lo])

    return halves(fwd), halves(inv), inv_square.astype(np.float32)


def row_scalars(nlat):
    rows = np.arange(nlat)
    cos_row = np.sin(np.pi * (rows + 0.5) / nlat)
    faces = np.arange(nlat + 1)
    cos_face = np.where((faces > 0) & (faces < nlat), np.sin(np.pi * faces / nlat), 0.0)
    table = np.zeros((3 * nlat + HALF,))
    table[0:nlat] = cos_row
    table[nlat : 2 * nlat] = 1.0 / cos_row
    table[2 * nlat : 3 * nlat + 1] = cos_face / 24.0
    return table.astype(np.float32), float(np.sum(cos_row))


def twelve(e, o):
    plus, minus = e[0] + e[6], e[0] - e[6]
    e15p, e15m, e24p, e24m = e[1] + e[5], e[1] - e[5], e[2] + e[4], e[2] - e[4]
    a, b = plus + e24p, e15p + e[3]
    big, mid = ROOT * e15m, minus + 0.5 * e24m
    c, d = plus - 0.5 * e24p, 0.5 * e15p - e[3]
    even = [a + b, mid + big, c + d, minus - e24m, c - d, mid - big, a - b]
    o15p, o15m, o24p, o24m = o[0] + o[4], o[0] - o[4], o[1] + o[3], o[1] - o[3]
    f, g = 0.5 * o15p + o[2], ROOT * o24p
    s, t = ROOT * o15m, ROOT * o24m
    odd = [f + g, s + t, o15p - o[2], s - t, f - g]
    return even, odd


def product_of(exps):
    result = 1.0 + exps[0]
    for e in exps[1:]:
        result = result * (1.0 + e)
    return result


def split(x):
    hi = x.astype(jnp.bfloat16)
    return hi, (x - hi.astype(jnp.float32)).astype(jnp.bfloat16)


def kernel(
    dims, area,
    h_hbm, z_hbm, c_hbm, rates_hbm, thr_hbm, flags_hbm, cut_hbm, scal_hbm, ksq_hbm, fwd_hbm, inv_hbm,
    out,
    h, z, c, rates, thr, flags, cut, scal, ksq, fwd, inv,
    halo, base, s_lo, s_hi, factor, ymat, wmat, part, box, mean_in, own_mean, level_rates, level_thresholds,
    in_sem, halo_send, halo_recv, up_send, x_recv, y_recv, mean_send, mean_recv, low_in,
):
    rows, levels, nlon, nlat = dims
    count = nlon // RADIX
    x, y, core = lax.axis_index("lat_0"), lax.axis_index("lat_1"), lax.axis_index("lat_2")
    position = (x * NY + y) * NC + core
    total = NX * NY * NC

    order = (2, 3, 0, 1)

    def fetch(src, dst, i):
        return pltpu.make_async_copy(src, dst, in_sem.at[i])

    h_in = {r: fetch(h_hbm.at[r], h.at[r], i) for i, r in enumerate(order)}
    c_up = fetch(c_hbm.at[rows - 1], c.at[rows - 1], 4)
    c_in = fetch(c_hbm.at[pl.ds(0, rows - 1)], c.at[pl.ds(0, rows - 1)], 3)
    small_in = [fetch(rates_hbm, rates, 5), fetch(thr_hbm, thr, 6), fetch(scal_hbm, scal, 7)]
    z_in = fetch(z_hbm, z, 0)
    tables_in = [fetch(fwd_hbm, fwd, 1), fetch(inv_hbm, inv, 2)]
    factor_in = [fetch(flags_hbm, flags, 5), fetch(cut_hbm, cut, 6), fetch(ksq_hbm, ksq, 7)]
    for copy in small_in + [h_in[r] for r in order] + [c_up]:
        copy.start()

    last = total - 1
    first = position * rows
    is_root = jnp.logical_and(x == 0, core == 1)
    is_first = position == 1
    is_later_root = jnp.logical_and(is_root, y > 0)

    def along(step):
        p = lax.rem(position + total + step, total)
        return {"lat_0": p // (NY * NC), "lat_1": lax.rem(p // NC, NY), "lat_2": lax.rem(p, NC)}

    def row(k):
        return {"lat_0": jnp.int32(k // NC), "lat_1": y, "lat_2": jnp.int32(k % NC)}

    def root(k):
        return {"lat_0": jnp.int32(0), "lat_1": jnp.int32(k), "lat_2": jnp.int32(1)}

    def signal(sem, device):
        pl.semaphore_signal(sem, inc=1, device_id=device, device_id_type=MESH)

    barrier = pltpu.get_barrier_semaphore()

    @pl.when(position > 0)
    def _():
        signal(barrier, along(-1))

    @pl.when(is_root)
    def _():
        for k in range(NX * NC):
            if k != 1:
                signal(barrier, row(k))

    @pl.when(is_first)
    def _():
        for k in range(1, NY):
            signal(barrier, root(k))

    greeted = jnp.where(is_first, 0, 1) + jnp.where(position < last, 1, 0)
    pl.semaphore_wait(barrier, greeted)

    @pl.when(position < last)
    def _():
        signal(low_in, along(1))

    def landed(ref, sem):
        pltpu.make_async_copy(ref, ref, sem).wait()

    def halo_copy(side, field):
        step, h_row, c_row = ((1, rows - 2, rows - 1), (-1, 0, 0))[side]
        src = c.at[c_row] if field == 2 else h.at[h_row + field]
        return pltpu.make_async_remote_copy(
            src, halo.at[side, field], halo_send.at[side], halo_recv.at[side], device_id=along(step), device_id_type=MESH
        )

    own_mean[...] = jnp.zeros_like(own_mean)
    base[:, :, nlon:] = jnp.zeros((rows, levels, base.shape[2] - nlon), jnp.float32)

    @pl.when(position == 0)
    def _():
        halo[0] = jnp.zeros_like(halo[0])

    @pl.when(position == last)
    def _():
        halo[1] = jnp.zeros_like(halo[1])

    for copy in small_in:
        copy.wait()

    for field in (0, 1):
        h_in[rows - 2 + field].wait()

        @pl.when(core == 0)
        def _():
            halo_copy(0, field).start()

    lane = lax.broadcasted_iota(jnp.int32, (8, HALF), 1)
    tile = jnp.zeros((8, HALF), jnp.float32)
    sub = lax.broadcasted_iota(jnp.int32, (8, 1), 0)

    def levels_of(ref, start):
        value = jnp.zeros((8, 1), jnp.float32)
        for k in range(8):
            value = jnp.where(sub == k, ref[start + k], value)
        return value

    full = nlon // HALF
    groups = range(levels // 8)
    rate_of = [levels_of(rates, 8 * g) for g in groups]
    threshold_of = [levels_of(thr, 8 * g) for g in groups]
    scaled_threshold = [LOG2E * value for value in threshold_of]
    wide, rest = [0.0 for g in groups], [0.0 for g in groups]
    for r in order:
        if r < 2:
            h_in[r].wait()
        for g in groups:
            lev = pl.ds(8 * g, 8)
            exps = [
                jnp.exp2(h[r, lev, HALF * j : HALF * (j + 1)] * LOG2E - scaled_threshold[g]) for j in range(full)
            ]
            logs = jnp.log2(product_of(exps[0:6])) + jnp.log2(product_of(exps[6:full]))
            wide[g] = wide[g] + scal[first + r] * logs
            logs = jnp.log2(1.0 + jnp.exp2(h[r, lev, HALF * full : nlon] * LOG2E - scaled_threshold[g]))
            rest[g] = rest[g] + scal[first + r] * logs
    short = jnp.zeros((8, HALF * (full + 1) - nlon), jnp.float32)
    for g in groups:
        sums = jnp.sum(wide[g] + jnp.concatenate([rest[g], short], axis=1), axis=1, keepdims=True)
        tile = jnp.where(lane == g, (-1.0 / LOG2E) * rate_of[g] * sums, tile)
        level_rates[g] = jnp.broadcast_to(rate_of[g], (8, HALF))
        level_thresholds[g] = jnp.broadcast_to(threshold_of[g], (8, HALF))
    part[...] = tile

    def part_copy(slot):
        return pltpu.make_async_remote_copy(
            part, box.at[slot], up_send, x_recv, device_id=row(1), device_id_type=MESH
        )

    @pl.when(jnp.logical_not(is_root))
    def _():
        part_copy(x * NC + core).start()

    c_up.wait()

    @pl.when(jnp.logical_and(core != 0, position < last))
    def _():
        halo_copy(0, 0).start()
        halo_copy(0, 1).start()

    @pl.when(position < last)
    def _():
        halo_copy(0, 2).start()

    for copy in [c_in, z_in] + factor_in + tables_in:
        copy.start()

    c_in.wait()
    z_in.wait()

    def inv_cos(r):
        return scal[nlat + first + r]

    def face(f):
        return scal[2 * nlat + first + f]

    def west(a):
        return pltpu.roll(a, 1, axis=1)

    def east(a):
        return pltpu.roll(a, nlon - 1, axis=1)

    def local_terms(g, carry):
        lev = pl.ds(pl.multiple_of(8 * g, 8), 8)
        hr = [h[r, lev, :] for r in range(rows)]
        rate, threshold = level_rates[g][:, 0:1], level_thresholds[g][:, 0:1]
        cr = [c[r, lev, :] for r in range(rows)]
        low = face(1) * (cr[0] + cr[1])
        high = face(3) * (cr[2] + cr[3])
        s_lo[lev, :] = low
        s_hi[lev, :] = high
        f1 = low * (7.0 * (hr[0] + hr[1]) - hr[2])
        f2 = face(2) * (cr[1] + cr[2]) * (7.0 * (hr[1] + hr[2]) - (hr[0] + hr[3]))
        f3 = high * (7.0 * (hr[2] + hr[3]) - hr[1])
        terms = [f1, f2 - f1, f3 - f2, -f3]
        for r in range(rows):
            pair = hr[r] + east(hr[r])
            zr = z[r, lev, :]
            speed = zr + east(zr)
            flux = speed * (8.0 * pair - (west(pair) + east(pair))) * (1.0 / 24.0)
            s = hr[r] - threshold
            source = rate * jnp.log(1.0 + jnp.exp(s))
            base[r, lev, 0:nlon] = (hr[r] - source) - (flux - west(flux)) - terms[r] * inv_cos(r)
        return carry

    lax.fori_loop(0, levels // 8, local_terms, 0)

    @pl.when(position > 0)
    def _():
        pl.semaphore_wait(low_in, 1)
        for field in range(3):
            halo_copy(1, field).start()

    for copy in factor_in:
        copy.wait()
    for r in range(rows):
        cutoff = cut[first + r].astype(jnp.float32)
        flag = flags[first + r].astype(jnp.float32)
        factor[r] = flag * (1.0 - jnp.minimum(1.0, cutoff * cutoff * ksq[...]))

    def sum_copy():
        return pltpu.make_async_remote_copy(
            part, box.at[NX * NC + y], up_send, y_recv, device_id=root(0), device_id_type=MESH
        )

    def mean_copy(device):
        return pltpu.make_async_remote_copy(
            own_mean, mean_in, mean_send, mean_recv, device_id=device, device_id_type=MESH
        )

    members = [*range(NC, NX * NC), 0]

    def gather_row():
        landed(box.at[pl.ds(0, len(members))], x_recv)
        acc = part[...]
        for k in members:
            acc = acc + box[k]
        return acc

    def spread_row():
        for k in members:
            mean_copy(row(k)).start()

    @pl.when(is_later_root)
    def _():
        part[...] = gather_row()
        sum_copy().start()

    for copy in tables_in:
        copy.wait()
    lanes = lax.broadcasted_iota(jnp.int32, (16, HALF), 1)
    units = 2 * levels
    blocks = levels // 16

    tail = nlon - HALF * (RADIX - 1)

    def piece(ref, j):
        if j < RADIX - 1:
            return ref[:, HALF * j : HALF * (j + 1)]
        return jnp.concatenate([ref[:, HALF * j : nlon], jnp.zeros((16, HALF - tail), jnp.float32)], axis=1)

    def with_halo(r, lev, j):
        side, near, far, edge, inner, f, through, outer = (
            (0, 1, 0, 0, 1, 0, s_lo, 0) if r < 2 else (1, 0, 1, rows - 1, rows - 2, rows, s_hi, rows - 1)
        )
        beside = piece(halo.at[side, near, lev], j)
        term = piece(through.at[lev], j) * beside
        if r == outer:
            speed = face(f) * (piece(halo.at[side, 2, lev], j) + piece(c.at[edge, lev], j))
            flux = speed * (
                7.0 * (beside + piece(h.at[edge, lev], j)) - (piece(halo.at[side, far, lev], j) + piece(h.at[inner, lev], j))
            )
            term = term + flux
        sign = 1.0 if r in (0, 2) else -1.0
        return base[r, lev, HALF * j : HALF * (j + 1)] + term * (sign * inv_cos(r))

    def product(hilo, table):
        first_part = jnp.dot(hilo, table[0], preferred_element_type=jnp.float32)
        second = jnp.dot(hilo[0:units], table[1], preferred_element_type=jnp.float32)
        return first_part[0:units] + first_part[units : 2 * units] + second

    def filter_rows(row0, shifts=None):
        def block_of(b):
            return row0 + b // blocks, pl.ds(16 * (b % blocks), 16), pl.ds(16 * b, 16), pl.ds(units + 16 * b, 16)

        def forward(b):
            r, lev, at_hi, at_lo = block_of(b)
            v = [with_halo(r, lev, j) for j in range(RADIX)]
            for j in range(RADIX):
                base[r, lev, HALF * j : HALF * (j + 1)] = v[j]
            u = [v[0]] + [
                pltpu.roll(jnp.where(lanes >= HALF - 8 * j, v[j - 1], v[j]), 8 * j, axis=1) for j in range(1, RADIX)
            ]
            e = [u[0]] + [u[j] + u[RADIX - j] for j in range(1, 6)] + [u[6]]
            o = [u[j] - u[RADIX - j] for j in range(1, 6)]
            even, odd = twelve(e, o)
            halves = [(even[0], even[6])] + [(even[m], odd[m - 1]) for m in range(1, 6)]
            for m, pair in enumerate(halves):
                for k, value in enumerate(pair):
                    hi, lo = split(value)
                    ymat[m, at_hi, HALF * k : HALF * (k + 1)] = hi
                    ymat[m, at_lo, HALF * k : HALF * (k + 1)] = lo

        def backward(b):
            r, lev, at, _ = block_of(b)
            w = [[wmat[m, at, HALF * k : HALF * (k + 1)] for k in range(2)] for m in range(RADIX // 2)]
            even, odd = twelve([w[0][0]] + [w[m][0] for m in range(1, 6)] + [w[0][1]], [w[m][1] for m in range(1, 6)])
            removed = [even[0]] + [even[j] + odd[j - 1] for j in range(1, 6)] + [even[6]]
            removed += [even[RADIX - j] - odd[RADIX - j - 1] for j in range(7, RADIX)]
            back = [removed[0]] + [pltpu.roll(removed[j], HALF - 8 * j, axis=1) for j in range(1, RADIX)]
            for j in range(RADIX):
                kept = base[r, lev, HALF * j : HALF * (j + 1)]
                if row0 == 0:
                    kept = kept - shifts[b % blocks]
                if j < RADIX - 1:
                    out[r, lev, HALF * j : HALF * (j + 1)] = kept - jnp.where(lanes < count - 8 * j, back[j], back[j + 1])
                else:
                    out[r, lev, HALF * j : nlon] = (kept - back[j])[:, 0:tail]

        for b in range(2 * blocks):
            forward(b)
        for m in range(RADIX // 2):
            waves = product(ymat[m], (fwd[0, m], fwd[1, m]))
            scaled = jnp.concatenate(
                [waves[r * levels : (r + 1) * levels] * factor[row0 + r, m : m + 1, :] for r in range(2)], axis=0
            )
            wmat[m] = product(jnp.concatenate(split(scaled), axis=0), (inv[0, m], inv[1, m]))
        if row0 == 0:
            for r in (2, 3):
                for b in range(blocks):
                    lev = pl.ds(16 * b, 16)
                    out[r, lev, :] = out[r, lev, :] - shifts[b]
        for b in range(2 * blocks):
            backward(b)

    @pl.when(position < last)
    def _():
        landed(halo.at[1], halo_recv.at[1])

    filter_rows(2)

    @pl.when(is_first)
    def _():
        landed(box.at[pl.ds(NX * NC + 1, NY - 1)], y_recv)
        acc = box[NX * NC + 1]
        for k in range(2, NY):
            acc = acc + box[NX * NC + k]
        own_mean[...] = (gather_row() + acc) * (1.0 / area)
        for k in range(1, NY):
            mean_copy(root(k)).start()
            for member in members[2 * k - 2 : 2 * k]:
                mean_copy(row(member)).start()
        mean_copy(row(0)).start()

    @pl.when(position > 0)
    def _():
        landed(halo.at[0], halo_recv.at[0])

    def mean_columns(ref):
        return [jnp.sum(jnp.where(lane == g, ref[...], 0.0), axis=1, keepdims=True) for g in groups]

    columns = mean_columns(own_mean)
    shifts = [jnp.concatenate(columns[2 * b : 2 * b + 2], axis=0) for b in range(blocks)]
    filter_rows(0, shifts)

    @pl.when(jnp.logical_not(is_first))
    def _():
        landed(mean_in, mean_recv)

    @pl.when(is_later_root)
    def _():
        own_mean[...] = mean_in[...]
        spread_row()

    @pl.when(jnp.logical_not(is_first))
    def _():
        for g, shift in zip(groups, mean_columns(mean_in)):
            lev = pl.ds(8 * g, 8)
            for r in range(rows):
                out[r, lev, :] = out[r, lev, :] - shift

    for side, sender in ((0, position < last), (1, position > 0)):

        @pl.when(sender)
        def _():
            landed(halo.at[side], halo_send.at[side])

    @pl.when(is_first)
    def _():
        landed(box.at[pl.ds(0, len(members) + NY - 1)], mean_send)

    @pl.when(is_later_root)
    def _():
        landed(box.at[pl.ds(0, len(members))], mean_send)

    @pl.when(jnp.logical_not(is_first))
    def _():
        landed(part, up_send)


def local(height, zonal, merid, rates, thresholds, flags, cutoffs):
    rows, levels, nlon = height.shape
    nlat = rows * NX * NY * NC
    fwd, inv, ksq = filter_tables(nlon)
    scalars, cos_sum = row_scalars(nlat)
    tiles = RADIX // 2
    dims = (rows, levels, nlon, nlat)
    f32, bf16 = jnp.float32, jnp.bfloat16
    vmem, smem, dma = pltpu.VMEM, pltpu.SMEM, pltpu.SemaphoreType.DMA
    operands = (height, zonal, merid, rates, thresholds, flags, cutoffs, scalars, ksq, fwd, inv)
    operands = [pltpu.with_memory_space_constraint(jnp.asarray(a), pltpu.HBM) for a in operands]
    return pl.pallas_call(
        functools.partial(kernel, dims, nlon * cos_sum),
        out_shape=vmem(height.shape, f32),
        in_specs=[pl.BlockSpec(memory_space=pltpu.HBM)] * len(operands),
        out_specs=pl.BlockSpec(memory_space=vmem),
        scratch_shapes=[
            vmem(height.shape, f32), vmem(height.shape, f32), vmem(height.shape, f32),
            smem(rates.shape, f32), smem(thresholds.shape, f32), smem(flags.shape, jnp.int32),
            smem(cutoffs.shape, jnp.int32), smem(scalars.shape, f32),
            vmem(ksq.shape, f32), vmem(fwd.shape, bf16), vmem(inv.shape, bf16),
            vmem((2, 3, levels, nlon), f32), vmem((rows, levels, RADIX * HALF), f32),
            vmem((levels, nlon), f32), vmem((levels, nlon), f32), vmem((rows, 8, 2 * HALF), f32),
            vmem((tiles, 4 * levels, 2 * HALF), bf16), vmem((tiles, 2 * levels, 2 * HALF), f32),
            vmem((8, HALF), f32), vmem((NX * NC + NY, 8, HALF), f32), vmem((8, HALF), f32),
            vmem((8, HALF), f32),
            vmem((levels // 8, 8, HALF), f32), vmem((levels // 8, 8, HALF), f32),
            dma((8,)), dma((2,)), dma((2,)), dma, dma, dma, dma, dma, pltpu.SemaphoreType.REGULAR,
        ],
        compiler_params=pltpu.CompilerParams(collective_id=0, has_side_effects=True, vmem_limit_bytes=16 * 2**20),
        name="advect_filter",
    )(*operands)


def solution(mesh):
    finer = Mesh(
        mesh.devices.reshape(mesh.shape["member"], NX, NY, NC), ("member", "lat_0", "lat_1", "lat_2")
    )
    whole = P(("member", "lat_0", "lat_1", "lat_2"), None, None)
    placed = (whole, whole, whole, P("member"), P("member"), P(), P())
    return jax.shard_map(local, mesh=finer, in_specs=placed, out_specs=whole, check_vma=False)
```

```python
import functools
import math

import jax
import jax.numpy as jnp
import numpy as np
from jax import lax
from jax.experimental import pallas as pl
from jax.experimental.pallas import tpu as pltpu
from jax.sharding import Mesh
from jax.sharding import PartitionSpec as P

MESH = pl.DeviceIdType.MESH
NX, NY, NC = 8, 8, 2
RADIX = 12
HALF = 128
ROOT = math.sqrt(0.75)
LOG2E = math.log2(math.e)


def filter_tables(nlon):
    count = nlon // RADIX
    tiles = RADIX // 2
    fwd = np.zeros((tiles, 2 * HALF, 2 * HALF))
    inv = np.zeros((tiles, 2 * HALF, 2 * HALF))
    waves = np.zeros((8, 2 * HALF), np.int64)
    r = np.arange(count)

    def trig(k):
        angle = 2.0 * np.pi / nlon * ((r * k) % nlon)
        return np.cos(angle), np.sin(angle)

    def real_part(base, shift):
        lane = base
        for q in range(count // 2 + 1):
            k = RADIX * q + shift
            if k > nlon // 2:
                continue
            cos, sin = trig(k)
            weight = (1.0 if k in (0, nlon // 2) else 2.0) / nlon
            rows = slice(base, base + count)
            fwd[0, rows, lane] = cos
            inv[0, lane, rows] = cos * weight
            waves[0, lane] = k
            lane += 1
            if k not in (0, nlon // 2):
                fwd[0, rows, lane] = sin
                inv[0, lane, rows] = sin * weight
                waves[0, lane] = k
                lane += 1
        assert lane == base + count

    real_part(0, 0)
    real_part(HALF, RADIX // 2)
    for m in range(1, tiles):
        for q in range(count):
            k = RADIX * q + m
            cos, sin = trig(k)
            fwd[m, 0:count, q] = cos
            fwd[m, HALF : HALF + count, q] = -sin
            fwd[m, 0:count, HALF + q] = sin
            fwd[m, HALF : HALF + count, HALF + q] = cos
            waves[m, q] = waves[m, HALF + q] = min(k, nlon - k)
        inv[m] = fwd[m].T * (2.0 / nlon)
    inv_square = 1.0 / np.maximum(waves, 1).astype(np.float64) ** 2

    def halves(table):
        hi = table.astype(np.float32).astype(jnp.bfloat16)
        lo = (table - hi.astype(np.float64)).astype(np.float32).astype(jnp.bfloat16)
        return np.stack([hi, lo])

    return halves(fwd), halves(inv), inv_square.astype(np.float32)


def row_scalars(nlat):
    rows = np.arange(nlat)
    cos_row = np.sin(np.pi * (rows + 0.5) / nlat)
    faces = np.arange(nlat + 1)
    cos_face = np.where((faces > 0) & (faces < nlat), np.sin(np.pi * faces / nlat), 0.0)
    table = np.zeros((3 * nlat + HALF,))
    table[0:nlat] = cos_row
    table[nlat : 2 * nlat] = 1.0 / cos_row
    table[2 * nlat : 3 * nlat + 1] = cos_face / 24.0
    return table.astype(np.float32), float(np.sum(cos_row))


def twelve(e, o):
    plus, minus = e[0] + e[6], e[0] - e[6]
    e15p, e15m, e24p, e24m = e[1] + e[5], e[1] - e[5], e[2] + e[4], e[2] - e[4]
    a, b = plus + e24p, e15p + e[3]
    big, mid = ROOT * e15m, minus + 0.5 * e24m
    c, d = plus - 0.5 * e24p, 0.5 * e15p - e[3]
    even = [a + b, mid + big, c + d, minus - e24m, c - d, mid - big, a - b]
    o15p, o15m, o24p, o24m = o[0] + o[4], o[0] - o[4], o[1] + o[3], o[1] - o[3]
    f, g = 0.5 * o15p + o[2], ROOT * o24p
    s, t = ROOT * o15m, ROOT * o24m
    odd = [f + g, s + t, o15p - o[2], s - t, f - g]
    return even, odd


def product_of(exps):
    result = 1.0 + exps[0]
    for e in exps[1:]:
        result = result * (1.0 + e)
    return result


def split(x):
    hi = x.astype(jnp.bfloat16)
    return hi, (x - hi.astype(jnp.float32)).astype(jnp.bfloat16)


def kernel(
    dims, area,
    h_hbm, z_hbm, c_hbm, rates_hbm, thr_hbm, flags_hbm, cut_hbm, scal_hbm, ksq_hbm, fwd_hbm, inv_hbm,
    out,
    h, z, c, rates, thr, flags, cut, scal, ksq, fwd, inv,
    halo, base, s_lo, s_hi, factor, ymat, wmat, part, box, mean_in, own_mean, level_rates, level_thresholds,
    in_sem, halo_send, halo_recv, up_send, x_recv, y_recv, mean_send, mean_recv, low_in,
):
    rows, levels, nlon, nlat = dims
    count = nlon // RADIX
    x, y, core = lax.axis_index("lat_0"), lax.axis_index("lat_1"), lax.axis_index("lat_2")
    position = (x * NY + y) * NC + core
    total = NX * NY * NC

    order = (2, 3, 0, 1)

    def fetch(src, dst, i):
        return pltpu.make_async_copy(src, dst, in_sem.at[i])

    h_in = {r: fetch(h_hbm.at[r], h.at[r], i) for i, r in enumerate(order)}
    c_up = fetch(c_hbm.at[rows - 1], c.at[rows - 1], 4)
    c_in = fetch(c_hbm.at[pl.ds(0, rows - 1)], c.at[pl.ds(0, rows - 1)], 3)
    small_in = [fetch(rates_hbm, rates, 5), fetch(thr_hbm, thr, 6), fetch(scal_hbm, scal, 7)]
    z_in = fetch(z_hbm, z, 0)
    tables_in = [fetch(fwd_hbm, fwd, 1), fetch(inv_hbm, inv, 2)]
    factor_in = [fetch(flags_hbm, flags, 5), fetch(cut_hbm, cut, 6), fetch(ksq_hbm, ksq, 7)]
    for copy in small_in + [h_in[r] for r in order] + [c_up]:
        copy.start()

    last = total - 1
    first = position * rows
    is_root = jnp.logical_and(x == 0, core == 1)
    is_first = position == 1
    is_later_root = jnp.logical_and(is_root, y > 0)

    def along(step):
        p = lax.rem(position + total + step, total)
        return {"lat_0": p // (NY * NC), "lat_1": lax.rem(p // NC, NY), "lat_2": lax.rem(p, NC)}

    def row(k):
        return {"lat_0": jnp.int32(k // NC), "lat_1": y, "lat_2": jnp.int32(k % NC)}

    def root(k):
        return {"lat_0": jnp.int32(0), "lat_1": jnp.int32(k), "lat_2": jnp.int32(1)}

    def signal(sem, device):
        pl.semaphore_signal(sem, inc=1, device_id=device, device_id_type=MESH)

    barrier = pltpu.get_barrier_semaphore()

    @pl.when(position > 0)
    def _():
        signal(barrier, along(-1))

    @pl.when(is_root)
    def _():
        for k in range(NX * NC):
            if k != 1:
                signal(barrier, row(k))

    @pl.when(is_first)
    def _():
        for k in range(1, NY):
            signal(barrier, root(k))

    to_start = jnp.logical_and(position > 1, jnp.logical_or(y == 0, is_root))

    @pl.when(to_start)
    def _():
        signal(barrier, {"lat_0": jnp.int32(0), "lat_1": jnp.int32(0), "lat_2": jnp.int32(0)})

    greeted = jnp.where(is_first, 0, 1) + jnp.where(position < last, 1, 0)
    greeted = greeted + jnp.where(position == 0, NX * NC - 2 + NY - 1, 0)
    pl.semaphore_wait(barrier, greeted)

    @pl.when(position < last)
    def _():
        signal(low_in, along(1))

    def landed(ref, sem):
        pltpu.make_async_copy(ref, ref, sem).wait()

    def halo_copy(side, field, from_hbm=False):
        step, h_row, c_row = ((1, rows - 2, rows - 1), (-1, 0, 0))[side]
        src = (c_hbm if from_hbm else c).at[c_row] if field == 2 else h.at[h_row + field]
        return pltpu.make_async_remote_copy(
            src, halo.at[side, field], halo_send.at[side], halo_recv.at[side], device_id=along(step), device_id_type=MESH
        )

    @pl.when(core == 0)
    def _():
        halo_copy(0, 2, from_hbm=True).start()

    own_mean[...] = jnp.zeros_like(own_mean)

    @pl.when(jnp.logical_and(y > 0, jnp.logical_not(is_root)))
    def _():
        mean_in[1] = jnp.zeros_like(mean_in[1])

    base[:, :, nlon:] = jnp.zeros((rows, levels, base.shape[2] - nlon), jnp.float32)

    @pl.when(position == 0)
    def _():
        halo[0] = jnp.zeros_like(halo[0])

    @pl.when(position == last)
    def _():
        halo[1] = jnp.zeros_like(halo[1])

    for copy in small_in:
        copy.wait()

    for field in (0, 1):
        h_in[rows - 2 + field].wait()

        @pl.when(core == 0)
        def _():
            halo_copy(0, field).start()

    lane = lax.broadcasted_iota(jnp.int32, (8, HALF), 1)
    tile = jnp.zeros((8, HALF), jnp.float32)
    sub = lax.broadcasted_iota(jnp.int32, (8, 1), 0)

    def levels_of(ref, start):
        value = jnp.zeros((8, 1), jnp.float32)
        for k in range(8):
            value = jnp.where(sub == k, ref[start + k], value)
        return value

    full = nlon // HALF
    groups = range(levels // 8)
    rate_of = [levels_of(rates, 8 * g) for g in groups]
    threshold_of = [levels_of(thr, 8 * g) for g in groups]
    scaled_threshold = [LOG2E * value for value in threshold_of]
    wide, rest = [0.0 for g in groups], [0.0 for g in groups]
    for r in order:
        if r < 2:
            h_in[r].wait()
        for g in groups:
            lev = pl.ds(8 * g, 8)
            exps = [
                jnp.exp2(h[r, lev, HALF * j : HALF * (j + 1)] * LOG2E - scaled_threshold[g]) for j in range(full)
            ]
            logs = jnp.log2(product_of(exps[0:6])) + jnp.log2(product_of(exps[6:full]))
            wide[g] = wide[g] + scal[first + r] * logs
            logs = jnp.log2(1.0 + jnp.exp2(h[r, lev, HALF * full : nlon] * LOG2E - scaled_threshold[g]))
            rest[g] = rest[g] + scal[first + r] * logs
    short = jnp.zeros((8, HALF * (full + 1) - nlon), jnp.float32)
    for g in groups:
        sums = jnp.sum(wide[g] + jnp.concatenate([rest[g], short], axis=1), axis=1, keepdims=True)
        tile = jnp.where(lane == g, (-1.0 / LOG2E) * rate_of[g] * sums, tile)
        level_rates[g] = jnp.broadcast_to(rate_of[g], (8, HALF))
        level_thresholds[g] = jnp.broadcast_to(threshold_of[g], (8, HALF))
    part[...] = tile

    members = [*range(NC, NX * NC), 0]

    def mean_copy(slot, source, device):
        return pltpu.make_async_remote_copy(
            source, mean_in.at[slot], mean_send, mean_recv, device_id=device, device_id_type=MESH
        )

    def send_b(device):
        mean_copy(1, part, device).start()

    def part_copy(slot):
        return pltpu.make_async_remote_copy(
            part, box.at[slot], up_send, x_recv, device_id=row(1), device_id_type=MESH
        )

    sends_part = jnp.logical_and(jnp.logical_not(is_root), position > 0)

    @pl.when(sends_part)
    def _():
        part_copy(x * NC + core).start()

    @pl.when(position == 0)
    def _():
        mean_in[1] = part[...]
        send_b(row(1))
        for k in range(1, NY):
            for member in members[2 * k - 2 : 2 * k]:
                send_b(row(member))
            send_b(root(k))

    for copy in [c_in, z_in] + factor_in + tables_in:
        copy.start()

    z_in.wait()
    c_up.wait()
    c_in.wait()

    @pl.when(jnp.logical_and(core != 0, position < last))
    def _():
        for field in range(3):
            halo_copy(0, field).start()


    def inv_cos(r):
        return scal[nlat + first + r]

    def face(f):
        return scal[2 * nlat + first + f]

    def west(a):
        return pltpu.roll(a, 1, axis=1)

    def east(a):
        return pltpu.roll(a, nlon - 1, axis=1)

    def local_terms(g, carry):
        lev = pl.ds(pl.multiple_of(8 * g, 8), 8)
        hr = [h[r, lev, :] for r in range(rows)]
        rate, threshold = level_rates[g][:, 0:1], level_thresholds[g][:, 0:1]
        cr = [c[r, lev, :] for r in range(rows)]
        low = face(1) * (cr[0] + cr[1])
        high = face(3) * (cr[2] + cr[3])
        s_lo[lev, :] = low
        s_hi[lev, :] = high
        f1 = low * (7.0 * (hr[0] + hr[1]) - hr[2])
        f2 = face(2) * (cr[1] + cr[2]) * (7.0 * (hr[1] + hr[2]) - (hr[0] + hr[3]))
        f3 = high * (7.0 * (hr[2] + hr[3]) - hr[1])
        terms = [f1, f2 - f1, f3 - f2, -f3]
        for r in range(rows):
            pair = hr[r] + east(hr[r])
            zr = z[r, lev, :]
            speed = zr + east(zr)
            flux = speed * (8.0 * pair - (west(pair) + east(pair))) * (1.0 / 24.0)
            s = hr[r] - threshold
            source = rate * jnp.log(1.0 + jnp.exp(s))
            base[r, lev, 0:nlon] = (hr[r] - source) - (flux - west(flux)) - terms[r] * inv_cos(r)
        return carry

    lax.fori_loop(0, levels // 8, local_terms, 0)

    @pl.when(position > 0)
    def _():
        pl.semaphore_wait(low_in, 1)
        for field in range(3):
            halo_copy(1, field).start()

    for copy in factor_in:
        copy.wait()
    for r in range(rows):
        cutoff = cut[first + r].astype(jnp.float32)
        flag = flags[first + r].astype(jnp.float32)
        factor[r] = flag * (1.0 - jnp.minimum(1.0, cutoff * cutoff * ksq[...]))

    def sum_copy():
        return pltpu.make_async_remote_copy(
            part, box.at[NX * NC + y], up_send, y_recv, device_id=root(0), device_id_type=MESH
        )

    def gather_row(senders):
        landed(box.at[pl.ds(0, len(senders))], x_recv)
        acc = part[...]
        for k in senders:
            acc = acc + box[k]
        return acc

    @pl.when(is_later_root)
    def _():
        part[...] = gather_row(members)
        sum_copy().start()

    for copy in tables_in:
        copy.wait()
    lanes = lax.broadcasted_iota(jnp.int32, (16, HALF), 1)
    units = 2 * levels
    blocks = levels // 16

    tail = nlon - HALF * (RADIX - 1)

    def piece(ref, j):
        if j < RADIX - 1:
            return ref[:, HALF * j : HALF * (j + 1)]
        return jnp.concatenate([ref[:, HALF * j : nlon], jnp.zeros((16, HALF - tail), jnp.float32)], axis=1)

    def with_halo(r, lev, j):
        side, near, far, edge, inner, f, through, outer = (
            (0, 1, 0, 0, 1, 0, s_lo, 0) if r < 2 else (1, 0, 1, rows - 1, rows - 2, rows, s_hi, rows - 1)
        )
        beside = piece(halo.at[side, near, lev], j)
        term = piece(through.at[lev], j) * beside
        if r == outer:
            speed = face(f) * (piece(halo.at[side, 2, lev], j) + piece(c.at[edge, lev], j))
            flux = speed * (
                7.0 * (beside + piece(h.at[edge, lev], j)) - (piece(halo.at[side, far, lev], j) + piece(h.at[inner, lev], j))
            )
            term = term + flux
        sign = 1.0 if r in (0, 2) else -1.0
        return base[r, lev, HALF * j : HALF * (j + 1)] + term * (sign * inv_cos(r))

    def product(hilo, table):
        first_part = jnp.dot(hilo, table[0], preferred_element_type=jnp.float32)
        second = jnp.dot(hilo[0:units], table[1], preferred_element_type=jnp.float32)
        return first_part[0:units] + first_part[units : 2 * units] + second

    def filter_rows(row0, shifts=None):
        def block_of(b):
            return row0 + b // blocks, pl.ds(16 * (b % blocks), 16), pl.ds(16 * b, 16), pl.ds(units + 16 * b, 16)

        def forward(b):
            r, lev, at_hi, at_lo = block_of(b)
            v = [with_halo(r, lev, j) for j in range(RADIX)]
            for j in range(RADIX):
                base[r, lev, HALF * j : HALF * (j + 1)] = v[j]
            u = [v[0]] + [
                pltpu.roll(jnp.where(lanes >= HALF - 8 * j, v[j - 1], v[j]), 8 * j, axis=1) for j in range(1, RADIX)
            ]
            e = [u[0]] + [u[j] + u[RADIX - j] for j in range(1, 6)] + [u[6]]
            o = [u[j] - u[RADIX - j] for j in range(1, 6)]
            even, odd = twelve(e, o)
            halves = [(even[0], even[6])] + [(even[m], odd[m - 1]) for m in range(1, 6)]
            for m, pair in enumerate(halves):
                for k, value in enumerate(pair):
                    hi, lo = split(value)
                    ymat[m, at_hi, HALF * k : HALF * (k + 1)] = hi
                    ymat[m, at_lo, HALF * k : HALF * (k + 1)] = lo

        def backward(b):
            r, lev, at, _ = block_of(b)
            w = [[wmat[m, at, HALF * k : HALF * (k + 1)] for k in range(2)] for m in range(RADIX // 2)]
            even, odd = twelve([w[0][0]] + [w[m][0] for m in range(1, 6)] + [w[0][1]], [w[m][1] for m in range(1, 6)])
            removed = [even[0]] + [even[j] + odd[j - 1] for j in range(1, 6)] + [even[6]]
            removed += [even[RADIX - j] - odd[RADIX - j - 1] for j in range(7, RADIX)]
            back = [removed[0]] + [pltpu.roll(removed[j], HALF - 8 * j, axis=1) for j in range(1, RADIX)]
            for j in range(RADIX):
                kept = base[r, lev, HALF * j : HALF * (j + 1)]
                if row0 == 0:
                    kept = kept - shifts[b % blocks]
                if j < RADIX - 1:
                    out[r, lev, HALF * j : HALF * (j + 1)] = kept - jnp.where(lanes < count - 8 * j, back[j], back[j + 1])
                else:
                    out[r, lev, HALF * j : nlon] = (kept - back[j])[:, 0:tail]

        for b in range(2 * blocks):
            forward(b)
        for m in range(RADIX // 2):
            waves = product(ymat[m], (fwd[0, m], fwd[1, m]))
            scaled = jnp.concatenate(
                [waves[r * levels : (r + 1) * levels] * factor[row0 + r, m : m + 1, :] for r in range(2)], axis=0
            )
            wmat[m] = product(jnp.concatenate(split(scaled), axis=0), (inv[0, m], inv[1, m]))
        if row0 == 0:
            for r in (2, 3):
                for b in range(blocks):
                    lev = pl.ds(16 * b, 16)
                    out[r, lev, :] = out[r, lev, :] - shifts[b]
        for b in range(2 * blocks):
            backward(b)

    @pl.when(position < last)
    def _():
        landed(halo.at[1], halo_recv.at[1])

    filter_rows(2)

    @pl.when(is_first)
    def _():
        landed(box.at[pl.ds(NX * NC + 1, NY - 1)], y_recv)
        acc = box[NX * NC + 1]
        for k in range(2, NY):
            acc = acc + box[NX * NC + k]
        mean_in[0] = gather_row(members[:-1]) + acc
        for k in range(1, NY):
            for member in members[2 * k - 2 : 2 * k]:
                mean_copy(0, mean_in.at[0], row(member)).start()
            mean_copy(0, mean_in.at[0], root(k)).start()
        mean_copy(0, mean_in.at[0], row(0)).start()

    @pl.when(position > 0)
    def _():
        landed(halo.at[0], halo_recv.at[0])

    @pl.when(is_first)
    def _():
        landed(mean_in.at[1], mean_recv)
        own_mean[...] = (mean_in[0] + mean_in[1]) * (1.0 / area)

    def mean_columns(value):
        return [jnp.sum(jnp.where(lane == g, value, 0.0), axis=1, keepdims=True) for g in groups]

    columns = mean_columns(own_mean[...])
    shifts = [jnp.concatenate(columns[2 * b : 2 * b + 2], axis=0) for b in range(blocks)]
    filter_rows(0, shifts)

    in_two = jnp.logical_or(is_later_root, jnp.logical_and(y == 0, position > 1))

    @pl.when(in_two)
    def _():
        landed(mean_in, mean_recv)

    @pl.when(jnp.logical_not(jnp.logical_or(in_two, is_first)))
    def _():
        landed(mean_in.at[0], mean_recv)

    @pl.when(is_later_root)
    def _():
        own_mean[...] = mean_in[0] + mean_in[1]
        for member in members:
            mean_copy(0, own_mean, row(member)).start()

    @pl.when(jnp.logical_not(is_first))
    def _():
        for g, shift in zip(groups, mean_columns((mean_in[0] + mean_in[1]) * (1.0 / area))):
            lev = pl.ds(8 * g, 8)
            for r in range(rows):
                out[r, lev, :] = out[r, lev, :] - shift

    for side, sender in ((0, position < last), (1, position > 0)):

        @pl.when(sender)
        def _():
            landed(halo.at[side], halo_send.at[side])

    @pl.when(position <= 1)
    def _():
        landed(box.at[pl.ds(0, len(members) + NY - 1)], mean_send)

    @pl.when(is_later_root)
    def _():
        landed(box.at[pl.ds(0, len(members))], mean_send)

    @pl.when(position > 1)
    def _():
        landed(part, up_send)


def local(height, zonal, merid, rates, thresholds, flags, cutoffs):
    rows, levels, nlon = height.shape
    nlat = rows * NX * NY * NC
    fwd, inv, ksq = filter_tables(nlon)
    scalars, cos_sum = row_scalars(nlat)
    tiles = RADIX // 2
    dims = (rows, levels, nlon, nlat)
    f32, bf16 = jnp.float32, jnp.bfloat16
    vmem, smem, dma = pltpu.VMEM, pltpu.SMEM, pltpu.SemaphoreType.DMA
    operands = (height, zonal, merid, rates, thresholds, flags, cutoffs, scalars, ksq, fwd, inv)
    operands = [pltpu.with_memory_space_constraint(jnp.asarray(a), pltpu.HBM) for a in operands]
    return pl.pallas_call(
        functools.partial(kernel, dims, nlon * cos_sum),
        out_shape=vmem(height.shape, f32),
        in_specs=[pl.BlockSpec(memory_space=pltpu.HBM)] * len(operands),
        out_specs=pl.BlockSpec(memory_space=vmem),
        scratch_shapes=[
            vmem(height.shape, f32), vmem(height.shape, f32), vmem(height.shape, f32),
            smem(rates.shape, f32), smem(thresholds.shape, f32), smem(flags.shape, jnp.int32),
            smem(cutoffs.shape, jnp.int32), smem(scalars.shape, f32),
            vmem(ksq.shape, f32), vmem(fwd.shape, bf16), vmem(inv.shape, bf16),
            vmem((2, 3, levels, nlon), f32), vmem((rows, levels, RADIX * HALF), f32),
            vmem((levels, nlon), f32), vmem((levels, nlon), f32), vmem((rows, 8, 2 * HALF), f32),
            vmem((tiles, 4 * levels, 2 * HALF), bf16), vmem((tiles, 2 * levels, 2 * HALF), f32),
            vmem((8, HALF), f32), vmem((NX * NC + NY, 8, HALF), f32), vmem((2, 8, HALF), f32),
            vmem((8, HALF), f32),
            vmem((levels // 8, 8, HALF), f32), vmem((levels // 8, 8, HALF), f32),
            dma((8,)), dma((2,)), dma((2,)), dma, dma, dma, dma, dma, pltpu.SemaphoreType.REGULAR,
        ],
        compiler_params=pltpu.CompilerParams(collective_id=0, has_side_effects=True, vmem_limit_bytes=16 * 2**20),
        name="advect_filter",
    )(*operands)


def solution(mesh):
    finer = Mesh(
        mesh.devices.reshape(mesh.shape["member"], NX, NY, NC), ("member", "lat_0", "lat_1", "lat_2")
    )
    whole = P(("member", "lat_0", "lat_1", "lat_2"), None, None)
    placed = (whole, whole, whole, P("member"), P("member"), P(), P())
    return jax.shard_map(local, mesh=finer, in_specs=placed, out_specs=whole, check_vma=False)
```

```python
import functools
import math

import jax
import jax.numpy as jnp
import numpy as np
from jax import lax
from jax.experimental import pallas as pl
from jax.experimental.pallas import tpu as pltpu
from jax.sharding import Mesh
from jax.sharding import PartitionSpec as P

MESH = pl.DeviceIdType.MESH
NX, NY, NC = 8, 8, 2
PIECES = 2
RADIX = 12
HALF = 128
ROOT = math.sqrt(0.75)
LOG2E = math.log2(math.e)


def filter_tables(nlon):
    count = nlon // RADIX
    tiles = RADIX // 2
    fwd = np.zeros((tiles, 2 * HALF, 2 * HALF))
    inv = np.zeros((tiles, 2 * HALF, 2 * HALF))
    waves = np.zeros((8, 2 * HALF), np.int64)
    r = np.arange(count)

    def trig(k):
        angle = 2.0 * np.pi / nlon * ((r * k) % nlon)
        return np.cos(angle), np.sin(angle)

    def real_part(base, shift):
        lane = base
        for q in range(count // 2 + 1):
            k = RADIX * q + shift
            if k > nlon // 2:
                continue
            cos, sin = trig(k)
            weight = (1.0 if k in (0, nlon // 2) else 2.0) / nlon
            rows = slice(base, base + count)
            fwd[0, rows, lane] = cos
            inv[0, lane, rows] = cos * weight
            waves[0, lane] = k
            lane += 1
            if k not in (0, nlon // 2):
                fwd[0, rows, lane] = sin
                inv[0, lane, rows] = sin * weight
                waves[0, lane] = k
                lane += 1
        assert lane == base + count

    real_part(0, 0)
    real_part(HALF, RADIX // 2)
    for m in range(1, tiles):
        for q in range(count):
            k = RADIX * q + m
            cos, sin = trig(k)
            fwd[m, 0:count, q] = cos
            fwd[m, HALF : HALF + count, q] = -sin
            fwd[m, 0:count, HALF + q] = sin
            fwd[m, HALF : HALF + count, HALF + q] = cos
            waves[m, q] = waves[m, HALF + q] = min(k, nlon - k)
        inv[m] = fwd[m].T * (2.0 / nlon)
    inv_square = 1.0 / np.maximum(waves, 1).astype(np.float64) ** 2

    def halves(table):
        hi = table.astype(np.float32).astype(jnp.bfloat16)
        lo = (table - hi.astype(np.float64)).astype(np.float32).astype(jnp.bfloat16)
        return np.stack([hi, lo])

    return halves(fwd), halves(inv), inv_square.astype(np.float32)


def row_scalars(nlat):
    rows = np.arange(nlat)
    cos_row = np.sin(np.pi * (rows + 0.5) / nlat)
    faces = np.arange(nlat + 1)
    cos_face = np.where((faces > 0) & (faces < nlat), np.sin(np.pi * faces / nlat), 0.0)
    table = np.zeros((3 * nlat + HALF,))
    table[0:nlat] = cos_row
    table[nlat : 2 * nlat] = 1.0 / cos_row
    table[2 * nlat : 3 * nlat + 1] = cos_face / 24.0
    return table.astype(np.float32), float(np.sum(cos_row))


def twelve(e, o):
    plus, minus = e[0] + e[6], e[0] - e[6]
    e15p, e15m, e24p, e24m = e[1] + e[5], e[1] - e[5], e[2] + e[4], e[2] - e[4]
    a, b = plus + e24p, e15p + e[3]
    big, mid = ROOT * e15m, minus + 0.5 * e24m
    c, d = plus - 0.5 * e24p, 0.5 * e15p - e[3]
    even = [a + b, mid + big, c + d, minus - e24m, c - d, mid - big, a - b]
    o15p, o15m, o24p, o24m = o[0] + o[4], o[0] - o[4], o[1] + o[3], o[1] - o[3]
    f, g = 0.5 * o15p + o[2], ROOT * o24p
    s, t = ROOT * o15m, ROOT * o24m
    odd = [f + g, s + t, o15p - o[2], s - t, f - g]
    return even, odd


def product_of(exps):
    result = 1.0 + exps[0]
    for e in exps[1:]:
        result = result * (1.0 + e)
    return result


def split(x):
    hi = x.astype(jnp.bfloat16)
    return hi, (x - hi.astype(jnp.float32)).astype(jnp.bfloat16)


def kernel(
    dims, area,
    h_hbm, z_hbm, c_hbm, rates_hbm, thr_hbm, flags_hbm, cut_hbm, scal_hbm, ksq_hbm, fwd_hbm, inv_hbm,
    out,
    h, z, c, rates, thr, flags, cut, scal, ksq, fwd, inv,
    halo, base, s_lo, s_hi, factor, ymat, wmat, part, box, mean_in, own_mean, level_rates, level_thresholds,
    in_sem, halo_send, halo_recv, up_send, x_recv, y_recv, mean_send, mean_recv, low_in,
):
    rows, levels, nlon, nlat = dims
    count = nlon // RADIX
    x, y, core = lax.axis_index("lat_0"), lax.axis_index("lat_1"), lax.axis_index("lat_2")
    position = (x * NY + y) * NC + core
    total = NX * NY * NC

    order = (2, 3, 0, 1)
    cut_at = levels // PIECES
    pieces = [pl.ds(cut_at * i, cut_at) for i in range(PIECES)]

    def fetch(src, dst, i):
        return pltpu.make_async_copy(src, dst, in_sem.at[i])

    up_in = [[fetch(h_hbm.at[r, p], h.at[r, p], PIECES * (r - 2) + i) for i, p in enumerate(pieces)] for r in (2, 3)]
    low_rows = fetch(h_hbm.at[pl.ds(0, 2)], h.at[pl.ds(0, 2)], 2 * PIECES)
    c_up = fetch(c_hbm.at[rows - 1], c.at[rows - 1], 2 * PIECES + 1)
    small_in = [fetch(src, dst, 2 * PIECES + 2 + i) for i, (src, dst) in enumerate(((rates_hbm, rates), (thr_hbm, thr), (scal_hbm, scal)))]
    z_in = fetch(z_hbm, z, 0)
    c_in = fetch(c_hbm.at[pl.ds(0, rows - 1)], c.at[pl.ds(0, rows - 1)], 2 * PIECES)
    tables_in = [fetch(fwd_hbm, fwd, 1), fetch(inv_hbm, inv, 2)]
    factor_in = [
        fetch(src, dst, 2 * PIECES + 2 + i) for i, (src, dst) in enumerate(((flags_hbm, flags), (cut_hbm, cut), (ksq_hbm, ksq)))
    ]
    for copy in small_in + up_in[0] + up_in[1] + [low_rows, c_up]:
        copy.start()

    last = total - 1
    first = position * rows
    is_root = jnp.logical_and(x == 0, core == 1)
    is_first = position == 1
    is_later_root = jnp.logical_and(is_root, y > 0)

    def along(step):
        p = lax.rem(position + total + step, total)
        return {"lat_0": p // (NY * NC), "lat_1": lax.rem(p // NC, NY), "lat_2": lax.rem(p, NC)}

    def row(k):
        return {"lat_0": jnp.int32(k // NC), "lat_1": y, "lat_2": jnp.int32(k % NC)}

    def root(k):
        return {"lat_0": jnp.int32(0), "lat_1": jnp.int32(k), "lat_2": jnp.int32(1)}

    def signal(sem, device):
        pl.semaphore_signal(sem, inc=1, device_id=device, device_id_type=MESH)

    barrier = pltpu.get_barrier_semaphore()

    @pl.when(position > 0)
    def _():
        signal(barrier, along(-1))

    @pl.when(is_root)
    def _():
        for k in range(NX * NC):
            if k != 1:
                signal(barrier, row(k))

    @pl.when(is_first)
    def _():
        for k in range(1, NY):
            signal(barrier, root(k))

    to_start = jnp.logical_and(position > 1, jnp.logical_or(y == 0, is_root))

    @pl.when(to_start)
    def _():
        signal(barrier, {"lat_0": jnp.int32(0), "lat_1": jnp.int32(0), "lat_2": jnp.int32(0)})

    greeted = jnp.where(is_first, 0, 1) + jnp.where(position < last, 1, 0)
    greeted = greeted + jnp.where(position == 0, NX * NC - 2 + NY - 1, 0)
    pl.semaphore_wait(barrier, greeted)

    @pl.when(position < last)
    def _():
        signal(low_in, along(1))

    def landed(ref, sem):
        pltpu.make_async_copy(ref, ref, sem).wait()

    def halo_copy(side, field, levs=slice(None)):
        step, h_row, c_row = ((1, rows - 2, rows - 1), (-1, 0, 0))[side]
        src = c.at[c_row, levs] if field == 2 else h.at[h_row + field, levs]
        return pltpu.make_async_remote_copy(
            src, halo.at[side, field, levs], halo_send.at[side], halo_recv.at[side],
            device_id=along(step), device_id_type=MESH,
        )

    own_mean[...] = jnp.zeros_like(own_mean)

    @pl.when(jnp.logical_and(y > 0, jnp.logical_not(is_root)))
    def _():
        mean_in[1] = jnp.zeros_like(mean_in[1])

    base[:, :, nlon:] = jnp.zeros((rows, levels, base.shape[2] - nlon), jnp.float32)

    @pl.when(position == 0)
    def _():
        halo[0] = jnp.zeros_like(halo[0])

    @pl.when(position == last)
    def _():
        halo[1] = jnp.zeros_like(halo[1])

    for field in (0, 1):
        for arrived, levs in zip(up_in[field], pieces):
            arrived.wait()

            @pl.when(core == 0)
            def _():
                halo_copy(0, field, levs).start()

    for copy in small_in:
        copy.wait()

    lane = lax.broadcasted_iota(jnp.int32, (8, HALF), 1)
    tile = jnp.zeros((8, HALF), jnp.float32)
    sub = lax.broadcasted_iota(jnp.int32, (8, 1), 0)

    def levels_of(ref, start):
        value = jnp.zeros((8, 1), jnp.float32)
        for k in range(8):
            value = jnp.where(sub == k, ref[start + k], value)
        return value

    full = nlon // HALF
    groups = range(levels // 8)
    rate_of = [levels_of(rates, 8 * g) for g in groups]
    threshold_of = [levels_of(thr, 8 * g) for g in groups]
    scaled_threshold = [LOG2E * value for value in threshold_of]
    wide, rest = [0.0 for g in groups], [0.0 for g in groups]
    for r in order:
        if r == 0:
            low_rows.wait()
        for g in groups:
            lev = pl.ds(8 * g, 8)
            exps = [
                jnp.exp2(h[r, lev, HALF * j : HALF * (j + 1)] * LOG2E - scaled_threshold[g]) for j in range(full)
            ]
            logs = jnp.log2(product_of(exps[0:6])) + jnp.log2(product_of(exps[6:full]))
            wide[g] = wide[g] + scal[first + r] * logs
            logs = jnp.log2(1.0 + jnp.exp2(h[r, lev, HALF * full : nlon] * LOG2E - scaled_threshold[g]))
            rest[g] = rest[g] + scal[first + r] * logs
    short = jnp.zeros((8, HALF * (full + 1) - nlon), jnp.float32)
    for g in groups:
        sums = jnp.sum(wide[g] + jnp.concatenate([rest[g], short], axis=1), axis=1, keepdims=True)
        tile = jnp.where(lane == g, (-1.0 / LOG2E) * rate_of[g] * sums, tile)
        level_rates[g] = jnp.broadcast_to(rate_of[g], (8, HALF))
        level_thresholds[g] = jnp.broadcast_to(threshold_of[g], (8, HALF))
    part[...] = tile

    members = [*range(NC, NX * NC), 0]

    def mean_copy(slot, source, device):
        return pltpu.make_async_remote_copy(
            source, mean_in.at[slot], mean_send, mean_recv, device_id=device, device_id_type=MESH
        )

    def send_b(device):
        mean_copy(1, part, device).start()

    def part_copy(slot):
        return pltpu.make_async_remote_copy(
            part, box.at[slot], up_send, x_recv, device_id=row(1), device_id_type=MESH
        )

    sends_part = jnp.logical_and(jnp.logical_not(is_root), position > 0)

    @pl.when(sends_part)
    def _():
        part_copy(x * NC + core).start()

    @pl.when(position == 0)
    def _():
        send_b(row(1))

    c_up.wait()

    @pl.when(jnp.logical_and(core != 0, position < last))
    def _():
        halo_copy(0, 0).start()
        halo_copy(0, 1).start()

    @pl.when(position < last)
    def _():
        halo_copy(0, 2).start()

    @pl.when(position == 0)
    def _():
        mean_in[1] = part[...]
        for k in range(1, NY):
            for member in members[2 * k - 2 : 2 * k]:
                send_b(row(member))
            send_b(root(k))

    for copy in [c_in, z_in] + factor_in + tables_in:
        copy.start()

    z_in.wait()
    c_in.wait()


    def inv_cos(r):
        return scal[nlat + first + r]

    def face(f):
        return scal[2 * nlat + first + f]

    def west(a):
        return pltpu.roll(a, 1, axis=1)

    def east(a):
        return pltpu.roll(a, nlon - 1, axis=1)

    def local_terms(g, carry):
        lev = pl.ds(pl.multiple_of(8 * g, 8), 8)
        hr = [h[r, lev, :] for r in range(rows)]
        rate, threshold = level_rates[g][:, 0:1], level_thresholds[g][:, 0:1]
        cr = [c[r, lev, :] for r in range(rows)]
        low = face(1) * (cr[0] + cr[1])
        high = face(3) * (cr[2] + cr[3])
        s_lo[lev, :] = low
        s_hi[lev, :] = high
        f1 = low * (7.0 * (hr[0] + hr[1]) - hr[2])
        f2 = face(2) * (cr[1] + cr[2]) * (7.0 * (hr[1] + hr[2]) - (hr[0] + hr[3]))
        f3 = high * (7.0 * (hr[2] + hr[3]) - hr[1])
        terms = [f1, f2 - f1, f3 - f2, -f3]
        for r in range(rows):
            pair = hr[r] + east(hr[r])
            zr = z[r, lev, :]
            speed = zr + east(zr)
            flux = speed * (8.0 * pair - (west(pair) + east(pair))) * (1.0 / 24.0)
            s = hr[r] - threshold
            source = rate * jnp.log(1.0 + jnp.exp(s))
            base[r, lev, 0:nlon] = (hr[r] - source) - (flux - west(flux)) - terms[r] * inv_cos(r)
        return carry

    lax.fori_loop(0, levels // 8, local_terms, 0)

    @pl.when(position > 0)
    def _():
        pl.semaphore_wait(low_in, 1)
        for field in range(3):
            halo_copy(1, field).start()

    for copy in factor_in:
        copy.wait()
    for r in range(rows):
        cutoff = cut[first + r].astype(jnp.float32)
        flag = flags[first + r].astype(jnp.float32)
        factor[r] = flag * (1.0 - jnp.minimum(1.0, cutoff * cutoff * ksq[...]))

    def sum_copy():
        return pltpu.make_async_remote_copy(
            part, box.at[NX * NC + y], up_send, y_recv, device_id=root(0), device_id_type=MESH
        )

    def gather_row(senders):
        landed(box.at[pl.ds(0, len(senders))], x_recv)
        acc = part[...]
        for k in senders:
            acc = acc + box[k]
        return acc

    @pl.when(is_later_root)
    def _():
        part[...] = gather_row(members)
        sum_copy().start()

    for copy in tables_in:
        copy.wait()
    lanes = lax.broadcasted_iota(jnp.int32, (16, HALF), 1)
    units = 2 * levels
    blocks = levels // 16

    tail = nlon - HALF * (RADIX - 1)

    def piece(ref, j):
        if j < RADIX - 1:
            return ref[:, HALF * j : HALF * (j + 1)]
        return jnp.concatenate([ref[:, HALF * j : nlon], jnp.zeros((16, HALF - tail), jnp.float32)], axis=1)

    def with_halo(r, lev, j):
        side, near, far, edge, inner, f, through, outer = (
            (0, 1, 0, 0, 1, 0, s_lo, 0) if r < 2 else (1, 0, 1, rows - 1, rows - 2, rows, s_hi, rows - 1)
        )
        beside = piece(halo.at[side, near, lev], j)
        term = piece(through.at[lev], j) * beside
        if r == outer:
            speed = face(f) * (piece(halo.at[side, 2, lev], j) + piece(c.at[edge, lev], j))
            flux = speed * (
                7.0 * (beside + piece(h.at[edge, lev], j)) - (piece(halo.at[side, far, lev], j) + piece(h.at[inner, lev], j))
            )
            term = term + flux
        sign = 1.0 if r in (0, 2) else -1.0
        return base[r, lev, HALF * j : HALF * (j + 1)] + term * (sign * inv_cos(r))

    def product(hilo, table):
        first_part = jnp.dot(hilo, table[0], preferred_element_type=jnp.float32)
        second = jnp.dot(hilo[0:units], table[1], preferred_element_type=jnp.float32)
        return first_part[0:units] + first_part[units : 2 * units] + second

    def filter_rows(row0, shifts=None):
        def block_of(b):
            return row0 + b // blocks, pl.ds(16 * (b % blocks), 16), pl.ds(16 * b, 16), pl.ds(units + 16 * b, 16)

        def forward(b):
            r, lev, at_hi, at_lo = block_of(b)
            v = [with_halo(r, lev, j) for j in range(RADIX)]
            for j in range(RADIX):
                base[r, lev, HALF * j : HALF * (j + 1)] = v[j]
            u = [v[0]] + [
                pltpu.roll(jnp.where(lanes >= HALF - 8 * j, v[j - 1], v[j]), 8 * j, axis=1) for j in range(1, RADIX)
            ]
            e = [u[0]] + [u[j] + u[RADIX - j] for j in range(1, 6)] + [u[6]]
            o = [u[j] - u[RADIX - j] for j in range(1, 6)]
            even, odd = twelve(e, o)
            halves = [(even[0], even[6])] + [(even[m], odd[m - 1]) for m in range(1, 6)]
            for m, pair in enumerate(halves):
                for k, value in enumerate(pair):
                    hi, lo = split(value)
                    ymat[m, at_hi, HALF * k : HALF * (k + 1)] = hi
                    ymat[m, at_lo, HALF * k : HALF * (k + 1)] = lo

        def backward(b):
            r, lev, at, _ = block_of(b)
            w = [[wmat[m, at, HALF * k : HALF * (k + 1)] for k in range(2)] for m in range(RADIX // 2)]
            even, odd = twelve([w[0][0]] + [w[m][0] for m in range(1, 6)] + [w[0][1]], [w[m][1] for m in range(1, 6)])
            removed = [even[0]] + [even[j] + odd[j - 1] for j in range(1, 6)] + [even[6]]
            removed += [even[RADIX - j] - odd[RADIX - j - 1] for j in range(7, RADIX)]
            back = [removed[0]] + [pltpu.roll(removed[j], HALF - 8 * j, axis=1) for j in range(1, RADIX)]
            for j in range(RADIX):
                kept = base[r, lev, HALF * j : HALF * (j + 1)]
                if row0 == 0:
                    kept = kept - shifts[b % blocks]
                if j < RADIX - 1:
                    out[r, lev, HALF * j : HALF * (j + 1)] = kept - jnp.where(lanes < count - 8 * j, back[j], back[j + 1])
                else:
                    out[r, lev, HALF * j : nlon] = (kept - back[j])[:, 0:tail]

        for b in range(2 * blocks):
            forward(b)
        for m in range(RADIX // 2):
            waves = product(ymat[m], (fwd[0, m], fwd[1, m]))
            scaled = jnp.concatenate(
                [waves[r * levels : (r + 1) * levels] * factor[row0 + r, m : m + 1, :] for r in range(2)], axis=0
            )
            wmat[m] = product(jnp.concatenate(split(scaled), axis=0), (inv[0, m], inv[1, m]))
        if row0 == 0:
            for r in (2, 3):
                for b in range(blocks):
                    lev = pl.ds(16 * b, 16)
                    out[r, lev, :] = out[r, lev, :] - shifts[b]
        for b in range(2 * blocks):
            backward(b)

    @pl.when(position < last)
    def _():
        landed(halo.at[1], halo_recv.at[1])

    filter_rows(2)

    @pl.when(is_first)
    def _():
        landed(box.at[pl.ds(NX * NC + 1, NY - 1)], y_recv)
        acc = box[NX * NC + 1]
        for k in range(2, NY):
            acc = acc + box[NX * NC + k]
        mean_in[0] = gather_row(members[:-1]) + acc
        for k in range(1, NY):
            for member in members[2 * k - 2 : 2 * k]:
                mean_copy(0, mean_in.at[0], row(member)).start()
            mean_copy(0, mean_in.at[0], root(k)).start()
        mean_copy(0, mean_in.at[0], row(0)).start()

    @pl.when(position > 0)
    def _():
        landed(halo.at[0], halo_recv.at[0])

    @pl.when(is_first)
    def _():
        landed(mean_in.at[1], mean_recv)
        own_mean[...] = (mean_in[0] + mean_in[1]) * (1.0 / area)

    def mean_columns(value):
        return [jnp.sum(jnp.where(lane == g, value, 0.0), axis=1, keepdims=True) for g in groups]

    columns = mean_columns(own_mean[...])
    shifts = [jnp.concatenate(columns[2 * b : 2 * b + 2], axis=0) for b in range(blocks)]
    filter_rows(0, shifts)

    in_two = jnp.logical_or(is_later_root, jnp.logical_and(y == 0, position > 1))

    @pl.when(in_two)
    def _():
        landed(mean_in, mean_recv)

    @pl.when(jnp.logical_not(jnp.logical_or(in_two, is_first)))
    def _():
        landed(mean_in.at[0], mean_recv)

    @pl.when(is_later_root)
    def _():
        own_mean[...] = mean_in[0] + mean_in[1]
        for member in members:
            mean_copy(0, own_mean, row(member)).start()

    @pl.when(jnp.logical_not(is_first))
    def _():
        for g, shift in zip(groups, mean_columns((mean_in[0] + mean_in[1]) * (1.0 / area))):
            lev = pl.ds(8 * g, 8)
            for r in range(rows):
                out[r, lev, :] = out[r, lev, :] - shift

    for side, sender in ((0, position < last), (1, position > 0)):

        @pl.when(sender)
        def _():
            landed(halo.at[side], halo_send.at[side])

    @pl.when(position <= 1)
    def _():
        landed(box.at[pl.ds(0, len(members) + NY - 1)], mean_send)

    @pl.when(is_later_root)
    def _():
        landed(box.at[pl.ds(0, len(members))], mean_send)

    @pl.when(position > 1)
    def _():
        landed(part, up_send)


def local(height, zonal, merid, rates, thresholds, flags, cutoffs):
    rows, levels, nlon = height.shape
    nlat = rows * NX * NY * NC
    fwd, inv, ksq = filter_tables(nlon)
    scalars, cos_sum = row_scalars(nlat)
    tiles = RADIX // 2
    dims = (rows, levels, nlon, nlat)
    f32, bf16 = jnp.float32, jnp.bfloat16
    vmem, smem, dma = pltpu.VMEM, pltpu.SMEM, pltpu.SemaphoreType.DMA
    operands = (height, zonal, merid, rates, thresholds, flags, cutoffs, scalars, ksq, fwd, inv)
    operands = [pltpu.with_memory_space_constraint(jnp.asarray(a), pltpu.HBM) for a in operands]
    return pl.pallas_call(
        functools.partial(kernel, dims, nlon * cos_sum),
        out_shape=vmem(height.shape, f32),
        in_specs=[pl.BlockSpec(memory_space=pltpu.HBM)] * len(operands),
        out_specs=pl.BlockSpec(memory_space=vmem),
        scratch_shapes=[
            vmem(height.shape, f32), vmem(height.shape, f32), vmem(height.shape, f32),
            smem(rates.shape, f32), smem(thresholds.shape, f32), smem(flags.shape, jnp.int32),
            smem(cutoffs.shape, jnp.int32), smem(scalars.shape, f32),
            vmem(ksq.shape, f32), vmem(fwd.shape, bf16), vmem(inv.shape, bf16),
            vmem((2, 3, levels, nlon), f32), vmem((rows, levels, RADIX * HALF), f32),
            vmem((levels, nlon), f32), vmem((levels, nlon), f32), vmem((rows, 8, 2 * HALF), f32),
            vmem((tiles, 4 * levels, 2 * HALF), bf16), vmem((tiles, 2 * levels, 2 * HALF), f32),
            vmem((8, HALF), f32), vmem((NX * NC + NY, 8, HALF), f32), vmem((2, 8, HALF), f32),
            vmem((8, HALF), f32),
            vmem((levels // 8, 8, HALF), f32), vmem((levels // 8, 8, HALF), f32),
            dma((2 * PIECES + 5,)), dma((2,)), dma((2,)), dma, dma, dma, dma, dma, pltpu.SemaphoreType.REGULAR,
        ],
        compiler_params=pltpu.CompilerParams(collective_id=0, has_side_effects=True, vmem_limit_bytes=16 * 2**20),
        name="advect_filter",
    )(*operands)


def solution(mesh):
    finer = Mesh(
        mesh.devices.reshape(mesh.shape["member"], NX, NY, NC), ("member", "lat_0", "lat_1", "lat_2")
    )
    whole = P(("member", "lat_0", "lat_1", "lat_2"), None, None)
    placed = (whole, whole, whole, P("member"), P("member"), P(), P())
    return jax.shard_map(local, mesh=finer, in_specs=placed, out_specs=whole, check_vma=False)
```

```python
import functools
import math

import jax
import jax.numpy as jnp
import numpy as np
from jax import lax
from jax.experimental import pallas as pl
from jax.experimental.pallas import tpu as pltpu
from jax.sharding import Mesh
from jax.sharding import PartitionSpec as P

MESH = pl.DeviceIdType.MESH
NX, NY, NC = 8, 8, 2
PIECES = 2
RADIX = 12
HALF = 128
ROOT = math.sqrt(0.75)
LOG2E = math.log2(math.e)


def filter_tables(nlon):
    count = nlon // RADIX
    tiles = RADIX // 2
    fwd = np.zeros((tiles, 2 * HALF, 2 * HALF))
    inv = np.zeros((tiles, 2 * HALF, 2 * HALF))
    waves = np.zeros((8, 2 * HALF), np.int64)
    r = np.arange(count)

    def trig(k):
        angle = 2.0 * np.pi / nlon * ((r * k) % nlon)
        return np.cos(angle), np.sin(angle)

    def real_part(base, shift):
        lane = base
        for q in range(count // 2 + 1):
            k = RADIX * q + shift
            if k > nlon // 2:
                continue
            cos, sin = trig(k)
            weight = (1.0 if k in (0, nlon // 2) else 2.0) / nlon
            rows = slice(base, base + count)
            fwd[0, rows, lane] = cos
            inv[0, lane, rows] = cos * weight
            waves[0, lane] = k
            lane += 1
            if k not in (0, nlon // 2):
                fwd[0, rows, lane] = sin
                inv[0, lane, rows] = sin * weight
                waves[0, lane] = k
                lane += 1
        assert lane == base + count

    real_part(0, 0)
    real_part(HALF, RADIX // 2)
    for m in range(1, tiles):
        for q in range(count):
            k = RADIX * q + m
            cos, sin = trig(k)
            fwd[m, 0:count, q] = cos
            fwd[m, HALF : HALF + count, q] = -sin
            fwd[m, 0:count, HALF + q] = sin
            fwd[m, HALF : HALF + count, HALF + q] = cos
            waves[m, q] = waves[m, HALF + q] = min(k, nlon - k)
        inv[m] = fwd[m].T * (2.0 / nlon)
    inv_square = 1.0 / np.maximum(waves, 1).astype(np.float64) ** 2

    def halves(table):
        hi = table.astype(np.float32).astype(jnp.bfloat16)
        lo = (table - hi.astype(np.float64)).astype(np.float32).astype(jnp.bfloat16)
        return np.stack([hi, lo])

    return halves(fwd), halves(inv), inv_square.astype(np.float32)


def row_scalars(nlat):
    rows = np.arange(nlat)
    cos_row = np.sin(np.pi * (rows + 0.5) / nlat)
    faces = np.arange(nlat + 1)
    cos_face = np.where((faces > 0) & (faces < nlat), np.sin(np.pi * faces / nlat), 0.0)
    table = np.zeros((3 * nlat + HALF,))
    table[0:nlat] = cos_row
    table[nlat : 2 * nlat] = 1.0 / cos_row
    table[2 * nlat : 3 * nlat + 1] = cos_face / 24.0
    return table.astype(np.float32), float(np.sum(cos_row))


def sums_of_twelve(e, o):
    plus, minus = e[0] + e[6], e[0] - e[6]
    e15p, e15m, e24p, e24m = e[1] + e[5], e[1] - e[5], e[2] + e[4], e[2] - e[4]
    o15p, o15m, o24p, o24m = o[0] + o[4], o[0] - o[4], o[1] + o[3], o[1] - o[3]
    return [
        plus + e24p, e15p + e[3], minus + 0.5 * e24m, ROOT * e15m, 0.5 * o15p + o[2], ROOT * o24p,
        plus - 0.5 * e24p, 0.5 * e15p - e[3], ROOT * o15m, ROOT * o24m, minus - e24m, o15p - o[2],
    ]


CLASSES = {
    0: ((0, 1, 1), (0, 1, -1)), 1: ((2, 3, 1), (4, 5, 1)), 5: ((2, 3, -1), (4, 5, -1)),
    2: ((6, 7, 1), (8, 9, 1)), 4: ((6, 7, -1), (8, 9, -1)), 3: ((10, None, 1), (11, None, 1)),
}


def combine(sums, which):
    i, j, sign = which
    if j is None:
        return sums(i)
    return sums(i) + sums(j) if sign > 0 else sums(i) - sums(j)


def twelve(e, o):
    sums = sums_of_twelve(e, o)
    parts = {m: [combine(lambda i: sums[i], which) for which in pair] for m, pair in CLASSES.items()}
    return [parts[m][0] for m in range(6)] + [parts[0][1]], [parts[m][1] for m in range(1, 6)]


def product_of(exps):
    result = 1.0 + exps[0]
    for e in exps[1:]:
        result = result * (1.0 + e)
    return result


def split(x):
    hi = x.astype(jnp.bfloat16)
    return hi, (x - hi.astype(jnp.float32)).astype(jnp.bfloat16)


def kernel(
    dims, area,
    h_hbm, z_hbm, c_hbm, rates_hbm, thr_hbm, flags_hbm, cut_hbm, scal_hbm, ksq_hbm, fwd_hbm, inv_hbm,
    out,
    h, z, c, rates, thr, flags, cut, scal, ksq, fwd, inv,
    halo, base, s_lo, s_hi, factor, mids, ymat, wmat, part, box, mean_in, own_mean, level_rates, level_thresholds,
    in_sem, halo_send, halo_recv, up_send, x_recv, y_recv, mean_send, mean_recv, low_in,
):
    rows, levels, nlon, nlat = dims
    count = nlon // RADIX
    x, y, core = lax.axis_index("lat_0"), lax.axis_index("lat_1"), lax.axis_index("lat_2")
    position = (x * NY + y) * NC + core
    total = NX * NY * NC

    order = (2, 3, 0, 1)
    cut_at = levels // PIECES
    pieces = [pl.ds(cut_at * i, cut_at) for i in range(PIECES)]

    def fetch(src, dst, i):
        return pltpu.make_async_copy(src, dst, in_sem.at[i])

    up_in = [[fetch(h_hbm.at[r, p], h.at[r, p], PIECES * (r - 2) + i) for i, p in enumerate(pieces)] for r in (2, 3)]
    low_rows = fetch(h_hbm.at[pl.ds(0, 2)], h.at[pl.ds(0, 2)], 2 * PIECES)
    c_up = fetch(c_hbm.at[rows - 1], c.at[rows - 1], 2 * PIECES + 1)
    small_in = [fetch(src, dst, 2 * PIECES + 2 + i) for i, (src, dst) in enumerate(((rates_hbm, rates), (thr_hbm, thr), (scal_hbm, scal)))]
    z_in = fetch(z_hbm, z, 0)
    c_in = fetch(c_hbm.at[pl.ds(0, rows - 1)], c.at[pl.ds(0, rows - 1)], 2 * PIECES)
    tables_in = [fetch(fwd_hbm, fwd, 1), fetch(inv_hbm, inv, 2)]
    factor_in = [
        fetch(src, dst, 2 * PIECES + 2 + i) for i, (src, dst) in enumerate(((flags_hbm, flags), (cut_hbm, cut), (ksq_hbm, ksq)))
    ]
    for copy in small_in + up_in[0] + up_in[1] + [low_rows, c_up]:
        copy.start()

    last = total - 1
    first = position * rows
    is_root = jnp.logical_and(x == 0, core == 1)
    is_first = position == 1
    is_later_root = jnp.logical_and(is_root, y > 0)

    def along(step):
        p = lax.rem(position + total + step, total)
        return {"lat_0": p // (NY * NC), "lat_1": lax.rem(p // NC, NY), "lat_2": lax.rem(p, NC)}

    def row(k):
        return {"lat_0": jnp.int32(k // NC), "lat_1": y, "lat_2": jnp.int32(k % NC)}

    def root(k):
        return {"lat_0": jnp.int32(0), "lat_1": jnp.int32(k), "lat_2": jnp.int32(1)}

    def signal(sem, device):
        pl.semaphore_signal(sem, inc=1, device_id=device, device_id_type=MESH)

    barrier = pltpu.get_barrier_semaphore()

    @pl.when(position > 0)
    def _():
        signal(barrier, along(-1))

    @pl.when(is_root)
    def _():
        for k in range(NX * NC):
            if k != 1:
                signal(barrier, row(k))

    @pl.when(is_first)
    def _():
        for k in range(1, NY):
            signal(barrier, root(k))

    to_start = jnp.logical_and(position > 1, jnp.logical_or(y == 0, is_root))

    @pl.when(to_start)
    def _():
        signal(barrier, {"lat_0": jnp.int32(0), "lat_1": jnp.int32(0), "lat_2": jnp.int32(0)})

    greeted = jnp.where(is_first, 0, 1) + jnp.where(position < last, 1, 0)
    greeted = greeted + jnp.where(position == 0, NX * NC - 2 + NY - 1, 0)
    pl.semaphore_wait(barrier, greeted)

    @pl.when(position < last)
    def _():
        signal(low_in, along(1))

    def landed(ref, sem):
        pltpu.make_async_copy(ref, ref, sem).wait()

    def halo_copy(side, field, levs=slice(None)):
        step, h_row, c_row = ((1, rows - 2, rows - 1), (-1, 0, 0))[side]
        src = c.at[c_row, levs] if field == 2 else h.at[h_row + field, levs]
        return pltpu.make_async_remote_copy(
            src, halo.at[side, field, levs], halo_send.at[side], halo_recv.at[side],
            device_id=along(step), device_id_type=MESH,
        )

    own_mean[...] = jnp.zeros_like(own_mean)

    @pl.when(jnp.logical_and(y > 0, jnp.logical_not(is_root)))
    def _():
        mean_in[1] = jnp.zeros_like(mean_in[1])

    base[:, :, nlon:] = jnp.zeros((rows, levels, base.shape[2] - nlon), jnp.float32)

    @pl.when(position == 0)
    def _():
        halo[0] = jnp.zeros_like(halo[0])

    @pl.when(position == last)
    def _():
        halo[1] = jnp.zeros_like(halo[1])

    for field in (0, 1):
        for arrived, levs in zip(up_in[field], pieces):
            arrived.wait()

            @pl.when(core == 0)
            def _():
                halo_copy(0, field, levs).start()

    for copy in small_in:
        copy.wait()

    lane = lax.broadcasted_iota(jnp.int32, (8, HALF), 1)
    tile = jnp.zeros((8, HALF), jnp.float32)
    sub = lax.broadcasted_iota(jnp.int32, (8, 1), 0)

    def levels_of(ref, start):
        value = jnp.zeros((8, 1), jnp.float32)
        for k in range(8):
            value = jnp.where(sub == k, ref[start + k], value)
        return value

    full = nlon // HALF
    groups = range(levels // 8)
    rate_of = [levels_of(rates, 8 * g) for g in groups]
    threshold_of = [levels_of(thr, 8 * g) for g in groups]
    scaled_threshold = [LOG2E * value for value in threshold_of]
    wide, rest = [0.0 for g in groups], [0.0 for g in groups]
    for r in order:
        if r == 0:
            low_rows.wait()
        for g in groups:
            lev = pl.ds(8 * g, 8)
            exps = [
                jnp.exp2(h[r, lev, HALF * j : HALF * (j + 1)] * LOG2E - scaled_threshold[g]) for j in range(full)
            ]
            logs = jnp.log2(product_of(exps[0:6])) + jnp.log2(product_of(exps[6:full]))
            wide[g] = wide[g] + scal[first + r] * logs
            logs = jnp.log2(1.0 + jnp.exp2(h[r, lev, HALF * full : nlon] * LOG2E - scaled_threshold[g]))
            rest[g] = rest[g] + scal[first + r] * logs
    short = jnp.zeros((8, HALF * (full + 1) - nlon), jnp.float32)
    for g in groups:
        sums = jnp.sum(wide[g] + jnp.concatenate([rest[g], short], axis=1), axis=1, keepdims=True)
        tile = jnp.where(lane == g, (-1.0 / LOG2E) * rate_of[g] * sums, tile)
        level_rates[g] = jnp.broadcast_to(rate_of[g], (8, HALF))
        level_thresholds[g] = jnp.broadcast_to(threshold_of[g], (8, HALF))
    part[...] = tile

    members = [*range(NC, NX * NC), 0]

    def mean_copy(slot, source, device):
        return pltpu.make_async_remote_copy(
            source, mean_in.at[slot], mean_send, mean_recv, device_id=device, device_id_type=MESH
        )

    def send_b(device):
        mean_copy(1, part, device).start()

    def part_copy(slot):
        return pltpu.make_async_remote_copy(
            part, box.at[slot], up_send, x_recv, device_id=row(1), device_id_type=MESH
        )

    sends_part = jnp.logical_and(jnp.logical_not(is_root), position > 0)

    @pl.when(sends_part)
    def _():
        part_copy(x * NC + core).start()

    @pl.when(position == 0)
    def _():
        send_b(row(1))

    c_up.wait()

    @pl.when(jnp.logical_and(core != 0, position < last))
    def _():
        halo_copy(0, 0).start()
        halo_copy(0, 1).start()

    @pl.when(position < last)
    def _():
        halo_copy(0, 2).start()

    @pl.when(position == 0)
    def _():
        mean_in[1] = part[...]
        for k in range(1, NY):
            for member in members[2 * k - 2 : 2 * k]:
                send_b(row(member))
            send_b(root(k))

    for copy in [c_in, z_in] + factor_in + tables_in:
        copy.start()

    z_in.wait()
    c_in.wait()


    def inv_cos(r):
        return scal[nlat + first + r]

    def face(f):
        return scal[2 * nlat + first + f]

    def west(a):
        return pltpu.roll(a, 1, axis=1)

    def east(a):
        return pltpu.roll(a, nlon - 1, axis=1)

    def local_terms(g, carry):
        lev = pl.ds(pl.multiple_of(8 * g, 8), 8)
        hr = [h[r, lev, :] for r in range(rows)]
        rate, threshold = level_rates[g][:, 0:1], level_thresholds[g][:, 0:1]
        cr = [c[r, lev, :] for r in range(rows)]
        low = face(1) * (cr[0] + cr[1])
        high = face(3) * (cr[2] + cr[3])
        s_lo[lev, :] = low
        s_hi[lev, :] = high
        f1 = low * (7.0 * (hr[0] + hr[1]) - hr[2])
        f2 = face(2) * (cr[1] + cr[2]) * (7.0 * (hr[1] + hr[2]) - (hr[0] + hr[3]))
        f3 = high * (7.0 * (hr[2] + hr[3]) - hr[1])
        terms = [f1, f2 - f1, f3 - f2, -f3]
        for r in range(rows):
            pair = hr[r] + east(hr[r])
            zr = z[r, lev, :]
            speed = zr + east(zr)
            flux = speed * (8.0 * pair - (west(pair) + east(pair))) * (1.0 / 24.0)
            s = hr[r] - threshold
            source = rate * jnp.log(1.0 + jnp.exp(s))
            base[r, lev, 0:nlon] = (hr[r] - source) - (flux - west(flux)) - terms[r] * inv_cos(r)
        return carry

    lax.fori_loop(0, levels // 8, local_terms, 0)

    @pl.when(position > 0)
    def _():
        pl.semaphore_wait(low_in, 1)
        for field in range(3):
            halo_copy(1, field).start()

    for copy in factor_in:
        copy.wait()
    for r in range(rows):
        cutoff = cut[first + r].astype(jnp.float32)
        flag = flags[first + r].astype(jnp.float32)
        factor[r] = flag * (1.0 - jnp.minimum(1.0, cutoff * cutoff * ksq[...]))

    def sum_copy():
        return pltpu.make_async_remote_copy(
            part, box.at[NX * NC + y], up_send, y_recv, device_id=root(0), device_id_type=MESH
        )

    def gather_row(senders):
        landed(box.at[pl.ds(0, len(senders))], x_recv)
        acc = part[...]
        for k in senders:
            acc = acc + box[k]
        return acc

    @pl.when(is_later_root)
    def _():
        part[...] = gather_row(members)
        sum_copy().start()

    for copy in tables_in:
        copy.wait()
    lanes = lax.broadcasted_iota(jnp.int32, (16, HALF), 1)
    units = 2 * levels
    blocks = levels // 16

    tail = nlon - HALF * (RADIX - 1)

    def piece(ref, j):
        if j < RADIX - 1:
            return ref[:, HALF * j : HALF * (j + 1)]
        return jnp.concatenate([ref[:, HALF * j : nlon], jnp.zeros((16, HALF - tail), jnp.float32)], axis=1)

    def with_halo(r, lev, j):
        side, near, far, edge, inner, f, through, outer = (
            (0, 1, 0, 0, 1, 0, s_lo, 0) if r < 2 else (1, 0, 1, rows - 1, rows - 2, rows, s_hi, rows - 1)
        )
        beside = piece(halo.at[side, near, lev], j)
        term = piece(through.at[lev], j) * beside
        if r == outer:
            speed = face(f) * (piece(halo.at[side, 2, lev], j) + piece(c.at[edge, lev], j))
            flux = speed * (
                7.0 * (beside + piece(h.at[edge, lev], j)) - (piece(halo.at[side, far, lev], j) + piece(h.at[inner, lev], j))
            )
            term = term + flux
        sign = 1.0 if r in (0, 2) else -1.0
        return base[r, lev, HALF * j : HALF * (j + 1)] + term * (sign * inv_cos(r))

    def product(hilo, table):
        first_part = jnp.dot(hilo, table[0], preferred_element_type=jnp.float32)
        second = jnp.dot(hilo[0:units], table[1], preferred_element_type=jnp.float32)
        return first_part[0:units] + first_part[units : 2 * units] + second

    def filter_rows(row0, shifts=None):
        def block_of(b):
            return row0 + b // blocks, pl.ds(16 * (b % blocks), 16), pl.ds(16 * b, 16), pl.ds(units + 16 * b, 16)

        def forward(b):
            r, lev, at_hi, at_lo = block_of(b)
            v = [with_halo(r, lev, j) for j in range(RADIX)]
            for j in range(RADIX):
                base[r, lev, HALF * j : HALF * (j + 1)] = v[j]
            u = [v[0]] + [
                pltpu.roll(jnp.where(lanes >= HALF - 8 * j, v[j - 1], v[j]), 8 * j, axis=1) for j in range(1, RADIX)
            ]
            e = [u[0]] + [u[j] + u[RADIX - j] for j in range(1, 6)] + [u[6]]
            o = [u[j] - u[RADIX - j] for j in range(1, 6)]
            for i, value in enumerate(sums_of_twelve(e, o)):
                mids[i, at_hi, :] = value

        def finish(m, b):
            _, _, at_hi, at_lo = block_of(b)
            for k, which in enumerate(CLASSES[m]):
                hi, lo = split(combine(lambda i: mids[i, at_hi, :], which))
                ymat[m, at_hi, HALF * k : HALF * (k + 1)] = hi
                ymat[m, at_lo, HALF * k : HALF * (k + 1)] = lo

        def backward(b):
            r, lev, at, _ = block_of(b)
            w = [[wmat[m, at, HALF * k : HALF * (k + 1)] for k in range(2)] for m in range(RADIX // 2)]
            even, odd = twelve([w[0][0]] + [w[m][0] for m in range(1, 6)] + [w[0][1]], [w[m][1] for m in range(1, 6)])
            removed = [even[0]] + [even[j] + odd[j - 1] for j in range(1, 6)] + [even[6]]
            removed += [even[RADIX - j] - odd[RADIX - j - 1] for j in range(7, RADIX)]
            back = [removed[0]] + [pltpu.roll(removed[j], HALF - 8 * j, axis=1) for j in range(1, RADIX)]
            for j in range(RADIX):
                kept = base[r, lev, HALF * j : HALF * (j + 1)]
                if row0 == 0:
                    kept = kept - shifts[b % blocks]
                if j < RADIX - 1:
                    out[r, lev, HALF * j : HALF * (j + 1)] = kept - jnp.where(lanes < count - 8 * j, back[j], back[j + 1])
                else:
                    out[r, lev, HALF * j : nlon] = (kept - back[j])[:, 0:tail]

        for b in range(2 * blocks):
            forward(b)
        for m in CLASSES:
            for b in range(2 * blocks):
                finish(m, b)
            waves = product(ymat[m], (fwd[0, m], fwd[1, m]))
            scaled = jnp.concatenate(
                [waves[r * levels : (r + 1) * levels] * factor[row0 + r, m : m + 1, :] for r in range(2)], axis=0
            )
            wmat[m] = product(jnp.concatenate(split(scaled), axis=0), (inv[0, m], inv[1, m]))
        if row0 == 0:
            for r in (2, 3):
                for b in range(blocks):
                    lev = pl.ds(16 * b, 16)
                    out[r, lev, :] = out[r, lev, :] - shifts[b]
        for b in range(2 * blocks):
            backward(b)

    @pl.when(position < last)
    def _():
        landed(halo.at[1], halo_recv.at[1])

    filter_rows(2)

    @pl.when(is_first)
    def _():
        landed(box.at[pl.ds(NX * NC + 1, NY - 1)], y_recv)
        acc = box[NX * NC + 1]
        for k in range(2, NY):
            acc = acc + box[NX * NC + k]
        mean_in[0] = gather_row(members[:-1]) + acc
        for k in range(1, NY):
            for member in members[2 * k - 2 : 2 * k]:
                mean_copy(0, mean_in.at[0], row(member)).start()
            mean_copy(0, mean_in.at[0], root(k)).start()
        mean_copy(0, mean_in.at[0], row(0)).start()

    @pl.when(position > 0)
    def _():
        landed(halo.at[0], halo_recv.at[0])

    @pl.when(is_first)
    def _():
        landed(mean_in.at[1], mean_recv)
        own_mean[...] = (mean_in[0] + mean_in[1]) * (1.0 / area)

    def mean_columns(value):
        return [jnp.sum(jnp.where(lane == g, value, 0.0), axis=1, keepdims=True) for g in groups]

    columns = mean_columns(own_mean[...])
    shifts = [jnp.concatenate(columns[2 * b : 2 * b + 2], axis=0) for b in range(blocks)]
    filter_rows(0, shifts)

    in_two = jnp.logical_or(is_later_root, jnp.logical_and(y == 0, position > 1))

    @pl.when(in_two)
    def _():
        landed(mean_in, mean_recv)

    @pl.when(jnp.logical_not(jnp.logical_or(in_two, is_first)))
    def _():
        landed(mean_in.at[0], mean_recv)

    @pl.when(is_later_root)
    def _():
        own_mean[...] = mean_in[0] + mean_in[1]
        for member in members:
            mean_copy(0, own_mean, row(member)).start()

    @pl.when(jnp.logical_not(is_first))
    def _():
        for g, shift in zip(groups, mean_columns((mean_in[0] + mean_in[1]) * (1.0 / area))):
            lev = pl.ds(8 * g, 8)
            for r in range(rows):
                out[r, lev, :] = out[r, lev, :] - shift

    for side, sender in ((0, position < last), (1, position > 0)):

        @pl.when(sender)
        def _():
            landed(halo.at[side], halo_send.at[side])

    @pl.when(position <= 1)
    def _():
        landed(box.at[pl.ds(0, len(members) + NY - 1)], mean_send)

    @pl.when(is_later_root)
    def _():
        landed(box.at[pl.ds(0, len(members))], mean_send)

    @pl.when(position > 1)
    def _():
        landed(part, up_send)


def local(height, zonal, merid, rates, thresholds, flags, cutoffs):
    rows, levels, nlon = height.shape
    nlat = rows * NX * NY * NC
    fwd, inv, ksq = filter_tables(nlon)
    scalars, cos_sum = row_scalars(nlat)
    tiles = RADIX // 2
    dims = (rows, levels, nlon, nlat)
    f32, bf16 = jnp.float32, jnp.bfloat16
    vmem, smem, dma = pltpu.VMEM, pltpu.SMEM, pltpu.SemaphoreType.DMA
    operands = (height, zonal, merid, rates, thresholds, flags, cutoffs, scalars, ksq, fwd, inv)
    operands = [pltpu.with_memory_space_constraint(jnp.asarray(a), pltpu.HBM) for a in operands]
    return pl.pallas_call(
        functools.partial(kernel, dims, nlon * cos_sum),
        out_shape=vmem(height.shape, f32),
        in_specs=[pl.BlockSpec(memory_space=pltpu.HBM)] * len(operands),
        out_specs=pl.BlockSpec(memory_space=vmem),
        scratch_shapes=[
            vmem(height.shape, f32), vmem(height.shape, f32), vmem(height.shape, f32),
            smem(rates.shape, f32), smem(thresholds.shape, f32), smem(flags.shape, jnp.int32),
            smem(cutoffs.shape, jnp.int32), smem(scalars.shape, f32),
            vmem(ksq.shape, f32), vmem(fwd.shape, bf16), vmem(inv.shape, bf16),
            vmem((2, 3, levels, nlon), f32), vmem((rows, levels, RADIX * HALF), f32),
            vmem((levels, nlon), f32), vmem((levels, nlon), f32), vmem((rows, 8, 2 * HALF), f32),
            vmem((RADIX, 2 * levels, HALF), f32), vmem((tiles, 4 * levels, 2 * HALF), bf16), vmem((tiles, 2 * levels, 2 * HALF), f32),
            vmem((8, HALF), f32), vmem((NX * NC + NY, 8, HALF), f32), vmem((2, 8, HALF), f32),
            vmem((8, HALF), f32),
            vmem((levels // 8, 8, HALF), f32), vmem((levels // 8, 8, HALF), f32),
            dma((2 * PIECES + 5,)), dma((2,)), dma((2,)), dma, dma, dma, dma, dma, pltpu.SemaphoreType.REGULAR,
        ],
        compiler_params=pltpu.CompilerParams(collective_id=0, has_side_effects=True, vmem_limit_bytes=16 * 2**20),
        name="advect_filter",
    )(*operands)


def solution(mesh):
    finer = Mesh(
        mesh.devices.reshape(mesh.shape["member"], NX, NY, NC), ("member", "lat_0", "lat_1", "lat_2")
    )
    whole = P(("member", "lat_0", "lat_1", "lat_2"), None, None)
    placed = (whole, whole, whole, P("member"), P("member"), P(), P())
    return jax.shard_map(local, mesh=finer, in_specs=placed, out_specs=whole, check_vma=False)
```

```python
import functools
import math

import jax
import jax.numpy as jnp
import numpy as np
from jax import lax
from jax.experimental import pallas as pl
from jax.experimental.pallas import tpu as pltpu
from jax.sharding import Mesh
from jax.sharding import PartitionSpec as P

MESH = pl.DeviceIdType.MESH
NX, NY, NC = 8, 8, 2
PIECES = 2
RADIX = 12
HALF = 128
ROOT = math.sqrt(0.75)
LOG2E = math.log2(math.e)


def filter_tables(nlon):
    count = nlon // RADIX
    tiles = RADIX // 2
    fwd = np.zeros((tiles, 2 * HALF, 2 * HALF))
    inv = np.zeros((tiles, 2 * HALF, 2 * HALF))
    waves = np.zeros((8, 2 * HALF), np.int64)
    r = np.arange(count)

    def trig(k):
        angle = 2.0 * np.pi / nlon * ((r * k) % nlon)
        return np.cos(angle), np.sin(angle)

    def real_part(base, shift):
        lane = base
        for q in range(count // 2 + 1):
            k = RADIX * q + shift
            if k > nlon // 2:
                continue
            cos, sin = trig(k)
            weight = (1.0 if k in (0, nlon // 2) else 2.0) / nlon
            rows = slice(base, base + count)
            fwd[0, rows, lane] = cos
            inv[0, lane, rows] = cos * weight
            waves[0, lane] = k
            lane += 1
            if k not in (0, nlon // 2):
                fwd[0, rows, lane] = sin
                inv[0, lane, rows] = sin * weight
                waves[0, lane] = k
                lane += 1
        assert lane == base + count

    real_part(0, 0)
    real_part(HALF, RADIX // 2)
    for m in range(1, tiles):
        for q in range(count):
            k = RADIX * q + m
            cos, sin = trig(k)
            fwd[m, 0:count, q] = cos
            fwd[m, HALF : HALF + count, q] = -sin
            fwd[m, 0:count, HALF + q] = sin
            fwd[m, HALF : HALF + count, HALF + q] = cos
            waves[m, q] = waves[m, HALF + q] = min(k, nlon - k)
        inv[m] = fwd[m].T * (2.0 / nlon)
    inv_square = 1.0 / np.maximum(waves, 1).astype(np.float64) ** 2

    def halves(table):
        hi = table.astype(np.float32).astype(jnp.bfloat16)
        lo = (table - hi.astype(np.float64)).astype(np.float32).astype(jnp.bfloat16)
        return np.stack([hi, lo])

    return halves(fwd), halves(inv), inv_square.astype(np.float32)


def row_scalars(nlat):
    rows = np.arange(nlat)
    cos_row = np.sin(np.pi * (rows + 0.5) / nlat)
    faces = np.arange(nlat + 1)
    cos_face = np.where((faces > 0) & (faces < nlat), np.sin(np.pi * faces / nlat), 0.0)
    table = np.zeros((3 * nlat + HALF,))
    table[0:nlat] = cos_row
    table[nlat : 2 * nlat] = 1.0 / cos_row
    table[2 * nlat : 3 * nlat + 1] = cos_face / 24.0
    return table.astype(np.float32), float(np.sum(cos_row))


def twelve(e, o):
    plus, minus = e[0] + e[6], e[0] - e[6]
    e15p, e15m, e24p, e24m = e[1] + e[5], e[1] - e[5], e[2] + e[4], e[2] - e[4]
    a, b = plus + e24p, e15p + e[3]
    big, mid = ROOT * e15m, minus + 0.5 * e24m
    c, d = plus - 0.5 * e24p, 0.5 * e15p - e[3]
    even = [a + b, mid + big, c + d, minus - e24m, c - d, mid - big, a - b]
    o15p, o15m, o24p, o24m = o[0] + o[4], o[0] - o[4], o[1] + o[3], o[1] - o[3]
    f, g = 0.5 * o15p + o[2], ROOT * o24p
    s, t = ROOT * o15m, ROOT * o24m
    odd = [f + g, s + t, o15p - o[2], s - t, f - g]
    return even, odd


def product_of(exps):
    result = 1.0 + exps[0]
    for e in exps[1:]:
        result = result * (1.0 + e)
    return result


def split(x):
    hi = x.astype(jnp.bfloat16)
    return hi, (x - hi.astype(jnp.float32)).astype(jnp.bfloat16)


def kernel(
    dims, area,
    h_hbm, z_hbm, c_hbm, rates_hbm, thr_hbm, flags_hbm, cut_hbm, scal_hbm, ksq_hbm, fwd_hbm, inv_hbm,
    out,
    h, z, c, rates, thr, flags, cut, scal, ksq, fwd, inv,
    halo, base, s_lo, s_hi, factor, ymat, wmat, part, box, mean_in, own_mean, level_rates, level_thresholds,
    in_sem, halo_send, halo_recv, up_send, x_recv, y_recv, mean_send, mean_recv, low_in,
):
    rows, levels, nlon, nlat = dims
    count = nlon // RADIX
    x, y, core = lax.axis_index("lat_0"), lax.axis_index("lat_1"), lax.axis_index("lat_2")
    position = (x * NY + y) * NC + core
    total = NX * NY * NC

    order = (3, 2, 0, 1)
    cut_at = levels // PIECES
    pieces = [pl.ds(cut_at * i, cut_at) for i in range(PIECES)]

    def fetch(src, dst, i):
        return pltpu.make_async_copy(src, dst, in_sem.at[i])

    up_in = [[fetch(h_hbm.at[r, p], h.at[r, p], PIECES * (r - 2) + i) for i, p in enumerate(pieces)] for r in (2, 3)]
    low_rows = fetch(h_hbm.at[pl.ds(0, 2)], h.at[pl.ds(0, 2)], 2 * PIECES)
    c_up = fetch(c_hbm.at[rows - 1], c.at[rows - 1], 2 * PIECES + 1)
    small_in = [fetch(src, dst, 2 * PIECES + 2 + i) for i, (src, dst) in enumerate(((rates_hbm, rates), (thr_hbm, thr), (scal_hbm, scal)))]
    z_in = fetch(z_hbm, z, 0)
    c_in = fetch(c_hbm.at[pl.ds(0, rows - 1)], c.at[pl.ds(0, rows - 1)], 2 * PIECES)
    tables_in = [fetch(fwd_hbm, fwd, 1), fetch(inv_hbm, inv, 2)]
    factor_in = [
        fetch(src, dst, 2 * PIECES + 2 + i) for i, (src, dst) in enumerate(((flags_hbm, flags), (cut_hbm, cut), (ksq_hbm, ksq)))
    ]
    for copy in small_in + up_in[1] + up_in[0] + [low_rows, c_up]:
        copy.start()

    last = total - 1
    first = position * rows
    is_root = jnp.logical_and(x == 0, core == 1)
    is_first = position == 1
    is_later_root = jnp.logical_and(is_root, y > 0)

    def along(step):
        p = lax.rem(position + total + step, total)
        return {"lat_0": p // (NY * NC), "lat_1": lax.rem(p // NC, NY), "lat_2": lax.rem(p, NC)}

    def row(k):
        return {"lat_0": jnp.int32(k // NC), "lat_1": y, "lat_2": jnp.int32(k % NC)}

    def root(k):
        return {"lat_0": jnp.int32(0), "lat_1": jnp.int32(k), "lat_2": jnp.int32(1)}

    def signal(sem, device):
        pl.semaphore_signal(sem, inc=1, device_id=device, device_id_type=MESH)

    barrier = pltpu.get_barrier_semaphore()

    @pl.when(position > 0)
    def _():
        signal(barrier, along(-1))

    @pl.when(is_root)
    def _():
        for k in range(NX * NC):
            if k != 1:
                signal(barrier, row(k))

    @pl.when(is_first)
    def _():
        for k in range(1, NY):
            signal(barrier, root(k))

    to_start = jnp.logical_and(position > 1, jnp.logical_or(y == 0, is_root))

    @pl.when(to_start)
    def _():
        signal(barrier, {"lat_0": jnp.int32(0), "lat_1": jnp.int32(0), "lat_2": jnp.int32(0)})

    greeted = jnp.where(is_first, 0, 1) + jnp.where(position < last, 1, 0)
    greeted = greeted + jnp.where(position == 0, NX * NC - 2 + NY - 1, 0)
    pl.semaphore_wait(barrier, greeted)

    @pl.when(position < last)
    def _():
        signal(low_in, along(1))

    def landed(ref, sem):
        pltpu.make_async_copy(ref, ref, sem).wait()

    def halo_copy(side, field, levs=slice(None)):
        step, h_row, c_row = ((1, rows - 2, rows - 1), (-1, 0, 0))[side]
        src = c.at[c_row, levs] if field == 2 else h.at[h_row + field, levs]
        return pltpu.make_async_remote_copy(
            src, halo.at[side, field, levs], halo_send.at[side], halo_recv.at[side, 0 if field == 1 - side else 1],
            device_id=along(step), device_id_type=MESH,
        )

    own_mean[...] = jnp.zeros_like(own_mean)

    @pl.when(jnp.logical_and(y > 0, jnp.logical_not(is_root)))
    def _():
        mean_in[1] = jnp.zeros_like(mean_in[1])

    base[:, :, nlon:] = jnp.zeros((rows, levels, base.shape[2] - nlon), jnp.float32)

    @pl.when(position == 0)
    def _():
        halo[0] = jnp.zeros_like(halo[0])

    @pl.when(position == last)
    def _():
        halo[1] = jnp.zeros_like(halo[1])

    for field in (1, 0):
        for arrived, levs in zip(up_in[field], pieces):
            arrived.wait()

            @pl.when(core == 0)
            def _():
                halo_copy(0, field, levs).start()

    for copy in small_in:
        copy.wait()

    lane = lax.broadcasted_iota(jnp.int32, (8, HALF), 1)
    tile = jnp.zeros((8, HALF), jnp.float32)
    sub = lax.broadcasted_iota(jnp.int32, (8, 1), 0)

    def levels_of(ref, start):
        value = jnp.zeros((8, 1), jnp.float32)
        for k in range(8):
            value = jnp.where(sub == k, ref[start + k], value)
        return value

    full = nlon // HALF
    groups = range(levels // 8)
    rate_of = [levels_of(rates, 8 * g) for g in groups]
    threshold_of = [levels_of(thr, 8 * g) for g in groups]
    scaled_threshold = [LOG2E * value for value in threshold_of]
    wide, rest = [0.0 for g in groups], [0.0 for g in groups]
    for r in order:
        if r == 0:
            low_rows.wait()
        for g in groups:
            lev = pl.ds(8 * g, 8)
            exps = [
                jnp.exp2(h[r, lev, HALF * j : HALF * (j + 1)] * LOG2E - scaled_threshold[g]) for j in range(full)
            ]
            logs = jnp.log2(product_of(exps[0:6])) + jnp.log2(product_of(exps[6:full]))
            wide[g] = wide[g] + scal[first + r] * logs
            logs = jnp.log2(1.0 + jnp.exp2(h[r, lev, HALF * full : nlon] * LOG2E - scaled_threshold[g]))
            rest[g] = rest[g] + scal[first + r] * logs
    short = jnp.zeros((8, HALF * (full + 1) - nlon), jnp.float32)
    for g in groups:
        sums = jnp.sum(wide[g] + jnp.concatenate([rest[g], short], axis=1), axis=1, keepdims=True)
        tile = jnp.where(lane == g, (-1.0 / LOG2E) * rate_of[g] * sums, tile)
        level_rates[g] = jnp.broadcast_to(rate_of[g], (8, HALF))
        level_thresholds[g] = jnp.broadcast_to(threshold_of[g], (8, HALF))
    part[...] = tile

    members = [*range(NC, NX * NC), 0]

    def mean_copy(slot, source, device):
        return pltpu.make_async_remote_copy(
            source, mean_in.at[slot], mean_send, mean_recv, device_id=device, device_id_type=MESH
        )

    def send_b(device):
        mean_copy(1, part, device).start()

    def part_copy(slot):
        return pltpu.make_async_remote_copy(
            part, box.at[slot], up_send, x_recv, device_id=row(1), device_id_type=MESH
        )

    sends_part = jnp.logical_and(jnp.logical_not(is_root), position > 0)

    @pl.when(sends_part)
    def _():
        part_copy(x * NC + core).start()

    @pl.when(position == 0)
    def _():
        send_b(row(1))

    c_up.wait()

    @pl.when(jnp.logical_and(core != 0, position < last))
    def _():
        halo_copy(0, 1).start()
        halo_copy(0, 0).start()

    @pl.when(position < last)
    def _():
        halo_copy(0, 2).start()

    @pl.when(position == 0)
    def _():
        mean_in[1] = part[...]
        for k in range(1, NY):
            for member in members[2 * k - 2 : 2 * k]:
                send_b(row(member))
            send_b(root(k))

    for copy in [c_in, z_in] + factor_in + tables_in:
        copy.start()

    z_in.wait()
    c_in.wait()


    def inv_cos(r):
        return scal[nlat + first + r]

    def face(f):
        return scal[2 * nlat + first + f]

    def west(a):
        return pltpu.roll(a, 1, axis=1)

    def east(a):
        return pltpu.roll(a, nlon - 1, axis=1)

    def local_terms(g, carry):
        lev = pl.ds(pl.multiple_of(8 * g, 8), 8)
        hr = [h[r, lev, :] for r in range(rows)]
        rate, threshold = level_rates[g][:, 0:1], level_thresholds[g][:, 0:1]
        cr = [c[r, lev, :] for r in range(rows)]
        low = face(1) * (cr[0] + cr[1])
        high = face(3) * (cr[2] + cr[3])
        s_lo[lev, :] = low
        s_hi[lev, :] = high
        f1 = low * (7.0 * (hr[0] + hr[1]) - hr[2])
        f2 = face(2) * (cr[1] + cr[2]) * (7.0 * (hr[1] + hr[2]) - (hr[0] + hr[3]))
        f3 = high * (7.0 * (hr[2] + hr[3]) - hr[1])
        terms = [f1, f2 - f1, f3 - f2, -f3]
        for r in range(rows):
            pair = hr[r] + east(hr[r])
            zr = z[r, lev, :]
            speed = zr + east(zr)
            flux = speed * (8.0 * pair - (west(pair) + east(pair))) * (1.0 / 24.0)
            s = hr[r] - threshold
            source = rate * jnp.log(1.0 + jnp.exp(s))
            base[r, lev, 0:nlon] = (hr[r] - source) - (flux - west(flux)) - terms[r] * inv_cos(r)
        return carry

    lax.fori_loop(0, levels // 8, local_terms, 0)

    @pl.when(position > 0)
    def _():
        pl.semaphore_wait(low_in, 1)
        for field in range(3):
            halo_copy(1, field).start()

    for copy in factor_in:
        copy.wait()
    for r in range(rows):
        cutoff = cut[first + r].astype(jnp.float32)
        flag = flags[first + r].astype(jnp.float32)
        factor[r] = flag * (1.0 - jnp.minimum(1.0, cutoff * cutoff * ksq[...]))

    def sum_copy():
        return pltpu.make_async_remote_copy(
            part, box.at[NX * NC + y], up_send, y_recv, device_id=root(0), device_id_type=MESH
        )

    def gather_row(senders):
        landed(box.at[pl.ds(0, len(senders))], x_recv)
        acc = part[...]
        for k in senders:
            acc = acc + box[k]
        return acc

    @pl.when(is_later_root)
    def _():
        part[...] = gather_row(members)
        sum_copy().start()

    for copy in tables_in:
        copy.wait()
    lanes = lax.broadcasted_iota(jnp.int32, (16, HALF), 1)
    units = 2 * levels
    blocks = levels // 16

    tail = nlon - HALF * (RADIX - 1)

    def piece(ref, j):
        if j < RADIX - 1:
            return ref[:, HALF * j : HALF * (j + 1)]
        return jnp.concatenate([ref[:, HALF * j : nlon], jnp.zeros((16, HALF - tail), jnp.float32)], axis=1)

    def with_halo(r, lev, j):
        side, near, far, edge, inner, f, through, outer = (
            (0, 1, 0, 0, 1, 0, s_lo, 0) if r < 2 else (1, 0, 1, rows - 1, rows - 2, rows, s_hi, rows - 1)
        )
        beside = piece(halo.at[side, near, lev], j)
        term = piece(through.at[lev], j) * beside
        if r == outer:
            speed = face(f) * (piece(halo.at[side, 2, lev], j) + piece(c.at[edge, lev], j))
            flux = speed * (
                7.0 * (beside + piece(h.at[edge, lev], j)) - (piece(halo.at[side, far, lev], j) + piece(h.at[inner, lev], j))
            )
            term = term + flux
        sign = 1.0 if r in (0, 2) else -1.0
        return base[r, lev, HALF * j : HALF * (j + 1)] + term * (sign * inv_cos(r))

    def product(hilo, table):
        first_part = jnp.dot(hilo, table[0], preferred_element_type=jnp.float32)
        second = jnp.dot(hilo[0:units], table[1], preferred_element_type=jnp.float32)
        return first_part[0:units] + first_part[units : 2 * units] + second

    def filter_rows(row0, side, between):
        sender = position > 0 if side == 0 else position < last
        outer = 0 if side == 0 else 1

        def block_of(b):
            return row0 + b // blocks, pl.ds(16 * (b % blocks), 16), pl.ds(16 * b, 16), pl.ds(units + 16 * b, 16)

        def forward(b):
            r, lev, at_hi, at_lo = block_of(b)
            v = [with_halo(r, lev, j) for j in range(RADIX)]
            for j in range(RADIX):
                base[r, lev, HALF * j : HALF * (j + 1)] = v[j]
            u = [v[0]] + [
                pltpu.roll(jnp.where(lanes >= HALF - 8 * j, v[j - 1], v[j]), 8 * j, axis=1) for j in range(1, RADIX)
            ]
            e = [u[0]] + [u[j] + u[RADIX - j] for j in range(1, 6)] + [u[6]]
            o = [u[j] - u[RADIX - j] for j in range(1, 6)]
            even, odd = twelve(e, o)
            halves = [(even[0], even[6])] + [(even[m], odd[m - 1]) for m in range(1, 6)]
            for m, pair in enumerate(halves):
                for k, value in enumerate(pair):
                    hi, lo = split(value)
                    ymat[m, at_hi, HALF * k : HALF * (k + 1)] = hi
                    ymat[m, at_lo, HALF * k : HALF * (k + 1)] = lo

        def backward(b):
            r, lev, at, _ = block_of(b)
            w = [[wmat[m, at, HALF * k : HALF * (k + 1)] for k in range(2)] for m in range(RADIX // 2)]
            even, odd = twelve([w[0][0]] + [w[m][0] for m in range(1, 6)] + [w[0][1]], [w[m][1] for m in range(1, 6)])
            removed = [even[0]] + [even[j] + odd[j - 1] for j in range(1, 6)] + [even[6]]
            removed += [even[RADIX - j] - odd[RADIX - j - 1] for j in range(7, RADIX)]
            back = [removed[0]] + [pltpu.roll(removed[j], HALF - 8 * j, axis=1) for j in range(1, RADIX)]
            for j in range(RADIX):
                kept = base[r, lev, HALF * j : HALF * (j + 1)]
                if row0 == 0:
                    kept = kept - shifts[b % blocks]
                if j < RADIX - 1:
                    out[r, lev, HALF * j : HALF * (j + 1)] = kept - jnp.where(lanes < count - 8 * j, back[j], back[j + 1])
                else:
                    out[r, lev, HALF * j : nlon] = (kept - back[j])[:, 0:tail]

        @pl.when(sender)
        def _():
            landed(halo.at[side, 0], halo_recv.at[side, 0])

        for b in range(blocks):
            forward((1 - outer) * blocks + b)
        shifts = between()

        @pl.when(sender)
        def _():
            landed(halo.at[side, pl.ds(1, 2)], halo_recv.at[side, 1])

        for b in range(blocks):
            forward(outer * blocks + b)
        for m in range(RADIX // 2):
            waves = product(ymat[m], (fwd[0, m], fwd[1, m]))
            scaled = jnp.concatenate(
                [waves[r * levels : (r + 1) * levels] * factor[row0 + r, m : m + 1, :] for r in range(2)], axis=0
            )
            wmat[m] = product(jnp.concatenate(split(scaled), axis=0), (inv[0, m], inv[1, m]))
        if row0 == 0:
            for r in (2, 3):
                for b in range(blocks):
                    lev = pl.ds(16 * b, 16)
                    out[r, lev, :] = out[r, lev, :] - shifts[b]
        for b in range(2 * blocks):
            backward(b)

    filter_rows(2, 1, lambda: None)

    @pl.when(is_first)
    def _():
        landed(box.at[pl.ds(NX * NC + 1, NY - 1)], y_recv)
        acc = box[NX * NC + 1]
        for k in range(2, NY):
            acc = acc + box[NX * NC + k]
        mean_in[0] = gather_row(members[:-1]) + acc
        for k in range(1, NY):
            for member in members[2 * k - 2 : 2 * k]:
                mean_copy(0, mean_in.at[0], row(member)).start()
            mean_copy(0, mean_in.at[0], root(k)).start()
        mean_copy(0, mean_in.at[0], row(0)).start()

    def mean_columns(value):
        return [jnp.sum(jnp.where(lane == g, value, 0.0), axis=1, keepdims=True) for g in groups]

    def known_shifts():
        @pl.when(is_first)
        def _():
            landed(mean_in.at[1], mean_recv)
            own_mean[...] = (mean_in[0] + mean_in[1]) * (1.0 / area)

        columns = mean_columns(own_mean[...])
        return [jnp.concatenate(columns[2 * b : 2 * b + 2], axis=0) for b in range(blocks)]

    filter_rows(0, 0, known_shifts)

    in_two = jnp.logical_or(is_later_root, jnp.logical_and(y == 0, position > 1))

    @pl.when(in_two)
    def _():
        landed(mean_in, mean_recv)

    @pl.when(jnp.logical_not(jnp.logical_or(in_two, is_first)))
    def _():
        landed(mean_in.at[0], mean_recv)

    @pl.when(is_later_root)
    def _():
        own_mean[...] = mean_in[0] + mean_in[1]
        for member in members:
            mean_copy(0, own_mean, row(member)).start()

    @pl.when(jnp.logical_not(is_first))
    def _():
        for g, shift in zip(groups, mean_columns((mean_in[0] + mean_in[1]) * (1.0 / area))):
            lev = pl.ds(8 * g, 8)
            for r in range(rows):
                out[r, lev, :] = out[r, lev, :] - shift

    for side, sender in ((0, position < last), (1, position > 0)):

        @pl.when(sender)
        def _():
            landed(halo.at[side], halo_send.at[side])

    @pl.when(position <= 1)
    def _():
        landed(box.at[pl.ds(0, len(members) + NY - 1)], mean_send)

    @pl.when(is_later_root)
    def _():
        landed(box.at[pl.ds(0, len(members))], mean_send)

    @pl.when(position > 1)
    def _():
        landed(part, up_send)


def local(height, zonal, merid, rates, thresholds, flags, cutoffs):
    rows, levels, nlon = height.shape
    nlat = rows * NX * NY * NC
    fwd, inv, ksq = filter_tables(nlon)
    scalars, cos_sum = row_scalars(nlat)
    tiles = RADIX // 2
    dims = (rows, levels, nlon, nlat)
    f32, bf16 = jnp.float32, jnp.bfloat16
    vmem, smem, dma = pltpu.VMEM, pltpu.SMEM, pltpu.SemaphoreType.DMA
    operands = (height, zonal, merid, rates, thresholds, flags, cutoffs, scalars, ksq, fwd, inv)
    operands = [pltpu.with_memory_space_constraint(jnp.asarray(a), pltpu.HBM) for a in operands]
    return pl.pallas_call(
        functools.partial(kernel, dims, nlon * cos_sum),
        out_shape=vmem(height.shape, f32),
        in_specs=[pl.BlockSpec(memory_space=pltpu.HBM)] * len(operands),
        out_specs=pl.BlockSpec(memory_space=vmem),
        scratch_shapes=[
            vmem(height.shape, f32), vmem(height.shape, f32), vmem(height.shape, f32),
            smem(rates.shape, f32), smem(thresholds.shape, f32), smem(flags.shape, jnp.int32),
            smem(cutoffs.shape, jnp.int32), smem(scalars.shape, f32),
            vmem(ksq.shape, f32), vmem(fwd.shape, bf16), vmem(inv.shape, bf16),
            vmem((2, 3, levels, nlon), f32), vmem((rows, levels, RADIX * HALF), f32),
            vmem((levels, nlon), f32), vmem((levels, nlon), f32), vmem((rows, 8, 2 * HALF), f32),
            vmem((tiles, 4 * levels, 2 * HALF), bf16), vmem((tiles, 2 * levels, 2 * HALF), f32),
            vmem((8, HALF), f32), vmem((NX * NC + NY, 8, HALF), f32), vmem((2, 8, HALF), f32),
            vmem((8, HALF), f32),
            vmem((levels // 8, 8, HALF), f32), vmem((levels // 8, 8, HALF), f32),
            dma((2 * PIECES + 5,)), dma((2,)), dma((2, 2)), dma, dma, dma, dma, dma, pltpu.SemaphoreType.REGULAR,
        ],
        compiler_params=pltpu.CompilerParams(collective_id=0, has_side_effects=True, vmem_limit_bytes=16 * 2**20),
        name="advect_filter",
    )(*operands)


def solution(mesh):
    finer = Mesh(
        mesh.devices.reshape(mesh.shape["member"], NX, NY, NC), ("member", "lat_0", "lat_1", "lat_2")
    )
    whole = P(("member", "lat_0", "lat_1", "lat_2"), None, None)
    placed = (whole, whole, whole, P("member"), P("member"), P(), P())
    return jax.shard_map(local, mesh=finer, in_specs=placed, out_specs=whole, check_vma=False)
```

```python
import functools
import math

import jax
import jax.numpy as jnp
import numpy as np
from jax import lax
from jax.experimental import pallas as pl
from jax.experimental.pallas import tpu as pltpu
from jax.sharding import Mesh
from jax.sharding import PartitionSpec as P

MESH = pl.DeviceIdType.MESH
NX, NY, NC = 8, 8, 2
PIECES = 2
RADIX = 12
HALF = 128
ROOT = math.sqrt(0.75)
LOG2E = math.log2(math.e)


def filter_tables(nlon):
    count = nlon // RADIX
    tiles = RADIX // 2
    fwd = np.zeros((tiles, 2 * HALF, 2 * HALF))
    inv = np.zeros((tiles, 2 * HALF, 2 * HALF))
    waves = np.zeros((8, 2 * HALF), np.int64)
    r = np.arange(count)

    def trig(k):
        angle = 2.0 * np.pi / nlon * ((r * k) % nlon)
        return np.cos(angle), np.sin(angle)

    def real_part(base, shift):
        lane = base
        for q in range(count // 2 + 1):
            k = RADIX * q + shift
            if k > nlon // 2:
                continue
            cos, sin = trig(k)
            weight = (1.0 if k in (0, nlon // 2) else 2.0) / nlon
            rows = slice(base, base + count)
            fwd[0, rows, lane] = cos
            inv[0, lane, rows] = cos * weight
            waves[0, lane] = k
            lane += 1
            if k not in (0, nlon // 2):
                fwd[0, rows, lane] = sin
                inv[0, lane, rows] = sin * weight
                waves[0, lane] = k
                lane += 1
        assert lane == base + count

    real_part(0, 0)
    real_part(HALF, RADIX // 2)
    for m in range(1, tiles):
        for q in range(count):
            k = RADIX * q + m
            cos, sin = trig(k)
            fwd[m, 0:count, q] = cos
            fwd[m, HALF : HALF + count, q] = -sin
            fwd[m, 0:count, HALF + q] = sin
            fwd[m, HALF : HALF + count, HALF + q] = cos
            waves[m, q] = waves[m, HALF + q] = min(k, nlon - k)
        inv[m] = fwd[m].T * (2.0 / nlon)
    inv_square = 1.0 / np.maximum(waves, 1).astype(np.float64) ** 2

    def halves(table):
        hi = table.astype(np.float32).astype(jnp.bfloat16)
        lo = (table - hi.astype(np.float64)).astype(np.float32).astype(jnp.bfloat16)
        return np.stack([hi, lo])

    return halves(fwd), halves(inv), inv_square.astype(np.float32)


def row_scalars(nlat):
    rows = np.arange(nlat)
    cos_row = np.sin(np.pi * (rows + 0.5) / nlat)
    faces = np.arange(nlat + 1)
    cos_face = np.where((faces > 0) & (faces < nlat), np.sin(np.pi * faces / nlat), 0.0)
    table = np.zeros((3 * nlat + HALF,))
    table[0:nlat] = cos_row
    table[nlat : 2 * nlat] = 1.0 / cos_row
    table[2 * nlat : 3 * nlat + 1] = cos_face / 24.0
    return table.astype(np.float32), float(np.sum(cos_row))


def twelve(e, o):
    plus, minus = e[0] + e[6], e[0] - e[6]
    e15p, e15m, e24p, e24m = e[1] + e[5], e[1] - e[5], e[2] + e[4], e[2] - e[4]
    a, b = plus + e24p, e15p + e[3]
    big, mid = ROOT * e15m, minus + 0.5 * e24m
    c, d = plus - 0.5 * e24p, 0.5 * e15p - e[3]
    even = [a + b, mid + big, c + d, minus - e24m, c - d, mid - big, a - b]
    o15p, o15m, o24p, o24m = o[0] + o[4], o[0] - o[4], o[1] + o[3], o[1] - o[3]
    f, g = 0.5 * o15p + o[2], ROOT * o24p
    s, t = ROOT * o15m, ROOT * o24m
    odd = [f + g, s + t, o15p - o[2], s - t, f - g]
    return even, odd


def product_of(exps):
    result = 1.0 + exps[0]
    for e in exps[1:]:
        result = result * (1.0 + e)
    return result


def split(x):
    hi = x.astype(jnp.bfloat16)
    return hi, (x - hi.astype(jnp.float32)).astype(jnp.bfloat16)


def kernel(
    dims, area,
    h_hbm, z_hbm, c_hbm, rates_hbm, thr_hbm, flags_hbm, cut_hbm, scal_hbm, ksq_hbm, fwd_hbm, inv_hbm,
    out,
    h, z, c, rates, thr, flags, cut, scal, ksq, fwd, inv,
    halo, base, s_lo, s_hi, factor, ymat, wmat, part, box, mean_in, own_mean, level_rates, level_thresholds,
    in_sem, halo_send, halo_recv, up_send, x_recv, y_recv, mean_send, mean_recv, low_in,
):
    rows, levels, nlon, nlat = dims
    count = nlon // RADIX
    x, y, core = lax.axis_index("lat_0"), lax.axis_index("lat_1"), lax.axis_index("lat_2")
    position = (x * NY + y) * NC + core
    total = NX * NY * NC

    order = (2, 3, 0, 1)
    cut_at = levels // PIECES
    pieces = [pl.ds(cut_at * i, cut_at) for i in range(PIECES)]

    def fetch(src, dst, i):
        return pltpu.make_async_copy(src, dst, in_sem.at[i])

    up_in = [[fetch(h_hbm.at[r, p], h.at[r, p], PIECES * (r - 2) + i) for i, p in enumerate(pieces)] for r in (2, 3)]
    low_rows = fetch(h_hbm.at[pl.ds(0, 2)], h.at[pl.ds(0, 2)], 2 * PIECES)
    c_up = fetch(c_hbm.at[rows - 1], c.at[rows - 1], 2 * PIECES + 1)
    small_in = [fetch(src, dst, 2 * PIECES + 2 + i) for i, (src, dst) in enumerate(((rates_hbm, rates), (thr_hbm, thr), (scal_hbm, scal)))]
    z_in = fetch(z_hbm, z, 0)
    c_in = fetch(c_hbm.at[pl.ds(0, rows - 1)], c.at[pl.ds(0, rows - 1)], 2 * PIECES)
    tables_in = [fetch(fwd_hbm, fwd, 1), fetch(inv_hbm, inv, 2)]
    factor_in = [
        fetch(src, dst, 2 * PIECES + 2 + i) for i, (src, dst) in enumerate(((flags_hbm, flags), (cut_hbm, cut), (ksq_hbm, ksq)))
    ]
    for copy in small_in + up_in[0] + up_in[1] + [c_up, low_rows]:
        copy.start()

    last = total - 1
    first = position * rows
    is_root = jnp.logical_and(x == 0, core == 1)
    is_first = position == 1
    is_later_root = jnp.logical_and(is_root, y > 0)

    def along(step):
        p = lax.rem(position + total + step, total)
        return {"lat_0": p // (NY * NC), "lat_1": lax.rem(p // NC, NY), "lat_2": lax.rem(p, NC)}

    def row(k):
        return {"lat_0": jnp.int32(k // NC), "lat_1": y, "lat_2": jnp.int32(k % NC)}

    def root(k):
        return {"lat_0": jnp.int32(0), "lat_1": jnp.int32(k), "lat_2": jnp.int32(1)}

    def signal(sem, device):
        pl.semaphore_signal(sem, inc=1, device_id=device, device_id_type=MESH)

    barrier = pltpu.get_barrier_semaphore()

    @pl.when(position > 0)
    def _():
        signal(barrier, along(-1))

    @pl.when(is_root)
    def _():
        for k in range(NX * NC):
            if k != 1:
                signal(barrier, row(k))

    @pl.when(is_first)
    def _():
        for k in range(1, NY):
            signal(barrier, root(k))

    to_start = jnp.logical_and(position > 1, jnp.logical_or(y == 0, is_root))

    @pl.when(to_start)
    def _():
        signal(barrier, {"lat_0": jnp.int32(0), "lat_1": jnp.int32(0), "lat_2": jnp.int32(0)})

    greeted = jnp.where(is_first, 0, 1) + jnp.where(position < last, 1, 0)
    greeted = greeted + jnp.where(position == 0, NX * NC - 2 + NY - 1, 0)
    pl.semaphore_wait(barrier, greeted)

    @pl.when(position < last)
    def _():
        signal(low_in, along(1))

    def landed(ref, sem):
        pltpu.make_async_copy(ref, ref, sem).wait()

    def halo_copy(side, field, levs=slice(None)):
        step, h_row, c_row = ((1, rows - 2, rows - 1), (-1, 0, 0))[side]
        src = c.at[c_row, levs] if field == 2 else h.at[h_row + field, levs]
        return pltpu.make_async_remote_copy(
            src, halo.at[side, field, levs], halo_send.at[side], halo_recv.at[side],
            device_id=along(step), device_id_type=MESH,
        )

    own_mean[...] = jnp.zeros_like(own_mean)

    @pl.when(jnp.logical_and(y > 0, jnp.logical_not(is_root)))
    def _():
        mean_in[1] = jnp.zeros_like(mean_in[1])

    base[:, :, nlon:] = jnp.zeros((rows, levels, base.shape[2] - nlon), jnp.float32)

    @pl.when(position == 0)
    def _():
        halo[0] = jnp.zeros_like(halo[0])

    @pl.when(position == last)
    def _():
        halo[1] = jnp.zeros_like(halo[1])

    for field in (0, 1):
        for arrived, levs in zip(up_in[field], pieces):
            arrived.wait()

            @pl.when(core == 0)
            def _():
                halo_copy(0, field, levs).start()

    for copy in small_in:
        copy.wait()

    lane = lax.broadcasted_iota(jnp.int32, (8, HALF), 1)
    tile = jnp.zeros((8, HALF), jnp.float32)
    sub = lax.broadcasted_iota(jnp.int32, (8, 1), 0)

    def levels_of(ref, start):
        value = jnp.zeros((8, 1), jnp.float32)
        for k in range(8):
            value = jnp.where(sub == k, ref[start + k], value)
        return value

    full = nlon // HALF
    groups = range(levels // 8)
    rate_of = [levels_of(rates, 8 * g) for g in groups]
    threshold_of = [levels_of(thr, 8 * g) for g in groups]
    scaled_threshold = [LOG2E * value for value in threshold_of]
    wide, rest = [0.0 for g in groups], [0.0 for g in groups]
    for r in order:
        if r == 0:
            c_up.wait()

            @pl.when(core == 0)
            def _():
                halo_copy(0, 2).start()

            low_rows.wait()
        for g in groups:
            lev = pl.ds(8 * g, 8)
            exps = [
                jnp.exp2(h[r, lev, HALF * j : HALF * (j + 1)] * LOG2E - scaled_threshold[g]) for j in range(full)
            ]
            logs = jnp.log2(product_of(exps[0:6])) + jnp.log2(product_of(exps[6:full]))
            wide[g] = wide[g] + scal[first + r] * logs
            logs = jnp.log2(1.0 + jnp.exp2(h[r, lev, HALF * full : nlon] * LOG2E - scaled_threshold[g]))
            rest[g] = rest[g] + scal[first + r] * logs
    short = jnp.zeros((8, HALF * (full + 1) - nlon), jnp.float32)
    for g in groups:
        sums = jnp.sum(wide[g] + jnp.concatenate([rest[g], short], axis=1), axis=1, keepdims=True)
        tile = jnp.where(lane == g, (-1.0 / LOG2E) * rate_of[g] * sums, tile)
        level_rates[g] = jnp.broadcast_to(rate_of[g], (8, HALF))
        level_thresholds[g] = jnp.broadcast_to(threshold_of[g], (8, HALF))
    part[...] = tile

    members = [*range(NC, NX * NC), 0]

    def mean_copy(slot, source, device):
        return pltpu.make_async_remote_copy(
            source, mean_in.at[slot], mean_send, mean_recv, device_id=device, device_id_type=MESH
        )

    def send_b(device):
        mean_copy(1, part, device).start()

    def part_copy(slot):
        return pltpu.make_async_remote_copy(
            part, box.at[slot], up_send, x_recv, device_id=row(1), device_id_type=MESH
        )

    sends_part = jnp.logical_and(jnp.logical_not(is_root), position > 0)

    @pl.when(sends_part)
    def _():
        part_copy(x * NC + core).start()

    @pl.when(position == 0)
    def _():
        send_b(row(1))

    @pl.when(jnp.logical_and(core != 0, position < last))
    def _():
        for field in range(3):
            halo_copy(0, field).start()

    @pl.when(position == 0)
    def _():
        mean_in[1] = part[...]
        for k in range(1, NY):
            for member in members[2 * k - 2 : 2 * k]:
                send_b(row(member))
            send_b(root(k))

    for copy in [c_in, z_in] + factor_in + tables_in:
        copy.start()

    z_in.wait()
    c_in.wait()


    def inv_cos(r):
        return scal[nlat + first + r]

    def face(f):
        return scal[2 * nlat + first + f]

    def west(a):
        return pltpu.roll(a, 1, axis=1)

    def east(a):
        return pltpu.roll(a, nlon - 1, axis=1)

    def local_terms(g, carry):
        lev = pl.ds(pl.multiple_of(8 * g, 8), 8)
        hr = [h[r, lev, :] for r in range(rows)]
        rate, threshold = level_rates[g][:, 0:1], level_thresholds[g][:, 0:1]
        cr = [c[r, lev, :] for r in range(rows)]
        low = face(1) * (cr[0] + cr[1])
        high = face(3) * (cr[2] + cr[3])
        s_lo[lev, :] = low
        s_hi[lev, :] = high
        f1 = low * (7.0 * (hr[0] + hr[1]) - hr[2])
        f2 = face(2) * (cr[1] + cr[2]) * (7.0 * (hr[1] + hr[2]) - (hr[0] + hr[3]))
        f3 = high * (7.0 * (hr[2] + hr[3]) - hr[1])
        terms = [f1, f2 - f1, f3 - f2, -f3]
        for r in range(rows):
            pair = hr[r] + east(hr[r])
            zr = z[r, lev, :]
            speed = zr + east(zr)
            flux = speed * (8.0 * pair - (west(pair) + east(pair))) * (1.0 / 24.0)
            s = hr[r] - threshold
            source = rate * jnp.log(1.0 + jnp.exp(s))
            base[r, lev, 0:nlon] = (hr[r] - source) - (flux - west(flux)) - terms[r] * inv_cos(r)
        return carry

    lax.fori_loop(0, levels // 8, local_terms, 0)

    @pl.when(position > 0)
    def _():
        pl.semaphore_wait(low_in, 1)
        for field in range(3):
            halo_copy(1, field).start()

    for copy in factor_in:
        copy.wait()
    for r in range(rows):
        cutoff = cut[first + r].astype(jnp.float32)
        flag = flags[first + r].astype(jnp.float32)
        factor[r] = flag * (1.0 - jnp.minimum(1.0, cutoff * cutoff * ksq[...]))

    def sum_copy():
        return pltpu.make_async_remote_copy(
            part, box.at[NX * NC + y], up_send, y_recv, device_id=root(0), device_id_type=MESH
        )

    def gather_row(senders):
        landed(box.at[pl.ds(0, len(senders))], x_recv)
        acc = part[...]
        for k in senders:
            acc = acc + box[k]
        return acc

    @pl.when(is_later_root)
    def _():
        part[...] = gather_row(members)
        sum_copy().start()

    for copy in tables_in:
        copy.wait()
    lanes = lax.broadcasted_iota(jnp.int32, (16, HALF), 1)
    units = 2 * levels
    blocks = levels // 16

    tail = nlon - HALF * (RADIX - 1)

    def piece(ref, j):
        if j < RADIX - 1:
            return ref[:, HALF * j : HALF * (j + 1)]
        return jnp.concatenate([ref[:, HALF * j : nlon], jnp.zeros((16, HALF - tail), jnp.float32)], axis=1)

    def with_halo(r, lev, j):
        side, near, far, edge, inner, f, through, outer = (
            (0, 1, 0, 0, 1, 0, s_lo, 0) if r < 2 else (1, 0, 1, rows - 1, rows - 2, rows, s_hi, rows - 1)
        )
        beside = piece(halo.at[side, near, lev], j)
        term = piece(through.at[lev], j) * beside
        if r == outer:
            speed = face(f) * (piece(halo.at[side, 2, lev], j) + piece(c.at[edge, lev], j))
            flux = speed * (
                7.0 * (beside + piece(h.at[edge, lev], j)) - (piece(halo.at[side, far, lev], j) + piece(h.at[inner, lev], j))
            )
            term = term + flux
        sign = 1.0 if r in (0, 2) else -1.0
        return base[r, lev, HALF * j : HALF * (j + 1)] + term * (sign * inv_cos(r))

    def product(hilo, table):
        first_part = jnp.dot(hilo, table[0], preferred_element_type=jnp.float32)
        second = jnp.dot(hilo[0:units], table[1], preferred_element_type=jnp.float32)
        return first_part[0:units] + first_part[units : 2 * units] + second

    def filter_rows(row0, known=None):
        def block_of(b):
            return row0 + b // blocks, pl.ds(16 * (b % blocks), 16), pl.ds(16 * b, 16), pl.ds(units + 16 * b, 16)

        def forward(b):
            r, lev, at_hi, at_lo = block_of(b)
            v = [with_halo(r, lev, j) for j in range(RADIX)]
            for j in range(RADIX):
                base[r, lev, HALF * j : HALF * (j + 1)] = v[j]
            u = [v[0]] + [
                pltpu.roll(jnp.where(lanes >= HALF - 8 * j, v[j - 1], v[j]), 8 * j, axis=1) for j in range(1, RADIX)
            ]
            e = [u[0]] + [u[j] + u[RADIX - j] for j in range(1, 6)] + [u[6]]
            o = [u[j] - u[RADIX - j] for j in range(1, 6)]
            even, odd = twelve(e, o)
            halves = [(even[0], even[6])] + [(even[m], odd[m - 1]) for m in range(1, 6)]
            for m, pair in enumerate(halves):
                for k, value in enumerate(pair):
                    hi, lo = split(value)
                    ymat[m, at_hi, HALF * k : HALF * (k + 1)] = hi
                    ymat[m, at_lo, HALF * k : HALF * (k + 1)] = lo

        def backward(b):
            r, lev, at, _ = block_of(b)
            w = [[wmat[m, at, HALF * k : HALF * (k + 1)] for k in range(2)] for m in range(RADIX // 2)]
            even, odd = twelve([w[0][0]] + [w[m][0] for m in range(1, 6)] + [w[0][1]], [w[m][1] for m in range(1, 6)])
            removed = [even[0]] + [even[j] + odd[j - 1] for j in range(1, 6)] + [even[6]]
            removed += [even[RADIX - j] - odd[RADIX - j - 1] for j in range(7, RADIX)]
            back = [removed[0]] + [pltpu.roll(removed[j], HALF - 8 * j, axis=1) for j in range(1, RADIX)]
            for j in range(RADIX):
                kept = base[r, lev, HALF * j : HALF * (j + 1)]
                if row0 == 0:
                    kept = kept - shifts[b % blocks]
                if j < RADIX - 1:
                    out[r, lev, HALF * j : HALF * (j + 1)] = kept - jnp.where(lanes < count - 8 * j, back[j], back[j + 1])
                else:
                    out[r, lev, HALF * j : nlon] = (kept - back[j])[:, 0:tail]

        for b in range(2 * blocks):
            forward(b)
        shifts = known() if known else None
        for m in range(RADIX // 2):
            waves = product(ymat[m], (fwd[0, m], fwd[1, m]))
            scaled = jnp.concatenate(
                [waves[r * levels : (r + 1) * levels] * factor[row0 + r, m : m + 1, :] for r in range(2)], axis=0
            )
            wmat[m] = product(jnp.concatenate(split(scaled), axis=0), (inv[0, m], inv[1, m]))
        if row0 == 0:
            for r in (2, 3):
                for b in range(blocks):
                    lev = pl.ds(16 * b, 16)
                    out[r, lev, :] = out[r, lev, :] - shifts[b]
        for b in range(2 * blocks):
            backward(b)

    @pl.when(position < last)
    def _():
        landed(halo.at[1], halo_recv.at[1])

    filter_rows(2)

    @pl.when(is_first)
    def _():
        landed(box.at[pl.ds(NX * NC + 1, NY - 1)], y_recv)
        acc = box[NX * NC + 1]
        for k in range(2, NY):
            acc = acc + box[NX * NC + k]
        mean_in[0] = gather_row(members[:-1]) + acc
        for k in range(1, NY):
            for member in members[2 * k - 2 : 2 * k]:
                mean_copy(0, mean_in.at[0], row(member)).start()
            mean_copy(0, mean_in.at[0], root(k)).start()
        mean_copy(0, mean_in.at[0], row(0)).start()

    @pl.when(position > 0)
    def _():
        landed(halo.at[0], halo_recv.at[0])

    def mean_columns(value):
        return [jnp.sum(jnp.where(lane == g, value, 0.0), axis=1, keepdims=True) for g in groups]

    def known_shifts():
        @pl.when(is_first)
        def _():
            landed(mean_in.at[1], mean_recv)
            own_mean[...] = (mean_in[0] + mean_in[1]) * (1.0 / area)

        columns = mean_columns(own_mean[...])
        return [jnp.concatenate(columns[2 * b : 2 * b + 2], axis=0) for b in range(blocks)]

    filter_rows(0, known_shifts)

    in_two = jnp.logical_or(is_later_root, jnp.logical_and(y == 0, position > 1))

    @pl.when(in_two)
    def _():
        landed(mean_in, mean_recv)

    @pl.when(jnp.logical_not(jnp.logical_or(in_two, is_first)))
    def _():
        landed(mean_in.at[0], mean_recv)

    @pl.when(is_later_root)
    def _():
        own_mean[...] = mean_in[0] + mean_in[1]
        for member in members:
            mean_copy(0, own_mean, row(member)).start()

    @pl.when(jnp.logical_not(is_first))
    def _():
        for g, shift in zip(groups, mean_columns((mean_in[0] + mean_in[1]) * (1.0 / area))):
            lev = pl.ds(8 * g, 8)
            for r in range(rows):
                out[r, lev, :] = out[r, lev, :] - shift

    for side, sender in ((0, position < last), (1, position > 0)):

        @pl.when(sender)
        def _():
            landed(halo.at[side], halo_send.at[side])

    @pl.when(position <= 1)
    def _():
        landed(box.at[pl.ds(0, len(members) + NY - 1)], mean_send)

    @pl.when(is_later_root)
    def _():
        landed(box.at[pl.ds(0, len(members))], mean_send)

    @pl.when(position > 1)
    def _():
        landed(part, up_send)


def local(height, zonal, merid, rates, thresholds, flags, cutoffs):
    rows, levels, nlon = height.shape
    nlat = rows * NX * NY * NC
    fwd, inv, ksq = filter_tables(nlon)
    scalars, cos_sum = row_scalars(nlat)
    tiles = RADIX // 2
    dims = (rows, levels, nlon, nlat)
    f32, bf16 = jnp.float32, jnp.bfloat16
    vmem, smem, dma = pltpu.VMEM, pltpu.SMEM, pltpu.SemaphoreType.DMA
    operands = (height, zonal, merid, rates, thresholds, flags, cutoffs, scalars, ksq, fwd, inv)
    operands = [pltpu.with_memory_space_constraint(jnp.asarray(a), pltpu.HBM) for a in operands]
    return pl.pallas_call(
        functools.partial(kernel, dims, nlon * cos_sum),
        out_shape=vmem(height.shape, f32),
        in_specs=[pl.BlockSpec(memory_space=pltpu.HBM)] * len(operands),
        out_specs=pl.BlockSpec(memory_space=vmem),
        scratch_shapes=[
            vmem(height.shape, f32), vmem(height.shape, f32), vmem(height.shape, f32),
            smem(rates.shape, f32), smem(thresholds.shape, f32), smem(flags.shape, jnp.int32),
            smem(cutoffs.shape, jnp.int32), smem(scalars.shape, f32),
            vmem(ksq.shape, f32), vmem(fwd.shape, bf16), vmem(inv.shape, bf16),
            vmem((2, 3, levels, nlon), f32), vmem((rows, levels, RADIX * HALF), f32),
            vmem((levels, nlon), f32), vmem((levels, nlon), f32), vmem((rows, 8, 2 * HALF), f32),
            vmem((tiles, 4 * levels, 2 * HALF), bf16), vmem((tiles, 2 * levels, 2 * HALF), f32),
            vmem((8, HALF), f32), vmem((NX * NC + NY, 8, HALF), f32), vmem((2, 8, HALF), f32),
            vmem((8, HALF), f32),
            vmem((levels // 8, 8, HALF), f32), vmem((levels // 8, 8, HALF), f32),
            dma((2 * PIECES + 5,)), dma((2,)), dma((2,)), dma, dma, dma, dma, dma, pltpu.SemaphoreType.REGULAR,
        ],
        compiler_params=pltpu.CompilerParams(collective_id=0, has_side_effects=True, vmem_limit_bytes=16 * 2**20),
        name="advect_filter",
    )(*operands)


def solution(mesh):
    finer = Mesh(
        mesh.devices.reshape(mesh.shape["member"], NX, NY, NC), ("member", "lat_0", "lat_1", "lat_2")
    )
    whole = P(("member", "lat_0", "lat_1", "lat_2"), None, None)
    placed = (whole, whole, whole, P("member"), P("member"), P(), P())
    return jax.shard_map(local, mesh=finer, in_specs=placed, out_specs=whole, check_vma=False)
```

```python
import functools
import math

import jax
import jax.numpy as jnp
import numpy as np
from jax import lax
from jax.experimental import pallas as pl
from jax.experimental.pallas import tpu as pltpu
from jax.sharding import Mesh
from jax.sharding import PartitionSpec as P

MESH = pl.DeviceIdType.MESH
NX, NY, NC = 8, 8, 2
PIECES = 2
NEAR_ROOTS = (1, 2)
RADIX = 12
HALF = 128
ROOT = math.sqrt(0.75)
LOG2E = math.log2(math.e)


def filter_tables(nlon):
    count = nlon // RADIX
    tiles = RADIX // 2
    fwd = np.zeros((tiles, 2 * HALF, 2 * HALF))
    inv = np.zeros((tiles, 2 * HALF, 2 * HALF))
    waves = np.zeros((8, 2 * HALF), np.int64)
    r = np.arange(count)

    def trig(k):
        angle = 2.0 * np.pi / nlon * ((r * k) % nlon)
        return np.cos(angle), np.sin(angle)

    def real_part(base, shift):
        lane = base
        for q in range(count // 2 + 1):
            k = RADIX * q + shift
            if k > nlon // 2:
                continue
            cos, sin = trig(k)
            weight = (1.0 if k in (0, nlon // 2) else 2.0) / nlon
            rows = slice(base, base + count)
            fwd[0, rows, lane] = cos
            inv[0, lane, rows] = cos * weight
            waves[0, lane] = k
            lane += 1
            if k not in (0, nlon // 2):
                fwd[0, rows, lane] = sin
                inv[0, lane, rows] = sin * weight
                waves[0, lane] = k
                lane += 1
        assert lane == base + count

    real_part(0, 0)
    real_part(HALF, RADIX // 2)
    for m in range(1, tiles):
        for q in range(count):
            k = RADIX * q + m
            cos, sin = trig(k)
            fwd[m, 0:count, q] = cos
            fwd[m, HALF : HALF + count, q] = -sin
            fwd[m, 0:count, HALF + q] = sin
            fwd[m, HALF : HALF + count, HALF + q] = cos
            waves[m, q] = waves[m, HALF + q] = min(k, nlon - k)
        inv[m] = fwd[m].T * (2.0 / nlon)
    inv_square = 1.0 / np.maximum(waves, 1).astype(np.float64) ** 2

    def halves(table):
        hi = table.astype(np.float32).astype(jnp.bfloat16)
        lo = (table - hi.astype(np.float64)).astype(np.float32).astype(jnp.bfloat16)
        return np.stack([hi, lo])

    return halves(fwd), halves(inv), inv_square.astype(np.float32)


def row_scalars(nlat):
    rows = np.arange(nlat)
    cos_row = np.sin(np.pi * (rows + 0.5) / nlat)
    faces = np.arange(nlat + 1)
    cos_face = np.where((faces > 0) & (faces < nlat), np.sin(np.pi * faces / nlat), 0.0)
    table = np.zeros((3 * nlat + HALF,))
    table[0:nlat] = cos_row
    table[nlat : 2 * nlat] = 1.0 / cos_row
    table[2 * nlat : 3 * nlat + 1] = cos_face / 24.0
    return table.astype(np.float32), float(np.sum(cos_row))


def twelve(e, o):
    plus, minus = e[0] + e[6], e[0] - e[6]
    e15p, e15m, e24p, e24m = e[1] + e[5], e[1] - e[5], e[2] + e[4], e[2] - e[4]
    a, b = plus + e24p, e15p + e[3]
    big, mid = ROOT * e15m, minus + 0.5 * e24m
    c, d = plus - 0.5 * e24p, 0.5 * e15p - e[3]
    even = [a + b, mid + big, c + d, minus - e24m, c - d, mid - big, a - b]
    o15p, o15m, o24p, o24m = o[0] + o[4], o[0] - o[4], o[1] + o[3], o[1] - o[3]
    f, g = 0.5 * o15p + o[2], ROOT * o24p
    s, t = ROOT * o15m, ROOT * o24m
    odd = [f + g, s + t, o15p - o[2], s - t, f - g]
    return even, odd


def product_of(exps):
    result = 1.0 + exps[0]
    for e in exps[1:]:
        result = result * (1.0 + e)
    return result


def split(x):
    hi = x.astype(jnp.bfloat16)
    return hi, (x - hi.astype(jnp.float32)).astype(jnp.bfloat16)


def kernel(
    dims, area,
    h_hbm, z_hbm, c_hbm, rates_hbm, thr_hbm, flags_hbm, cut_hbm, scal_hbm, ksq_hbm, fwd_hbm, inv_hbm,
    out,
    h, z, c, rates, thr, flags, cut, scal, ksq, fwd, inv,
    halo, base, s_lo, s_hi, factor, ymat, wmat, part, box, mean_in, own_mean, level_rates, level_thresholds,
    in_sem, halo_send, halo_recv, up_send, x_recv, y_recv, mean_send, mean_recv, low_in,
):
    rows, levels, nlon, nlat = dims
    count = nlon // RADIX
    x, y, core = lax.axis_index("lat_0"), lax.axis_index("lat_1"), lax.axis_index("lat_2")
    position = (x * NY + y) * NC + core
    total = NX * NY * NC

    order = (2, 3, 0, 1)
    cut_at = levels // PIECES
    pieces = [pl.ds(cut_at * i, cut_at) for i in range(PIECES)]

    def fetch(src, dst, i):
        return pltpu.make_async_copy(src, dst, in_sem.at[i])

    up_in = [[fetch(h_hbm.at[r, p], h.at[r, p], PIECES * (r - 2) + i) for i, p in enumerate(pieces)] for r in (2, 3)]
    low_rows = fetch(h_hbm.at[pl.ds(0, 2)], h.at[pl.ds(0, 2)], 2 * PIECES)
    c_up = fetch(c_hbm.at[rows - 1], c.at[rows - 1], 2 * PIECES + 1)
    small_in = [fetch(src, dst, 2 * PIECES + 2 + i) for i, (src, dst) in enumerate(((rates_hbm, rates), (thr_hbm, thr), (scal_hbm, scal)))]
    z_in = fetch(z_hbm, z, 0)
    c_in = fetch(c_hbm.at[pl.ds(0, rows - 1)], c.at[pl.ds(0, rows - 1)], 2 * PIECES)
    tables_in = [fetch(fwd_hbm, fwd, 1), fetch(inv_hbm, inv, 2)]
    factor_in = [
        fetch(src, dst, 2 * PIECES + 2 + i) for i, (src, dst) in enumerate(((flags_hbm, flags), (cut_hbm, cut), (ksq_hbm, ksq)))
    ]
    for copy in small_in + up_in[0] + up_in[1] + [low_rows, c_up]:
        copy.start()

    last = total - 1
    first = position * rows
    is_root = jnp.logical_and(x == 0, core == 1)
    is_first = position == 1
    is_later_root = jnp.logical_and(is_root, y > 0)

    def along(step):
        p = lax.rem(position + total + step, total)
        return {"lat_0": p // (NY * NC), "lat_1": lax.rem(p // NC, NY), "lat_2": lax.rem(p, NC)}

    def row(k):
        return {"lat_0": jnp.int32(k // NC), "lat_1": y, "lat_2": jnp.int32(k % NC)}

    def root(k):
        return {"lat_0": jnp.int32(0), "lat_1": jnp.int32(k), "lat_2": jnp.int32(1)}

    def signal(sem, device):
        pl.semaphore_signal(sem, inc=1, device_id=device, device_id_type=MESH)

    barrier = pltpu.get_barrier_semaphore()

    @pl.when(position > 0)
    def _():
        signal(barrier, along(-1))

    @pl.when(is_root)
    def _():
        for k in range(NX * NC):
            if k != 1:
                signal(barrier, row(k))

    @pl.when(is_first)
    def _():
        for k in range(1, NY):
            signal(barrier, root(k))

    to_start = jnp.logical_and(position > 1, jnp.logical_or(y == 0, is_root))

    @pl.when(to_start)
    def _():
        signal(barrier, {"lat_0": jnp.int32(0), "lat_1": jnp.int32(0), "lat_2": jnp.int32(0)})

    greeted = jnp.where(is_first, 0, 1) + jnp.where(position < last, 1, 0)
    greeted = greeted + jnp.where(position == 0, NX * NC - 2 + NY - 1, 0)
    pl.semaphore_wait(barrier, greeted)

    @pl.when(position < last)
    def _():
        signal(low_in, along(1))

    def landed(ref, sem):
        pltpu.make_async_copy(ref, ref, sem).wait()

    def halo_copy(side, field, levs=slice(None)):
        step, h_row, c_row = ((1, rows - 2, rows - 1), (-1, 0, 0))[side]
        src = c.at[c_row, levs] if field == 2 else h.at[h_row + field, levs]
        return pltpu.make_async_remote_copy(
            src, halo.at[side, field, levs], halo_send.at[side], halo_recv.at[side],
            device_id=along(step), device_id_type=MESH,
        )

    own_mean[...] = jnp.zeros_like(own_mean)

    @pl.when(jnp.logical_and(y > 0, jnp.logical_not(is_root)))
    def _():
        mean_in[1] = jnp.zeros_like(mean_in[1])

    base[:, :, nlon:] = jnp.zeros((rows, levels, base.shape[2] - nlon), jnp.float32)

    @pl.when(position == 0)
    def _():
        halo[0] = jnp.zeros_like(halo[0])

    @pl.when(position == last)
    def _():
        halo[1] = jnp.zeros_like(halo[1])

    for field in (0, 1):
        for arrived, levs in zip(up_in[field], pieces):
            arrived.wait()

            @pl.when(core == 0)
            def _():
                halo_copy(0, field, levs).start()

    for copy in small_in:
        copy.wait()

    lane = lax.broadcasted_iota(jnp.int32, (8, HALF), 1)
    tile = jnp.zeros((8, HALF), jnp.float32)
    sub = lax.broadcasted_iota(jnp.int32, (8, 1), 0)

    def levels_of(ref, start):
        value = jnp.zeros((8, 1), jnp.float32)
        for k in range(8):
            value = jnp.where(sub == k, ref[start + k], value)
        return value

    full = nlon // HALF
    groups = range(levels // 8)
    rate_of = [levels_of(rates, 8 * g) for g in groups]
    threshold_of = [levels_of(thr, 8 * g) for g in groups]
    scaled_threshold = [LOG2E * value for value in threshold_of]
    wide, rest = [0.0 for g in groups], [0.0 for g in groups]
    for r in order:
        if r == 0:
            low_rows.wait()
        for g in groups:
            lev = pl.ds(8 * g, 8)
            exps = [
                jnp.exp2(h[r, lev, HALF * j : HALF * (j + 1)] * LOG2E - scaled_threshold[g]) for j in range(full)
            ]
            logs = jnp.log2(product_of(exps[0:6])) + jnp.log2(product_of(exps[6:full]))
            wide[g] = wide[g] + scal[first + r] * logs
            logs = jnp.log2(1.0 + jnp.exp2(h[r, lev, HALF * full : nlon] * LOG2E - scaled_threshold[g]))
            rest[g] = rest[g] + scal[first + r] * logs
    short = jnp.zeros((8, HALF * (full + 1) - nlon), jnp.float32)
    for g in groups:
        sums = jnp.sum(wide[g] + jnp.concatenate([rest[g], short], axis=1), axis=1, keepdims=True)
        tile = jnp.where(lane == g, (-1.0 / LOG2E) * rate_of[g] * sums, tile)
        level_rates[g] = jnp.broadcast_to(rate_of[g], (8, HALF))
        level_thresholds[g] = jnp.broadcast_to(threshold_of[g], (8, HALF))
    part[...] = tile

    members = [*range(NC, NX * NC), 0]

    def mean_copy(slot, source, device):
        return pltpu.make_async_remote_copy(
            source, mean_in.at[slot], mean_send, mean_recv, device_id=device, device_id_type=MESH
        )

    def send_b(device):
        mean_copy(1, part, device).start()

    def part_copy(slot):
        return pltpu.make_async_remote_copy(
            part, box.at[slot], up_send, x_recv, device_id=row(1), device_id_type=MESH
        )

    sends_part = jnp.logical_and(jnp.logical_not(is_root), position > 0)

    @pl.when(sends_part)
    def _():
        part_copy(x * NC + core).start()

    @pl.when(position == 0)
    def _():
        send_b(row(1))

    c_up.wait()

    @pl.when(jnp.logical_and(core != 0, position < last))
    def _():
        halo_copy(0, 0).start()
        halo_copy(0, 1).start()

    @pl.when(position < last)
    def _():
        halo_copy(0, 2).start()

    @pl.when(position == 0)
    def _():
        mean_in[1] = part[...]
        for k in range(1, NY):
            for member in members[2 * k - 2 : 2 * k]:
                send_b(row(member))
            send_b(root(k))

    for copy in [c_in, z_in] + factor_in + tables_in:
        copy.start()

    z_in.wait()
    c_in.wait()


    def inv_cos(r):
        return scal[nlat + first + r]

    def face(f):
        return scal[2 * nlat + first + f]

    def west(a):
        return pltpu.roll(a, 1, axis=1)

    def east(a):
        return pltpu.roll(a, nlon - 1, axis=1)

    def local_terms(g, carry):
        lev = pl.ds(pl.multiple_of(8 * g, 8), 8)
        hr = [h[r, lev, :] for r in range(rows)]
        rate, threshold = level_rates[g][:, 0:1], level_thresholds[g][:, 0:1]
        cr = [c[r, lev, :] for r in range(rows)]
        low = face(1) * (cr[0] + cr[1])
        high = face(3) * (cr[2] + cr[3])
        s_lo[lev, :] = low
        s_hi[lev, :] = high
        f1 = low * (7.0 * (hr[0] + hr[1]) - hr[2])
        f2 = face(2) * (cr[1] + cr[2]) * (7.0 * (hr[1] + hr[2]) - (hr[0] + hr[3]))
        f3 = high * (7.0 * (hr[2] + hr[3]) - hr[1])
        terms = [f1, f2 - f1, f3 - f2, -f3]
        for r in range(rows):
            pair = hr[r] + east(hr[r])
            zr = z[r, lev, :]
            speed = zr + east(zr)
            flux = speed * (8.0 * pair - (west(pair) + east(pair))) * (1.0 / 24.0)
            s = hr[r] - threshold
            source = rate * jnp.log(1.0 + jnp.exp(s))
            base[r, lev, 0:nlon] = (hr[r] - source) - (flux - west(flux)) - terms[r] * inv_cos(r)
        return carry

    lax.fori_loop(0, levels // 8, local_terms, 0)

    @pl.when(position > 0)
    def _():
        pl.semaphore_wait(low_in, 1)
        for field in range(3):
            halo_copy(1, field).start()

    for copy in factor_in:
        copy.wait()
    for r in range(rows):
        cutoff = cut[first + r].astype(jnp.float32)
        flag = flags[first + r].astype(jnp.float32)
        factor[r] = flag * (1.0 - jnp.minimum(1.0, cutoff * cutoff * ksq[...]))

    def sum_copy():
        return pltpu.make_async_remote_copy(
            part, box.at[NX * NC + y], up_send, y_recv, device_id=root(0), device_id_type=MESH
        )

    def gather_row(senders):
        landed(box.at[pl.ds(0, len(senders))], x_recv)
        acc = part[...]
        for k in senders:
            acc = acc + box[k]
        return acc

    @pl.when(is_later_root)
    def _():
        part[...] = gather_row(members)
        sum_copy().start()

    for copy in tables_in:
        copy.wait()
    lanes = lax.broadcasted_iota(jnp.int32, (16, HALF), 1)
    units = 2 * levels
    blocks = levels // 16

    tail = nlon - HALF * (RADIX - 1)

    def piece(ref, j):
        if j < RADIX - 1:
            return ref[:, HALF * j : HALF * (j + 1)]
        return jnp.concatenate([ref[:, HALF * j : nlon], jnp.zeros((16, HALF - tail), jnp.float32)], axis=1)

    def with_halo(r, lev, j):
        side, near, far, edge, inner, f, through, outer = (
            (0, 1, 0, 0, 1, 0, s_lo, 0) if r < 2 else (1, 0, 1, rows - 1, rows - 2, rows, s_hi, rows - 1)
        )
        beside = piece(halo.at[side, near, lev], j)
        term = piece(through.at[lev], j) * beside
        if r == outer:
            speed = face(f) * (piece(halo.at[side, 2, lev], j) + piece(c.at[edge, lev], j))
            flux = speed * (
                7.0 * (beside + piece(h.at[edge, lev], j)) - (piece(halo.at[side, far, lev], j) + piece(h.at[inner, lev], j))
            )
            term = term + flux
        sign = 1.0 if r in (0, 2) else -1.0
        return base[r, lev, HALF * j : HALF * (j + 1)] + term * (sign * inv_cos(r))

    def product(hilo, table):
        first_part = jnp.dot(hilo, table[0], preferred_element_type=jnp.float32)
        second = jnp.dot(hilo[0:units], table[1], preferred_element_type=jnp.float32)
        return first_part[0:units] + first_part[units : 2 * units] + second

    def filter_rows(row0, shifts=None):
        def block_of(b):
            return row0 + b // blocks, pl.ds(16 * (b % blocks), 16), pl.ds(16 * b, 16), pl.ds(units + 16 * b, 16)

        def forward(b):
            r, lev, at_hi, at_lo = block_of(b)
            v = [with_halo(r, lev, j) for j in range(RADIX)]
            for j in range(RADIX):
                base[r, lev, HALF * j : HALF * (j + 1)] = v[j]
            u = [v[0]] + [
                pltpu.roll(jnp.where(lanes >= HALF - 8 * j, v[j - 1], v[j]), 8 * j, axis=1) for j in range(1, RADIX)
            ]
            e = [u[0]] + [u[j] + u[RADIX - j] for j in range(1, 6)] + [u[6]]
            o = [u[j] - u[RADIX - j] for j in range(1, 6)]
            even, odd = twelve(e, o)
            halves = [(even[0], even[6])] + [(even[m], odd[m - 1]) for m in range(1, 6)]
            for m, pair in enumerate(halves):
                for k, value in enumerate(pair):
                    hi, lo = split(value)
                    ymat[m, at_hi, HALF * k : HALF * (k + 1)] = hi
                    ymat[m, at_lo, HALF * k : HALF * (k + 1)] = lo

        def backward(b):
            r, lev, at, _ = block_of(b)
            w = [[wmat[m, at, HALF * k : HALF * (k + 1)] for k in range(2)] for m in range(RADIX // 2)]
            even, odd = twelve([w[0][0]] + [w[m][0] for m in range(1, 6)] + [w[0][1]], [w[m][1] for m in range(1, 6)])
            removed = [even[0]] + [even[j] + odd[j - 1] for j in range(1, 6)] + [even[6]]
            removed += [even[RADIX - j] - odd[RADIX - j - 1] for j in range(7, RADIX)]
            back = [removed[0]] + [pltpu.roll(removed[j], HALF - 8 * j, axis=1) for j in range(1, RADIX)]
            for j in range(RADIX):
                kept = base[r, lev, HALF * j : HALF * (j + 1)]
                if row0 == 0:
                    kept = kept - shifts[b % blocks]
                if j < RADIX - 1:
                    out[r, lev, HALF * j : HALF * (j + 1)] = kept - jnp.where(lanes < count - 8 * j, back[j], back[j + 1])
                else:
                    out[r, lev, HALF * j : nlon] = (kept - back[j])[:, 0:tail]

        for b in range(2 * blocks):
            forward(b)
        for m in range(RADIX // 2):
            waves = product(ymat[m], (fwd[0, m], fwd[1, m]))
            scaled = jnp.concatenate(
                [waves[r * levels : (r + 1) * levels] * factor[row0 + r, m : m + 1, :] for r in range(2)], axis=0
            )
            wmat[m] = product(jnp.concatenate(split(scaled), axis=0), (inv[0, m], inv[1, m]))
        if row0 == 0:
            for r in (2, 3):
                for b in range(blocks):
                    lev = pl.ds(16 * b, 16)
                    out[r, lev, :] = out[r, lev, :] - shifts[b]
        for b in range(2 * blocks):
            backward(b)

    @pl.when(position < last)
    def _():
        landed(halo.at[1], halo_recv.at[1])

    filter_rows(2)

    @pl.when(is_first)
    def _():
        landed(box.at[pl.ds(NX * NC + 1, NY - 1)], y_recv)
        acc = box[NX * NC + 1]
        for k in range(2, NY):
            acc = acc + box[NX * NC + k]
        mean_in[0] = gather_row(members[:-1]) + acc
        for k in range(1, NY):
            for member in members[2 * k - 2 : 2 * k]:
                mean_copy(0, mean_in.at[0], row(member)).start()
            if k in NEAR_ROOTS:
                mean_copy(0, mean_in.at[0], root(k)).start()

    @pl.when(position > 0)
    def _():
        landed(halo.at[0], halo_recv.at[0])

    @pl.when(is_first)
    def _():
        landed(mean_in.at[1], mean_recv)
        own_mean[...] = (mean_in[0] + mean_in[1]) * (1.0 / area)

    def mean_columns(value):
        return [jnp.sum(jnp.where(lane == g, value, 0.0), axis=1, keepdims=True) for g in groups]

    columns = mean_columns(own_mean[...])
    shifts = [jnp.concatenate(columns[2 * b : 2 * b + 2], axis=0) for b in range(blocks)]
    filter_rows(0, shifts)

    @pl.when(is_first)
    def _():
        for k in range(1, NY):
            if k not in NEAR_ROOTS:
                mean_copy(0, mean_in.at[0], root(k)).start()
        mean_copy(0, mean_in.at[0], row(0)).start()

    in_two = jnp.logical_or(is_later_root, jnp.logical_and(y == 0, position > 1))

    @pl.when(in_two)
    def _():
        landed(mean_in, mean_recv)

    @pl.when(jnp.logical_not(jnp.logical_or(in_two, is_first)))
    def _():
        landed(mean_in.at[0], mean_recv)

    @pl.when(is_later_root)
    def _():
        own_mean[...] = mean_in[0] + mean_in[1]
        for member in members:
            mean_copy(0, own_mean, row(member)).start()

    @pl.when(jnp.logical_not(is_first))
    def _():
        for g, shift in zip(groups, mean_columns((mean_in[0] + mean_in[1]) * (1.0 / area))):
            lev = pl.ds(8 * g, 8)
            for r in range(rows):
                out[r, lev, :] = out[r, lev, :] - shift

    for side, sender in ((0, position < last), (1, position > 0)):

        @pl.when(sender)
        def _():
            landed(halo.at[side], halo_send.at[side])

    @pl.when(position <= 1)
    def _():
        landed(box.at[pl.ds(0, len(members) + NY - 1)], mean_send)

    @pl.when(is_later_root)
    def _():
        landed(box.at[pl.ds(0, len(members))], mean_send)

    @pl.when(position > 1)
    def _():
        landed(part, up_send)


def local(height, zonal, merid, rates, thresholds, flags, cutoffs):
    rows, levels, nlon = height.shape
    nlat = rows * NX * NY * NC
    fwd, inv, ksq = filter_tables(nlon)
    scalars, cos_sum = row_scalars(nlat)
    tiles = RADIX // 2
    dims = (rows, levels, nlon, nlat)
    f32, bf16 = jnp.float32, jnp.bfloat16
    vmem, smem, dma = pltpu.VMEM, pltpu.SMEM, pltpu.SemaphoreType.DMA
    operands = (height, zonal, merid, rates, thresholds, flags, cutoffs, scalars, ksq, fwd, inv)
    operands = [pltpu.with_memory_space_constraint(jnp.asarray(a), pltpu.HBM) for a in operands]
    return pl.pallas_call(
        functools.partial(kernel, dims, nlon * cos_sum),
        out_shape=vmem(height.shape, f32),
        in_specs=[pl.BlockSpec(memory_space=pltpu.HBM)] * len(operands),
        out_specs=pl.BlockSpec(memory_space=vmem),
        scratch_shapes=[
            vmem(height.shape, f32), vmem(height.shape, f32), vmem(height.shape, f32),
            smem(rates.shape, f32), smem(thresholds.shape, f32), smem(flags.shape, jnp.int32),
            smem(cutoffs.shape, jnp.int32), smem(scalars.shape, f32),
            vmem(ksq.shape, f32), vmem(fwd.shape, bf16), vmem(inv.shape, bf16),
            vmem((2, 3, levels, nlon), f32), vmem((rows, levels, RADIX * HALF), f32),
            vmem((levels, nlon), f32), vmem((levels, nlon), f32), vmem((rows, 8, 2 * HALF), f32),
            vmem((tiles, 4 * levels, 2 * HALF), bf16), vmem((tiles, 2 * levels, 2 * HALF), f32),
            vmem((8, HALF), f32), vmem((NX * NC + NY, 8, HALF), f32), vmem((2, 8, HALF), f32),
            vmem((8, HALF), f32),
            vmem((levels // 8, 8, HALF), f32), vmem((levels // 8, 8, HALF), f32),
            dma((2 * PIECES + 5,)), dma((2,)), dma((2,)), dma, dma, dma, dma, dma, pltpu.SemaphoreType.REGULAR,
        ],
        compiler_params=pltpu.CompilerParams(collective_id=0, has_side_effects=True, vmem_limit_bytes=16 * 2**20),
        name="advect_filter",
    )(*operands)


def solution(mesh):
    finer = Mesh(
        mesh.devices.reshape(mesh.shape["member"], NX, NY, NC), ("member", "lat_0", "lat_1", "lat_2")
    )
    whole = P(("member", "lat_0", "lat_1", "lat_2"), None, None)
    placed = (whole, whole, whole, P("member"), P("member"), P(), P())
    return jax.shard_map(local, mesh=finer, in_specs=placed, out_specs=whole, check_vma=False)
```

```python
import functools
import math

import jax
import jax.numpy as jnp
import numpy as np
from jax import lax
from jax.experimental import pallas as pl
from jax.experimental.pallas import tpu as pltpu
from jax.sharding import Mesh
from jax.sharding import PartitionSpec as P

MESH = pl.DeviceIdType.MESH
NX, NY, NC = 8, 8, 2
PIECES = 2
RADIX = 12
HALF = 128
ROOT = math.sqrt(0.75)
LOG2E = math.log2(math.e)


def filter_tables(nlon):
    count = nlon // RADIX
    tiles = RADIX // 2
    fwd = np.zeros((tiles, 2 * HALF, 2 * HALF))
    inv = np.zeros((tiles, 2 * HALF, 2 * HALF))
    waves = np.zeros((8, 2 * HALF), np.int64)
    r = np.arange(count)

    def trig(k):
        angle = 2.0 * np.pi / nlon * ((r * k) % nlon)
        return np.cos(angle), np.sin(angle)

    def real_part(base, shift):
        lane = base
        for q in range(count // 2 + 1):
            k = RADIX * q + shift
            if k > nlon // 2:
                continue
            cos, sin = trig(k)
            weight = (1.0 if k in (0, nlon // 2) else 2.0) / nlon
            rows = slice(base, base + count)
            fwd[0, rows, lane] = cos
            inv[0, lane, rows] = cos * weight
            waves[0, lane] = k
            lane += 1
            if k not in (0, nlon // 2):
                fwd[0, rows, lane] = sin
                inv[0, lane, rows] = sin * weight
                waves[0, lane] = k
                lane += 1
        assert lane == base + count

    real_part(0, 0)
    real_part(HALF, RADIX // 2)
    for m in range(1, tiles):
        for q in range(count):
            k = RADIX * q + m
            cos, sin = trig(k)
            fwd[m, 0:count, q] = cos
            fwd[m, HALF : HALF + count, q] = -sin
            fwd[m, 0:count, HALF + q] = sin
            fwd[m, HALF : HALF + count, HALF + q] = cos
            waves[m, q] = waves[m, HALF + q] = min(k, nlon - k)
        inv[m] = fwd[m].T * (2.0 / nlon)
    inv_square = 1.0 / np.maximum(waves, 1).astype(np.float64) ** 2

    def halves(table):
        hi = table.astype(np.float32).astype(jnp.bfloat16)
        lo = (table - hi.astype(np.float64)).astype(np.float32).astype(jnp.bfloat16)
        return np.stack([hi, lo])

    return halves(fwd), halves(inv), inv_square.astype(np.float32)


def row_scalars(nlat):
    rows = np.arange(nlat)
    cos_row = np.sin(np.pi * (rows + 0.5) / nlat)
    faces = np.arange(nlat + 1)
    cos_face = np.where((faces > 0) & (faces < nlat), np.sin(np.pi * faces / nlat), 0.0)
    table = np.zeros((3 * nlat + HALF,))
    table[0:nlat] = cos_row
    table[nlat : 2 * nlat] = 1.0 / cos_row
    table[2 * nlat : 3 * nlat + 1] = cos_face / 24.0
    return table.astype(np.float32), float(np.sum(cos_row))


def twelve(e, o):
    plus, minus = e[0] + e[6], e[0] - e[6]
    e15p, e15m, e24p, e24m = e[1] + e[5], e[1] - e[5], e[2] + e[4], e[2] - e[4]
    a, b = plus + e24p, e15p + e[3]
    big, mid = ROOT * e15m, minus + 0.5 * e24m
    c, d = plus - 0.5 * e24p, 0.5 * e15p - e[3]
    even = [a + b, mid + big, c + d, minus - e24m, c - d, mid - big, a - b]
    o15p, o15m, o24p, o24m = o[0] + o[4], o[0] - o[4], o[1] + o[3], o[1] - o[3]
    f, g = 0.5 * o15p + o[2], ROOT * o24p
    s, t = ROOT * o15m, ROOT * o24m
    odd = [f + g, s + t, o15p - o[2], s - t, f - g]
    return even, odd


def product_of(exps):
    result = 1.0 + exps[0]
    for e in exps[1:]:
        result = result * (1.0 + e)
    return result


def split(x):
    hi = x.astype(jnp.bfloat16)
    return hi, (x - hi.astype(jnp.float32)).astype(jnp.bfloat16)


def kernel(
    dims, area,
    h_hbm, z_hbm, c_hbm, rates_hbm, thr_hbm, flags_hbm, cut_hbm, scal_hbm, ksq_hbm, fwd_hbm, inv_hbm,
    out,
    h, z, c, rates, thr, flags, cut, scal, ksq, fwd, inv,
    halo, base, s_lo, s_hi, factor, ymat, wmat, part, box, mean_in, own_mean, level_rates, level_thresholds,
    in_sem, halo_send, halo_recv, up_send, x_recv, y_recv, mean_send, mean_recv, low_in,
):
    rows, levels, nlon, nlat = dims
    count = nlon // RADIX
    x, y, core = lax.axis_index("lat_0"), lax.axis_index("lat_1"), lax.axis_index("lat_2")
    position = (x * NY + y) * NC + core
    total = NX * NY * NC

    order = (2, 3, 0, 1)
    cut_at = levels // PIECES
    pieces = [pl.ds(cut_at * i, cut_at) for i in range(PIECES)]

    def fetch(src, dst, i):
        return pltpu.make_async_copy(src, dst, in_sem.at[i])

    up_in = [[fetch(h_hbm.at[r, p], h.at[r, p], PIECES * (r - 2) + i) for i, p in enumerate(pieces)] for r in (2, 3)]
    low_rows = fetch(h_hbm.at[pl.ds(0, 2)], h.at[pl.ds(0, 2)], 2 * PIECES)
    c_up = fetch(c_hbm.at[rows - 1], c.at[rows - 1], 2 * PIECES + 1)
    small_in = [fetch(src, dst, 2 * PIECES + 2 + i) for i, (src, dst) in enumerate(((rates_hbm, rates), (thr_hbm, thr), (scal_hbm, scal)))]
    z_in = fetch(z_hbm, z, 0)
    c_in = fetch(c_hbm.at[pl.ds(0, rows - 1)], c.at[pl.ds(0, rows - 1)], 2 * PIECES)
    tables_in = [fetch(fwd_hbm, fwd, 1), fetch(inv_hbm, inv, 2)]
    factor_in = [
        fetch(src, dst, 2 * PIECES + 2 + i) for i, (src, dst) in enumerate(((flags_hbm, flags), (cut_hbm, cut), (ksq_hbm, ksq)))
    ]
    for copy in up_in[0] + up_in[1] + small_in + [low_rows, c_up]:
        copy.start()

    last = total - 1
    first = position * rows
    is_root = jnp.logical_and(x == 0, core == 1)
    is_first = position == 1
    is_later_root = jnp.logical_and(is_root, y > 0)

    def along(step):
        p = lax.rem(position + total + step, total)
        return {"lat_0": p // (NY * NC), "lat_1": lax.rem(p // NC, NY), "lat_2": lax.rem(p, NC)}

    def row(k):
        return {"lat_0": jnp.int32(k // NC), "lat_1": y, "lat_2": jnp.int32(k % NC)}

    def root(k):
        return {"lat_0": jnp.int32(0), "lat_1": jnp.int32(k), "lat_2": jnp.int32(1)}

    def signal(sem, device):
        pl.semaphore_signal(sem, inc=1, device_id=device, device_id_type=MESH)

    barrier = pltpu.get_barrier_semaphore()

    @pl.when(position > 0)
    def _():
        signal(barrier, along(-1))

    @pl.when(is_root)
    def _():
        for k in range(NX * NC):
            if k != 1:
                signal(barrier, row(k))

    @pl.when(is_first)
    def _():
        for k in range(1, NY):
            signal(barrier, root(k))

    to_start = jnp.logical_and(position > 1, jnp.logical_or(y == 0, is_root))

    @pl.when(to_start)
    def _():
        signal(barrier, {"lat_0": jnp.int32(0), "lat_1": jnp.int32(0), "lat_2": jnp.int32(0)})

    greeted = jnp.where(is_first, 0, 1) + jnp.where(position < last, 1, 0)
    greeted = greeted + jnp.where(position == 0, NX * NC - 2 + NY - 1, 0)
    pl.semaphore_wait(barrier, greeted)

    @pl.when(position < last)
    def _():
        signal(low_in, along(1))

    def landed(ref, sem):
        pltpu.make_async_copy(ref, ref, sem).wait()

    def halo_copy(side, field, levs=slice(None)):
        step, h_row, c_row = ((1, rows - 2, rows - 1), (-1, 0, 0))[side]
        src = c.at[c_row, levs] if field == 2 else h.at[h_row + field, levs]
        return pltpu.make_async_remote_copy(
            src, halo.at[side, field, levs], halo_send.at[side], halo_recv.at[side],
            device_id=along(step), device_id_type=MESH,
        )

    own_mean[...] = jnp.zeros_like(own_mean)

    @pl.when(jnp.logical_and(y > 0, jnp.logical_not(is_root)))
    def _():
        mean_in[1] = jnp.zeros_like(mean_in[1])

    base[:, :, nlon:] = jnp.zeros((rows, levels, base.shape[2] - nlon), jnp.float32)

    @pl.when(position == 0)
    def _():
        halo[0] = jnp.zeros_like(halo[0])

    @pl.when(position == last)
    def _():
        halo[1] = jnp.zeros_like(halo[1])

    for field in (0, 1):
        for arrived, levs in zip(up_in[field], pieces):
            arrived.wait()

            @pl.when(core == 0)
            def _():
                halo_copy(0, field, levs).start()

    for copy in small_in:
        copy.wait()

    lane = lax.broadcasted_iota(jnp.int32, (8, HALF), 1)
    tile = jnp.zeros((8, HALF), jnp.float32)
    sub = lax.broadcasted_iota(jnp.int32, (8, 1), 0)

    def levels_of(ref, start):
        value = jnp.zeros((8, 1), jnp.float32)
        for k in range(8):
            value = jnp.where(sub == k, ref[start + k], value)
        return value

    full = nlon // HALF
    groups = range(levels // 8)
    rate_of = [levels_of(rates, 8 * g) for g in groups]
    threshold_of = [levels_of(thr, 8 * g) for g in groups]
    scaled_threshold = [LOG2E * value for value in threshold_of]
    wide, rest = [0.0 for g in groups], [0.0 for g in groups]
    for r in order:
        if r == 0:
            low_rows.wait()
        for g in groups:
            lev = pl.ds(8 * g, 8)
            exps = [
                jnp.exp2(h[r, lev, HALF * j : HALF * (j + 1)] * LOG2E - scaled_threshold[g]) for j in range(full)
            ]
            logs = jnp.log2(product_of(exps[0:6])) + jnp.log2(product_of(exps[6:full]))
            wide[g] = wide[g] + scal[first + r] * logs
            logs = jnp.log2(1.0 + jnp.exp2(h[r, lev, HALF * full : nlon] * LOG2E - scaled_threshold[g]))
            rest[g] = rest[g] + scal[first + r] * logs
    short = jnp.zeros((8, HALF * (full + 1) - nlon), jnp.float32)
    for g in groups:
        sums = jnp.sum(wide[g] + jnp.concatenate([rest[g], short], axis=1), axis=1, keepdims=True)
        tile = jnp.where(lane == g, (-1.0 / LOG2E) * rate_of[g] * sums, tile)
        level_rates[g] = jnp.broadcast_to(rate_of[g], (8, HALF))
        level_thresholds[g] = jnp.broadcast_to(threshold_of[g], (8, HALF))
    part[...] = tile

    members = [*range(NC, NX * NC), 0]

    def mean_copy(slot, source, device):
        return pltpu.make_async_remote_copy(
            source, mean_in.at[slot], mean_send, mean_recv, device_id=device, device_id_type=MESH
        )

    def send_b(device):
        mean_copy(1, part, device).start()

    def part_copy(slot):
        return pltpu.make_async_remote_copy(
            part, box.at[slot], up_send, x_recv, device_id=row(1), device_id_type=MESH
        )

    sends_part = jnp.logical_and(jnp.logical_not(is_root), position > 0)

    @pl.when(sends_part)
    def _():
        part_copy(x * NC + core).start()

    @pl.when(position == 0)
    def _():
        send_b(row(1))

    c_up.wait()

    @pl.when(jnp.logical_and(core != 0, position < last))
    def _():
        halo_copy(0, 0).start()
        halo_copy(0, 1).start()

    @pl.when(position < last)
    def _():
        halo_copy(0, 2).start()

    @pl.when(position == 0)
    def _():
        mean_in[1] = part[...]
        for k in range(1, NY):
            for member in members[2 * k - 2 : 2 * k]:
                send_b(row(member))
            send_b(root(k))

    for copy in [c_in, z_in] + factor_in + tables_in:
        copy.start()

    z_in.wait()
    c_in.wait()


    def inv_cos(r):
        return scal[nlat + first + r]

    def face(f):
        return scal[2 * nlat + first + f]

    def west(a):
        return pltpu.roll(a, 1, axis=1)

    def east(a):
        return pltpu.roll(a, nlon - 1, axis=1)

    def local_terms(g, carry):
        lev = pl.ds(pl.multiple_of(8 * g, 8), 8)
        hr = [h[r, lev, :] for r in range(rows)]
        rate, threshold = level_rates[g][:, 0:1], level_thresholds[g][:, 0:1]
        cr = [c[r, lev, :] for r in range(rows)]
        low = face(1) * (cr[0] + cr[1])
        high = face(3) * (cr[2] + cr[3])
        s_lo[lev, :] = low
        s_hi[lev, :] = high
        f1 = low * (7.0 * (hr[0] + hr[1]) - hr[2])
        f2 = face(2) * (cr[1] + cr[2]) * (7.0 * (hr[1] + hr[2]) - (hr[0] + hr[3]))
        f3 = high * (7.0 * (hr[2] + hr[3]) - hr[1])
        terms = [f1, f2 - f1, f3 - f2, -f3]
        for r in range(rows):
            pair = hr[r] + east(hr[r])
            zr = z[r, lev, :]
            speed = zr + east(zr)
            flux = speed * (8.0 * pair - (west(pair) + east(pair))) * (1.0 / 24.0)
            s = hr[r] - threshold
            source = rate * jnp.log(1.0 + jnp.exp(s))
            base[r, lev, 0:nlon] = (hr[r] - source) - (flux - west(flux)) - terms[r] * inv_cos(r)
        return carry

    lax.fori_loop(0, levels // 8, local_terms, 0)

    @pl.when(position > 0)
    def _():
        pl.semaphore_wait(low_in, 1)
        for field in range(3):
            halo_copy(1, field).start()

    for copy in factor_in:
        copy.wait()
    for r in range(rows):
        cutoff = cut[first + r].astype(jnp.float32)
        flag = flags[first + r].astype(jnp.float32)
        factor[r] = flag * (1.0 - jnp.minimum(1.0, cutoff * cutoff * ksq[...]))

    def sum_copy():
        return pltpu.make_async_remote_copy(
            part, box.at[NX * NC + y], up_send, y_recv, device_id=root(0), device_id_type=MESH
        )

    def gather_row(senders):
        landed(box.at[pl.ds(0, len(senders))], x_recv)
        acc = part[...]
        for k in senders:
            acc = acc + box[k]
        return acc

    @pl.when(is_later_root)
    def _():
        part[...] = gather_row(members)
        sum_copy().start()

    for copy in tables_in:
        copy.wait()
    lanes = lax.broadcasted_iota(jnp.int32, (16, HALF), 1)
    units = 2 * levels
    blocks = levels // 16

    tail = nlon - HALF * (RADIX - 1)

    def piece(ref, j):
        if j < RADIX - 1:
            return ref[:, HALF * j : HALF * (j + 1)]
        return jnp.concatenate([ref[:, HALF * j : nlon], jnp.zeros((16, HALF - tail), jnp.float32)], axis=1)

    def with_halo(r, lev, j):
        side, near, far, edge, inner, f, through, outer = (
            (0, 1, 0, 0, 1, 0, s_lo, 0) if r < 2 else (1, 0, 1, rows - 1, rows - 2, rows, s_hi, rows - 1)
        )
        beside = piece(halo.at[side, near, lev], j)
        term = piece(through.at[lev], j) * beside
        if r == outer:
            speed = face(f) * (piece(halo.at[side, 2, lev], j) + piece(c.at[edge, lev], j))
            flux = speed * (
                7.0 * (beside + piece(h.at[edge, lev], j)) - (piece(halo.at[side, far, lev], j) + piece(h.at[inner, lev], j))
            )
            term = term + flux
        sign = 1.0 if r in (0, 2) else -1.0
        return base[r, lev, HALF * j : HALF * (j + 1)] + term * (sign * inv_cos(r))

    def product(hilo, table):
        first_part = jnp.dot(hilo, table[0], preferred_element_type=jnp.float32)
        second = jnp.dot(hilo[0:units], table[1], preferred_element_type=jnp.float32)
        return first_part[0:units] + first_part[units : 2 * units] + second

    def filter_rows(row0, shifts=None):
        def block_of(b):
            return row0 + b // blocks, pl.ds(16 * (b % blocks), 16), pl.ds(16 * b, 16), pl.ds(units + 16 * b, 16)

        def forward(b):
            r, lev, at_hi, at_lo = block_of(b)
            v = [with_halo(r, lev, j) for j in range(RADIX)]
            for j in range(RADIX):
                base[r, lev, HALF * j : HALF * (j + 1)] = v[j]
            u = [v[0]] + [
                pltpu.roll(jnp.where(lanes >= HALF - 8 * j, v[j - 1], v[j]), 8 * j, axis=1) for j in range(1, RADIX)
            ]
            e = [u[0]] + [u[j] + u[RADIX - j] for j in range(1, 6)] + [u[6]]
            o = [u[j] - u[RADIX - j] for j in range(1, 6)]
            even, odd = twelve(e, o)
            halves = [(even[0], even[6])] + [(even[m], odd[m - 1]) for m in range(1, 6)]
            for m, pair in enumerate(halves):
                for k, value in enumerate(pair):
                    hi, lo = split(value)
                    ymat[m, at_hi, HALF * k : HALF * (k + 1)] = hi
                    ymat[m, at_lo, HALF * k : HALF * (k + 1)] = lo

        def backward(b):
            r, lev, at, _ = block_of(b)
            w = [[wmat[m, at, HALF * k : HALF * (k + 1)] for k in range(2)] for m in range(RADIX // 2)]
            even, odd = twelve([w[0][0]] + [w[m][0] for m in range(1, 6)] + [w[0][1]], [w[m][1] for m in range(1, 6)])
            removed = [even[0]] + [even[j] + odd[j - 1] for j in range(1, 6)] + [even[6]]
            removed += [even[RADIX - j] - odd[RADIX - j - 1] for j in range(7, RADIX)]
            back = [removed[0]] + [pltpu.roll(removed[j], HALF - 8 * j, axis=1) for j in range(1, RADIX)]
            for j in range(RADIX):
                kept = base[r, lev, HALF * j : HALF * (j + 1)]
                if row0 == 0:
                    kept = kept - shifts[b % blocks]
                if j < RADIX - 1:
                    out[r, lev, HALF * j : HALF * (j + 1)] = kept - jnp.where(lanes < count - 8 * j, back[j], back[j + 1])
                else:
                    out[r, lev, HALF * j : nlon] = (kept - back[j])[:, 0:tail]

        for b in range(2 * blocks):
            forward(b)
        for m in range(RADIX // 2):
            waves = product(ymat[m], (fwd[0, m], fwd[1, m]))
            scaled = jnp.concatenate(
                [waves[r * levels : (r + 1) * levels] * factor[row0 + r, m : m + 1, :] for r in range(2)], axis=0
            )
            wmat[m] = product(jnp.concatenate(split(scaled), axis=0), (inv[0, m], inv[1, m]))
        if row0 == 0:
            for r in (2, 3):
                for b in range(blocks):
                    lev = pl.ds(16 * b, 16)
                    out[r, lev, :] = out[r, lev, :] - shifts[b]
        for b in range(2 * blocks):
            backward(b)

    @pl.when(position < last)
    def _():
        landed(halo.at[1], halo_recv.at[1])

    filter_rows(2)

    @pl.when(is_first)
    def _():
        landed(box.at[pl.ds(NX * NC + 1, NY - 1)], y_recv)
        acc = box[NX * NC + 1]
        for k in range(2, NY):
            acc = acc + box[NX * NC + k]
        mean_in[0] = gather_row(members[:-1]) + acc
        for k in range(1, NY):
            for member in members[2 * k - 2 : 2 * k]:
                mean_copy(0, mean_in.at[0], row(member)).start()
            mean_copy(0, mean_in.at[0], root(k)).start()
        mean_copy(0, mean_in.at[0], row(0)).start()

    @pl.when(position > 0)
    def _():
        landed(halo.at[0], halo_recv.at[0])

    @pl.when(is_first)
    def _():
        landed(mean_in.at[1], mean_recv)
        own_mean[...] = (mean_in[0] + mean_in[1]) * (1.0 / area)

    def mean_columns(value):
        return [jnp.sum(jnp.where(lane == g, value, 0.0), axis=1, keepdims=True) for g in groups]

    columns = mean_columns(own_mean[...])
    shifts = [jnp.concatenate(columns[2 * b : 2 * b + 2], axis=0) for b in range(blocks)]
    filter_rows(0, shifts)

    in_two = jnp.logical_or(is_later_root, jnp.logical_and(y == 0, position > 1))

    @pl.when(in_two)
    def _():
        landed(mean_in, mean_recv)

    @pl.when(jnp.logical_not(jnp.logical_or(in_two, is_first)))
    def _():
        landed(mean_in.at[0], mean_recv)

    @pl.when(is_later_root)
    def _():
        own_mean[...] = mean_in[0] + mean_in[1]
        for member in members:
            mean_copy(0, own_mean, row(member)).start()

    @pl.when(jnp.logical_not(is_first))
    def _():
        for g, shift in zip(groups, mean_columns((mean_in[0] + mean_in[1]) * (1.0 / area))):
            lev = pl.ds(8 * g, 8)
            for r in range(rows):
                out[r, lev, :] = out[r, lev, :] - shift

    for side, sender in ((0, position < last), (1, position > 0)):

        @pl.when(sender)
        def _():
            landed(halo.at[side], halo_send.at[side])

    @pl.when(position <= 1)
    def _():
        landed(box.at[pl.ds(0, len(members) + NY - 1)], mean_send)

    @pl.when(is_later_root)
    def _():
        landed(box.at[pl.ds(0, len(members))], mean_send)

    @pl.when(position > 1)
    def _():
        landed(part, up_send)


def local(height, zonal, merid, rates, thresholds, flags, cutoffs):
    rows, levels, nlon = height.shape
    nlat = rows * NX * NY * NC
    fwd, inv, ksq = filter_tables(nlon)
    scalars, cos_sum = row_scalars(nlat)
    tiles = RADIX // 2
    dims = (rows, levels, nlon, nlat)
    f32, bf16 = jnp.float32, jnp.bfloat16
    vmem, smem, dma = pltpu.VMEM, pltpu.SMEM, pltpu.SemaphoreType.DMA
    operands = (height, zonal, merid, rates, thresholds, flags, cutoffs, scalars, ksq, fwd, inv)
    operands = [pltpu.with_memory_space_constraint(jnp.asarray(a), pltpu.HBM) for a in operands]
    return pl.pallas_call(
        functools.partial(kernel, dims, nlon * cos_sum),
        out_shape=vmem(height.shape, f32),
        in_specs=[pl.BlockSpec(memory_space=pltpu.HBM)] * len(operands),
        out_specs=pl.BlockSpec(memory_space=vmem),
        scratch_shapes=[
            vmem(height.shape, f32), vmem(height.shape, f32), vmem(height.shape, f32),
            smem(rates.shape, f32), smem(thresholds.shape, f32), smem(flags.shape, jnp.int32),
            smem(cutoffs.shape, jnp.int32), smem(scalars.shape, f32),
            vmem(ksq.shape, f32), vmem(fwd.shape, bf16), vmem(inv.shape, bf16),
            vmem((2, 3, levels, nlon), f32), vmem((rows, levels, RADIX * HALF), f32),
            vmem((levels, nlon), f32), vmem((levels, nlon), f32), vmem((rows, 8, 2 * HALF), f32),
            vmem((tiles, 4 * levels, 2 * HALF), bf16), vmem((tiles, 2 * levels, 2 * HALF), f32),
            vmem((8, HALF), f32), vmem((NX * NC + NY, 8, HALF), f32), vmem((2, 8, HALF), f32),
            vmem((8, HALF), f32),
            vmem((levels // 8, 8, HALF), f32), vmem((levels // 8, 8, HALF), f32),
            dma((2 * PIECES + 5,)), dma((2,)), dma((2,)), dma, dma, dma, dma, dma, pltpu.SemaphoreType.REGULAR,
        ],
        compiler_params=pltpu.CompilerParams(collective_id=0, has_side_effects=True, vmem_limit_bytes=16 * 2**20),
        name="advect_filter",
    )(*operands)


def solution(mesh):
    finer = Mesh(
        mesh.devices.reshape(mesh.shape["member"], NX, NY, NC), ("member", "lat_0", "lat_1", "lat_2")
    )
    whole = P(("member", "lat_0", "lat_1", "lat_2"), None, None)
    placed = (whole, whole, whole, P("member"), P("member"), P(), P())
    return jax.shard_map(local, mesh=finer, in_specs=placed, out_specs=whole, check_vma=False)
```

```python
import functools
import math

import jax
import jax.numpy as jnp
import numpy as np
from jax import lax
from jax.experimental import pallas as pl
from jax.experimental.pallas import tpu as pltpu
from jax.sharding import Mesh
from jax.sharding import PartitionSpec as P

MESH = pl.DeviceIdType.MESH
NX, NY, NC = 8, 8, 2
PIECES = 4
RADIX = 12
HALF = 128
ROOT = math.sqrt(0.75)
LOG2E = math.log2(math.e)


def filter_tables(nlon):
    count = nlon // RADIX
    tiles = RADIX // 2
    fwd = np.zeros((tiles, 2 * HALF, 2 * HALF))
    inv = np.zeros((tiles, 2 * HALF, 2 * HALF))
    waves = np.zeros((8, 2 * HALF), np.int64)
    r = np.arange(count)

    def trig(k):
        angle = 2.0 * np.pi / nlon * ((r * k) % nlon)
        return np.cos(angle), np.sin(angle)

    def real_part(base, shift):
        lane = base
        for q in range(count // 2 + 1):
            k = RADIX * q + shift
            if k > nlon // 2:
                continue
            cos, sin = trig(k)
            weight = (1.0 if k in (0, nlon // 2) else 2.0) / nlon
            rows = slice(base, base + count)
            fwd[0, rows, lane] = cos
            inv[0, lane, rows] = cos * weight
            waves[0, lane] = k
            lane += 1
            if k not in (0, nlon // 2):
                fwd[0, rows, lane] = sin
                inv[0, lane, rows] = sin * weight
                waves[0, lane] = k
                lane += 1
        assert lane == base + count

    real_part(0, 0)
    real_part(HALF, RADIX // 2)
    for m in range(1, tiles):
        for q in range(count):
            k = RADIX * q + m
            cos, sin = trig(k)
            fwd[m, 0:count, q] = cos
            fwd[m, HALF : HALF + count, q] = -sin
            fwd[m, 0:count, HALF + q] = sin
            fwd[m, HALF : HALF + count, HALF + q] = cos
            waves[m, q] = waves[m, HALF + q] = min(k, nlon - k)
        inv[m] = fwd[m].T * (2.0 / nlon)
    inv_square = 1.0 / np.maximum(waves, 1).astype(np.float64) ** 2

    def halves(table):
        hi = table.astype(np.float32).astype(jnp.bfloat16)
        lo = (table - hi.astype(np.float64)).astype(np.float32).astype(jnp.bfloat16)
        return np.stack([hi, lo])

    return halves(fwd), halves(inv), inv_square.astype(np.float32)


def row_scalars(nlat):
    rows = np.arange(nlat)
    cos_row = np.sin(np.pi * (rows + 0.5) / nlat)
    faces = np.arange(nlat + 1)
    cos_face = np.where((faces > 0) & (faces < nlat), np.sin(np.pi * faces / nlat), 0.0)
    table = np.zeros((3 * nlat + HALF,))
    table[0:nlat] = cos_row
    table[nlat : 2 * nlat] = 1.0 / cos_row
    table[2 * nlat : 3 * nlat + 1] = cos_face / 24.0
    return table.astype(np.float32), float(np.sum(cos_row))


def twelve(e, o):
    plus, minus = e[0] + e[6], e[0] - e[6]
    e15p, e15m, e24p, e24m = e[1] + e[5], e[1] - e[5], e[2] + e[4], e[2] - e[4]
    a, b = plus + e24p, e15p + e[3]
    big, mid = ROOT * e15m, minus + 0.5 * e24m
    c, d = plus - 0.5 * e24p, 0.5 * e15p - e[3]
    even = [a + b, mid + big, c + d, minus - e24m, c - d, mid - big, a - b]
    o15p, o15m, o24p, o24m = o[0] + o[4], o[0] - o[4], o[1] + o[3], o[1] - o[3]
    f, g = 0.5 * o15p + o[2], ROOT * o24p
    s, t = ROOT * o15m, ROOT * o24m
    odd = [f + g, s + t, o15p - o[2], s - t, f - g]
    return even, odd


def product_of(exps):
    result = 1.0 + exps[0]
    for e in exps[1:]:
        result = result * (1.0 + e)
    return result


def split(x):
    hi = x.astype(jnp.bfloat16)
    return hi, (x - hi.astype(jnp.float32)).astype(jnp.bfloat16)


def kernel(
    dims, area,
    h_hbm, z_hbm, c_hbm, rates_hbm, thr_hbm, flags_hbm, cut_hbm, scal_hbm, ksq_hbm, fwd_hbm, inv_hbm,
    out,
    h, z, c, rates, thr, flags, cut, scal, ksq, fwd, inv,
    halo, base, s_lo, s_hi, factor, ymat, wmat, part, box, mean_in, own_mean, level_rates, level_thresholds,
    in_sem, halo_send, halo_recv, up_send, x_recv, y_recv, mean_send, mean_recv, low_in,
):
    rows, levels, nlon, nlat = dims
    count = nlon // RADIX
    x, y, core = lax.axis_index("lat_0"), lax.axis_index("lat_1"), lax.axis_index("lat_2")
    position = (x * NY + y) * NC + core
    total = NX * NY * NC

    order = (2, 3, 0, 1)
    cut_at = levels // PIECES
    pieces = [pl.ds(cut_at * i, cut_at) for i in range(PIECES)]

    def fetch(src, dst, i):
        return pltpu.make_async_copy(src, dst, in_sem.at[i])

    up_in = [[fetch(h_hbm.at[r, p], h.at[r, p], PIECES * (r - 2) + i) for i, p in enumerate(pieces)] for r in (2, 3)]
    low_rows = fetch(h_hbm.at[pl.ds(0, 2)], h.at[pl.ds(0, 2)], 2 * PIECES)
    c_up = fetch(c_hbm.at[rows - 1], c.at[rows - 1], 2 * PIECES + 1)
    small_in = [fetch(src, dst, 2 * PIECES + 2 + i) for i, (src, dst) in enumerate(((rates_hbm, rates), (thr_hbm, thr), (scal_hbm, scal)))]
    z_in = fetch(z_hbm, z, 0)
    c_in = fetch(c_hbm.at[pl.ds(0, rows - 1)], c.at[pl.ds(0, rows - 1)], 2 * PIECES)
    tables_in = [fetch(fwd_hbm, fwd, 1), fetch(inv_hbm, inv, 2)]
    factor_in = [
        fetch(src, dst, 2 * PIECES + 2 + i) for i, (src, dst) in enumerate(((flags_hbm, flags), (cut_hbm, cut), (ksq_hbm, ksq)))
    ]
    for copy in small_in + up_in[0] + up_in[1] + [low_rows, c_up]:
        copy.start()

    last = total - 1
    first = position * rows
    is_root = jnp.logical_and(x == 0, core == 1)
    is_first = position == 1
    is_later_root = jnp.logical_and(is_root, y > 0)

    def along(step):
        p = lax.rem(position + total + step, total)
        return {"lat_0": p // (NY * NC), "lat_1": lax.rem(p // NC, NY), "lat_2": lax.rem(p, NC)}

    def row(k):
        return {"lat_0": jnp.int32(k // NC), "lat_1": y, "lat_2": jnp.int32(k % NC)}

    def root(k):
        return {"lat_0": jnp.int32(0), "lat_1": jnp.int32(k), "lat_2": jnp.int32(1)}

    def signal(sem, device):
        pl.semaphore_signal(sem, inc=1, device_id=device, device_id_type=MESH)

    barrier = pltpu.get_barrier_semaphore()

    @pl.when(position > 0)
    def _():
        signal(barrier, along(-1))

    @pl.when(is_root)
    def _():
        for k in range(NX * NC):
            if k != 1:
                signal(barrier, row(k))

    @pl.when(is_first)
    def _():
        for k in range(1, NY):
            signal(barrier, root(k))

    to_start = jnp.logical_and(position > 1, jnp.logical_or(y == 0, is_root))

    @pl.when(to_start)
    def _():
        signal(barrier, {"lat_0": jnp.int32(0), "lat_1": jnp.int32(0), "lat_2": jnp.int32(0)})

    greeted = jnp.where(is_first, 0, 1) + jnp.where(position < last, 1, 0)
    greeted = greeted + jnp.where(position == 0, NX * NC - 2 + NY - 1, 0)
    pl.semaphore_wait(barrier, greeted)

    @pl.when(position < last)
    def _():
        signal(low_in, along(1))

    def landed(ref, sem):
        pltpu.make_async_copy(ref, ref, sem).wait()

    def halo_copy(side, field, levs=slice(None)):
        step, h_row, c_row = ((1, rows - 2, rows - 1), (-1, 0, 0))[side]
        src = c.at[c_row, levs] if field == 2 else h.at[h_row + field, levs]
        return pltpu.make_async_remote_copy(
            src, halo.at[side, field, levs], halo_send.at[side], halo_recv.at[side],
            device_id=along(step), device_id_type=MESH,
        )

    own_mean[...] = jnp.zeros_like(own_mean)

    @pl.when(jnp.logical_and(y > 0, jnp.logical_not(is_root)))
    def _():
        mean_in[1] = jnp.zeros_like(mean_in[1])

    base[:, :, nlon:] = jnp.zeros((rows, levels, base.shape[2] - nlon), jnp.float32)

    @pl.when(position == 0)
    def _():
        halo[0] = jnp.zeros_like(halo[0])

    @pl.when(position == last)
    def _():
        halo[1] = jnp.zeros_like(halo[1])

    for field in (0, 1):
        for arrived, levs in zip(up_in[field], pieces):
            arrived.wait()

            @pl.when(core == 0)
            def _():
                halo_copy(0, field, levs).start()

    for copy in small_in:
        copy.wait()

    lane = lax.broadcasted_iota(jnp.int32, (8, HALF), 1)
    tile = jnp.zeros((8, HALF), jnp.float32)
    sub = lax.broadcasted_iota(jnp.int32, (8, 1), 0)

    def levels_of(ref, start):
        value = jnp.zeros((8, 1), jnp.float32)
        for k in range(8):
            value = jnp.where(sub == k, ref[start + k], value)
        return value

    full = nlon // HALF
    groups = range(levels // 8)
    rate_of = [levels_of(rates, 8 * g) for g in groups]
    threshold_of = [levels_of(thr, 8 * g) for g in groups]
    scaled_threshold = [LOG2E * value for value in threshold_of]
    wide, rest = [0.0 for g in groups], [0.0 for g in groups]
    for r in order:
        if r == 0:
            low_rows.wait()
        for g in groups:
            lev = pl.ds(8 * g, 8)
            exps = [
                jnp.exp2(h[r, lev, HALF * j : HALF * (j + 1)] * LOG2E - scaled_threshold[g]) for j in range(full)
            ]
            logs = jnp.log2(product_of(exps[0:6])) + jnp.log2(product_of(exps[6:full]))
            wide[g] = wide[g] + scal[first + r] * logs
            logs = jnp.log2(1.0 + jnp.exp2(h[r, lev, HALF * full : nlon] * LOG2E - scaled_threshold[g]))
            rest[g] = rest[g] + scal[first + r] * logs
    short = jnp.zeros((8, HALF * (full + 1) - nlon), jnp.float32)
    for g in groups:
        sums = jnp.sum(wide[g] + jnp.concatenate([rest[g], short], axis=1), axis=1, keepdims=True)
        tile = jnp.where(lane == g, (-1.0 / LOG2E) * rate_of[g] * sums, tile)
        level_rates[g] = jnp.broadcast_to(rate_of[g], (8, HALF))
        level_thresholds[g] = jnp.broadcast_to(threshold_of[g], (8, HALF))
    part[...] = tile

    members = [*range(NC, NX * NC), 0]

    def mean_copy(slot, source, device):
        return pltpu.make_async_remote_copy(
            source, mean_in.at[slot], mean_send, mean_recv, device_id=device, device_id_type=MESH
        )

    def send_b(device):
        mean_copy(1, part, device).start()

    def part_copy(slot):
        return pltpu.make_async_remote_copy(
            part, box.at[slot], up_send, x_recv, device_id=row(1), device_id_type=MESH
        )

    sends_part = jnp.logical_and(jnp.logical_not(is_root), position > 0)

    @pl.when(sends_part)
    def _():
        part_copy(x * NC + core).start()

    @pl.when(position == 0)
    def _():
        send_b(row(1))

    c_up.wait()

    @pl.when(jnp.logical_and(core != 0, position < last))
    def _():
        halo_copy(0, 0).start()
        halo_copy(0, 1).start()

    @pl.when(position < last)
    def _():
        halo_copy(0, 2).start()

    @pl.when(position == 0)
    def _():
        mean_in[1] = part[...]
        for k in range(1, NY):
            for member in members[2 * k - 2 : 2 * k]:
                send_b(row(member))
            send_b(root(k))

    for copy in [c_in, z_in] + factor_in + tables_in:
        copy.start()

    z_in.wait()
    c_in.wait()


    def inv_cos(r):
        return scal[nlat + first + r]

    def face(f):
        return scal[2 * nlat + first + f]

    def west(a):
        return pltpu.roll(a, 1, axis=1)

    def east(a):
        return pltpu.roll(a, nlon - 1, axis=1)

    def local_terms(g, carry):
        lev = pl.ds(pl.multiple_of(8 * g, 8), 8)
        hr = [h[r, lev, :] for r in range(rows)]
        rate, threshold = level_rates[g][:, 0:1], level_thresholds[g][:, 0:1]
        cr = [c[r, lev, :] for r in range(rows)]
        low = face(1) * (cr[0] + cr[1])
        high = face(3) * (cr[2] + cr[3])
        s_lo[lev, :] = low
        s_hi[lev, :] = high
        f1 = low * (7.0 * (hr[0] + hr[1]) - hr[2])
        f2 = face(2) * (cr[1] + cr[2]) * (7.0 * (hr[1] + hr[2]) - (hr[0] + hr[3]))
        f3 = high * (7.0 * (hr[2] + hr[3]) - hr[1])
        terms = [f1, f2 - f1, f3 - f2, -f3]
        for r in range(rows):
            pair = hr[r] + east(hr[r])
            zr = z[r, lev, :]
            speed = zr + east(zr)
            flux = speed * (8.0 * pair - (west(pair) + east(pair))) * (1.0 / 24.0)
            s = hr[r] - threshold
            source = rate * jnp.log(1.0 + jnp.exp(s))
            base[r, lev, 0:nlon] = (hr[r] - source) - (flux - west(flux)) - terms[r] * inv_cos(r)
        return carry

    lax.fori_loop(0, levels // 8, local_terms, 0)

    @pl.when(position > 0)
    def _():
        pl.semaphore_wait(low_in, 1)
        for field in range(3):
            halo_copy(1, field).start()

    for copy in factor_in:
        copy.wait()
    for r in range(rows):
        cutoff = cut[first + r].astype(jnp.float32)
        flag = flags[first + r].astype(jnp.float32)
        factor[r] = flag * (1.0 - jnp.minimum(1.0, cutoff * cutoff * ksq[...]))

    def sum_copy():
        return pltpu.make_async_remote_copy(
            part, box.at[NX * NC + y], up_send, y_recv, device_id=root(0), device_id_type=MESH
        )

    def gather_row(senders):
        landed(box.at[pl.ds(0, len(senders))], x_recv)
        acc = part[...]
        for k in senders:
            acc = acc + box[k]
        return acc

    @pl.when(is_later_root)
    def _():
        part[...] = gather_row(members)
        sum_copy().start()

    for copy in tables_in:
        copy.wait()
    lanes = lax.broadcasted_iota(jnp.int32, (16, HALF), 1)
    units = 2 * levels
    blocks = levels // 16

    tail = nlon - HALF * (RADIX - 1)

    def piece(ref, j):
        if j < RADIX - 1:
            return ref[:, HALF * j : HALF * (j + 1)]
        return jnp.concatenate([ref[:, HALF * j : nlon], jnp.zeros((16, HALF - tail), jnp.float32)], axis=1)

    def with_halo(r, lev, j):
        side, near, far, edge, inner, f, through, outer = (
            (0, 1, 0, 0, 1, 0, s_lo, 0) if r < 2 else (1, 0, 1, rows - 1, rows - 2, rows, s_hi, rows - 1)
        )
        beside = piece(halo.at[side, near, lev], j)
        term = piece(through.at[lev], j) * beside
        if r == outer:
            speed = face(f) * (piece(halo.at[side, 2, lev], j) + piece(c.at[edge, lev], j))
            flux = speed * (
                7.0 * (beside + piece(h.at[edge, lev], j)) - (piece(halo.at[side, far, lev], j) + piece(h.at[inner, lev], j))
            )
            term = term + flux
        sign = 1.0 if r in (0, 2) else -1.0
        return base[r, lev, HALF * j : HALF * (j + 1)] + term * (sign * inv_cos(r))

    def product(hilo, table):
        first_part = jnp.dot(hilo, table[0], preferred_element_type=jnp.float32)
        second = jnp.dot(hilo[0:units], table[1], preferred_element_type=jnp.float32)
        return first_part[0:units] + first_part[units : 2 * units] + second

    def filter_rows(row0, shifts=None):
        def block_of(b):
            return row0 + b // blocks, pl.ds(16 * (b % blocks), 16), pl.ds(16 * b, 16), pl.ds(units + 16 * b, 16)

        def forward(b):
            r, lev, at_hi, at_lo = block_of(b)
            v = [with_halo(r, lev, j) for j in range(RADIX)]
            for j in range(RADIX):
                base[r, lev, HALF * j : HALF * (j + 1)] = v[j]
            u = [v[0]] + [
                pltpu.roll(jnp.where(lanes >= HALF - 8 * j, v[j - 1], v[j]), 8 * j, axis=1) for j in range(1, RADIX)
            ]
            e = [u[0]] + [u[j] + u[RADIX - j] for j in range(1, 6)] + [u[6]]
            o = [u[j] - u[RADIX - j] for j in range(1, 6)]
            even, odd = twelve(e, o)
            halves = [(even[0], even[6])] + [(even[m], odd[m - 1]) for m in range(1, 6)]
            for m, pair in enumerate(halves):
                for k, value in enumerate(pair):
                    hi, lo = split(value)
                    ymat[m, at_hi, HALF * k : HALF * (k + 1)] = hi
                    ymat[m, at_lo, HALF * k : HALF * (k + 1)] = lo

        def backward(b):
            r, lev, at, _ = block_of(b)
            w = [[wmat[m, at, HALF * k : HALF * (k + 1)] for k in range(2)] for m in range(RADIX // 2)]
            even, odd = twelve([w[0][0]] + [w[m][0] for m in range(1, 6)] + [w[0][1]], [w[m][1] for m in range(1, 6)])
            removed = [even[0]] + [even[j] + odd[j - 1] for j in range(1, 6)] + [even[6]]
            removed += [even[RADIX - j] - odd[RADIX - j - 1] for j in range(7, RADIX)]
            back = [removed[0]] + [pltpu.roll(removed[j], HALF - 8 * j, axis=1) for j in range(1, RADIX)]
            for j in range(RADIX):
                kept = base[r, lev, HALF * j : HALF * (j + 1)]
                if row0 == 0:
                    kept = kept - shifts[b % blocks]
                if j < RADIX - 1:
                    out[r, lev, HALF * j : HALF * (j + 1)] = kept - jnp.where(lanes < count - 8 * j, back[j], back[j + 1])
                else:
                    out[r, lev, HALF * j : nlon] = (kept - back[j])[:, 0:tail]

        for b in range(2 * blocks):
            forward(b)
        for m in range(RADIX // 2):
            waves = product(ymat[m], (fwd[0, m], fwd[1, m]))
            scaled = jnp.concatenate(
                [waves[r * levels : (r + 1) * levels] * factor[row0 + r, m : m + 1, :] for r in range(2)], axis=0
            )
            wmat[m] = product(jnp.concatenate(split(scaled), axis=0), (inv[0, m], inv[1, m]))
        if row0 == 0:
            for r in (2, 3):
                for b in range(blocks):
                    lev = pl.ds(16 * b, 16)
                    out[r, lev, :] = out[r, lev, :] - shifts[b]
        for b in range(2 * blocks):
            backward(b)

    @pl.when(position < last)
    def _():
        landed(halo.at[1], halo_recv.at[1])

    filter_rows(2)

    @pl.when(is_first)
    def _():
        landed(box.at[pl.ds(NX * NC + 1, NY - 1)], y_recv)
        acc = box[NX * NC + 1]
        for k in range(2, NY):
            acc = acc + box[NX * NC + k]
        mean_in[0] = gather_row(members[:-1]) + acc
        for k in range(1, NY):
            for member in members[2 * k - 2 : 2 * k]:
                mean_copy(0, mean_in.at[0], row(member)).start()
            mean_copy(0, mean_in.at[0], root(k)).start()
        mean_copy(0, mean_in.at[0], row(0)).start()

    @pl.when(position > 0)
    def _():
        landed(halo.at[0], halo_recv.at[0])

    @pl.when(is_first)
    def _():
        landed(mean_in.at[1], mean_recv)
        own_mean[...] = (mean_in[0] + mean_in[1]) * (1.0 / area)

    def mean_columns(value):
        return [jnp.sum(jnp.where(lane == g, value, 0.0), axis=1, keepdims=True) for g in groups]

    columns = mean_columns(own_mean[...])
    shifts = [jnp.concatenate(columns[2 * b : 2 * b + 2], axis=0) for b in range(blocks)]
    filter_rows(0, shifts)

    in_two = jnp.logical_or(is_later_root, jnp.logical_and(y == 0, position > 1))

    @pl.when(in_two)
    def _():
        landed(mean_in, mean_recv)

    @pl.when(jnp.logical_not(jnp.logical_or(in_two, is_first)))
    def _():
        landed(mean_in.at[0], mean_recv)

    @pl.when(is_later_root)
    def _():
        own_mean[...] = mean_in[0] + mean_in[1]
        for member in members:
            mean_copy(0, own_mean, row(member)).start()

    @pl.when(jnp.logical_not(is_first))
    def _():
        for g, shift in zip(groups, mean_columns((mean_in[0] + mean_in[1]) * (1.0 / area))):
            lev = pl.ds(8 * g, 8)
            for r in range(rows):
                out[r, lev, :] = out[r, lev, :] - shift

    for side, sender in ((0, position < last), (1, position > 0)):

        @pl.when(sender)
        def _():
            landed(halo.at[side], halo_send.at[side])

    @pl.when(position <= 1)
    def _():
        landed(box.at[pl.ds(0, len(members) + NY - 1)], mean_send)

    @pl.when(is_later_root)
    def _():
        landed(box.at[pl.ds(0, len(members))], mean_send)

    @pl.when(position > 1)
    def _():
        landed(part, up_send)


def local(height, zonal, merid, rates, thresholds, flags, cutoffs):
    rows, levels, nlon = height.shape
    nlat = rows * NX * NY * NC
    fwd, inv, ksq = filter_tables(nlon)
    scalars, cos_sum = row_scalars(nlat)
    tiles = RADIX // 2
    dims = (rows, levels, nlon, nlat)
    f32, bf16 = jnp.float32, jnp.bfloat16
    vmem, smem, dma = pltpu.VMEM, pltpu.SMEM, pltpu.SemaphoreType.DMA
    operands = (height, zonal, merid, rates, thresholds, flags, cutoffs, scalars, ksq, fwd, inv)
    operands = [pltpu.with_memory_space_constraint(jnp.asarray(a), pltpu.HBM) for a in operands]
    return pl.pallas_call(
        functools.partial(kernel, dims, nlon * cos_sum),
        out_shape=vmem(height.shape, f32),
        in_specs=[pl.BlockSpec(memory_space=pltpu.HBM)] * len(operands),
        out_specs=pl.BlockSpec(memory_space=vmem),
        scratch_shapes=[
            vmem(height.shape, f32), vmem(height.shape, f32), vmem(height.shape, f32),
            smem(rates.shape, f32), smem(thresholds.shape, f32), smem(flags.shape, jnp.int32),
            smem(cutoffs.shape, jnp.int32), smem(scalars.shape, f32),
            vmem(ksq.shape, f32), vmem(fwd.shape, bf16), vmem(inv.shape, bf16),
            vmem((2, 3, levels, nlon), f32), vmem((rows, levels, RADIX * HALF), f32),
            vmem((levels, nlon), f32), vmem((levels, nlon), f32), vmem((rows, 8, 2 * HALF), f32),
            vmem((tiles, 4 * levels, 2 * HALF), bf16), vmem((tiles, 2 * levels, 2 * HALF), f32),
            vmem((8, HALF), f32), vmem((NX * NC + NY, 8, HALF), f32), vmem((2, 8, HALF), f32),
            vmem((8, HALF), f32),
            vmem((levels // 8, 8, HALF), f32), vmem((levels // 8, 8, HALF), f32),
            dma((2 * PIECES + 5,)), dma((2,)), dma((2,)), dma, dma, dma, dma, dma, pltpu.SemaphoreType.REGULAR,
        ],
        compiler_params=pltpu.CompilerParams(collective_id=0, has_side_effects=True, vmem_limit_bytes=16 * 2**20),
        name="advect_filter",
    )(*operands)


def solution(mesh):
    finer = Mesh(
        mesh.devices.reshape(mesh.shape["member"], NX, NY, NC), ("member", "lat_0", "lat_1", "lat_2")
    )
    whole = P(("member", "lat_0", "lat_1", "lat_2"), None, None)
    placed = (whole, whole, whole, P("member"), P("member"), P(), P())
    return jax.shard_map(local, mesh=finer, in_specs=placed, out_specs=whole, check_vma=False)
```
